32 devices in a mesh: tensor: 8 (over z, x), expert: 2 (over core), dp: 2 (over y).
Axes of the slice: x: 2, y: 2, z: 4, core: 2. Of those that a mesh axis runs over, the one named last changes fastest.
Arguments:
- tokens: bfloat16 [512, 2048], P(('expert', 'dp')), may hold values from -6 to 6
- tangent: bfloat16 [512, 2048], P(('expert', 'dp')), may hold values from -6 to 6
- cotangent: bfloat16 [512, 2048], P(('expert', 'dp')), may hold values from -0.59765625 to 0.59765625
- expert_ids: int32 [512, 8], P(('expert', 'dp')), may hold values from 0 to 15, all different within a row; in each aligned block of 128 rows (0 to 127, 128 to 255, ...) at most 96 rows name the same one
- gates: float32 [512, 8], P(('expert', 'dp')), may hold values from 0.1 to 1
- w_in: bfloat16 [16, 2, 768, 2048], P(('tensor', 'expert'), None, None, 'dp'), may hold values from -0.125 to 0.125
- v_in: bfloat16 [16, 2, 768, 2048], P(('tensor', 'expert'), None, None, 'dp'), may hold values from -0.125 to 0.125
- w_out: bfloat16 [16, 768, 2048], P(('tensor', 'expert'), None, 'dp'), may hold values from -0.21875 to 0.21875
- v_out: bfloat16 [16, 768, 2048], P(('tensor', 'expert'), None, 'dp'), may hold values from -0.21875 to 0.21875
Outputs:
- hvp_tokens: float32 [512, 2048], P(('expert', 'dp'))
- hvp_in: float32 [16, 2, 768, 2048], P(('tensor', 'expert'), None, None, 'dp')
- hvp_out: float32 [16, 768, 2048], P(('tensor', 'expert'), None, 'dp')
The draws below stay inside these ranges and needn't reach their ends.
Inputs may be any that keep to these rules, and one draw needn't show every extreme that they name: `expert_ids`: each token names 8 different experts; among the tokens of one block of 128 no expert is named more than 96 times, and some expert reaches 96 in some blocks.
All inputs are finite; a program needn't handle non-finite values.
Results may differ from the reference program's by a relative error of at most 0.013.
Values may be sent and summed in bfloat16 or wider, within the bound.
A program may use at most 128 MiB of HBM per device.

```python
import math
import jax
import jax.numpy as jnp
import numpy as np
from jax import lax

D = 2048
FF = 768
TOPK = 8
TOK_DEV = 128
EXPERTS = 16
CAP = 96
TOKENS = 512
N_EXPERT = 2
N_DP = 2


def level_of(rng, extent, pieces, least, high):
    def one(axis_at, blocks):
        draws = jax.random.uniform(jax.random.fold_in(jax.random.fold_in(rng, 6), axis_at), (blocks,), jnp.float32, least / len(pieces), high / len(pieces))
        return jnp.repeat(jnp.exp(draws), extent[axis_at] // blocks).reshape((-1,) + (1,) * (len(extent) - axis_at - 1))

    level = one(*pieces[0])
    for cut in pieces[1:]:
        level = level * one(*cut)
    return level


def routed_block(rng, own, number, rows, number_of, top, reach, slope):
    order = jax.random.permutation(rng, number_of)
    heavy_load, ordinary = shares(number_of, rows * top, reach, slope, True), shares(number_of, rows * top, reach, slope, False)
    places = jnp.arange(number_of)

    def named(tallies, turn):
        used = int((tallies > 0).sum())
        fixed = max(1, used // 4)
        passed = fixed + (places - fixed + turn * (used - fixed)) % max(1, number_of - fixed)
        return jnp.zeros((number_of,), jnp.int32).at[order[jnp.where(places < fixed, places, passed)]].set(jnp.asarray(tallies, jnp.int32))

    tallies = jnp.where(number % 4 == 0, named(heavy_load, number // 4), named(ordinary, number - number // 4 - 1))
    mixed = jax.random.permutation(jax.random.fold_in(own, 3), number_of)
    source_of, receiver = mixed[0:number_of // 2 * 2:2], mixed[1:number_of // 2 * 2:2]
    room = jnp.minimum(tallies[source_of] - 1, reach - tallies[receiver]) // 2
    room = jnp.where((source_of == order[0]) | (receiver == order[0]) | (tallies[receiver] == 0), 0, jnp.maximum(room, 0))
    passed = jax.random.randint(jax.random.fold_in(own, 4), (number_of // 2,), 0, 1 << 20) % (room + 1)
    tallies = tallies.at[source_of].add(-passed).at[receiver].add(passed)
    items = jnp.searchsorted(jnp.cumsum(tallies), jnp.arange(rows * top), side="right").astype(jnp.int32)
    table = items.reshape(top, rows).T
    table = table[jax.random.permutation(jax.random.fold_in(own, 1), rows)]
    turn = jax.random.randint(jax.random.fold_in(own, 2), (rows, 1), 0, top)
    return jnp.take_along_axis(table, (jnp.arange(top)[None, :] + turn) % top, axis=1)


def shares(amount, total, reach, lean, full):
    portions = [(1 << 20) // math.isqrt(standing ** lean) + 1 for standing in range(1, amount + 1)]
    largest = reach if full else min(reach, max(-(-total // amount), total * portions[0] // sum(portions)))
    least = 1 if total - largest >= amount - 1 else 0
    holding, rest = [largest] + [least] * (amount - 1), total - largest - least * (amount - 1)
    while rest > 0:
        free = [i for i in range(1, amount) if holding[i] < largest] or [i for i in range(1, amount) if holding[i] < reach]
        mass, budget = sum([portions[i] for i in free]), rest
        for i in free:
            addition = min(reach - holding[i], max(1, budget * portions[i] // mass), rest)
            holding[i] = holding[i] + addition
            rest = rest - addition
    return np.array(holding)


def scatter_about(rng, extent, width, bound, split=(), kind=jnp.bfloat16):
    factor_of = level_of(rng, extent, split, -0.22, 0.18) if split else 1.0
    entries = jax.random.normal(rng, extent, jnp.float32) * width * factor_of
    return jnp.minimum(jnp.maximum(entries, -bound), bound).astype(kind)


def setup_inputs(seed: int = 0) -> dict:
    key_of = jax.random.split(jax.random.key(seed), 10)
    tokens = scatter_about(key_of[0], (TOKENS, D), 1.0, 6.0, ((0, 4),))
    tangent = scatter_about(key_of[1], (TOKENS, D), 1.0, 6.0, ((0, 4),))
    cotangent = scatter_about(key_of[2], (TOKENS, D), 0.1, 0.59765625, ((0, 4),))
    expert_ids_keys = jax.random.split(jax.random.fold_in(key_of[3], 1), TOKENS // TOK_DEV)
    expert_ids_turns = jax.random.permutation(jax.random.fold_in(key_of[3], 3), TOKENS // TOK_DEV)
    expert_ids = jax.vmap(lambda own, number: routed_block(jax.random.fold_in(key_of[3], 2), own, number, TOK_DEV, EXPERTS, TOPK, CAP, 2))(expert_ids_keys, expert_ids_turns).reshape((TOKENS, TOPK))
    gates = jnp.clip(jnp.exp(math.log(1.0) - 2.3025851 * jax.random.uniform(key_of[4], (TOKENS, TOPK), jnp.float32) ** level_of(key_of[4], (TOKENS, TOPK), ((0, 4),), -0.2, 0.2)), 0.1, 1.0)
    w_in = scatter_about(key_of[5], (EXPERTS, 2, FF, D), D ** -0.5, 0.125, ((0, 16), (3, 2)))
    v_in = scatter_about(key_of[6], (EXPERTS, 2, FF, D), D ** -0.5, 0.125, ((0, 16), (3, 2)))
    w_out = scatter_about(key_of[7], (EXPERTS, FF, D), FF ** -0.5, 0.21875, ((0, 16), (2, 2)))
    v_out = scatter_about(key_of[8], (EXPERTS, FF, D), FF ** -0.5, 0.21875, ((0, 16), (2, 2)))
    return {"tokens": tokens, "tangent": tangent, "cotangent": cotangent, "expert_ids": expert_ids, "gates": gates, "w_in": w_in, "v_in": v_in, "w_out": w_out, "v_out": v_out}


def rounded(value):
    return lax.optimization_barrier(value.astype(jnp.bfloat16)).astype(jnp.float32)


def reference(tokens, tangent, cotangent, expert_ids, gates, w_in, v_in, w_out, v_out):
    blocks = N_EXPERT * N_DP
    pairs = TOK_DEV * TOPK
    picks = expert_ids.reshape(blocks, pairs).astype(jnp.int32)
    onehot = (picks[:, :, None] == jnp.arange(EXPERTS, dtype=jnp.int32)[None, None, :]).astype(jnp.int32)
    running = jnp.cumsum(onehot, axis=1) - 1
    slots = jnp.sum(onehot * running, axis=2).astype(jnp.int32)
    block_ids = jnp.broadcast_to(jnp.arange(blocks, dtype=jnp.int32)[:, None], (blocks, pairs))
    replica = block_ids % N_DP
    source = block_ids // N_DP
    token_ids = block_ids * TOK_DEV + (jnp.arange(pairs, dtype=jnp.int32) // TOPK)[None, :]
    shape = (N_DP, EXPERTS, N_EXPERT, CAP)
    tables = jnp.full(shape, TOKENS, jnp.int32).at[replica, picks, source, slots].set(token_ids)
    scales = jnp.zeros(shape, jnp.float32).at[replica, picks, source, slots].set(gates.reshape(blocks, pairs))
    zero_row = jnp.zeros((1, D), jnp.bfloat16)
    pad_x = jnp.concatenate([tokens, zero_row], axis=0)
    pad_u = jnp.concatenate([tangent, zero_row], axis=0)
    pad_c = jnp.concatenate([cotangent, zero_row], axis=0)

    def one_expert(carry, expert):
        index = tables[:, expert].reshape(N_DP, -1)
        scale = scales[:, expert].reshape(N_DP, -1)
        rows_x = pad_x[index].astype(jnp.float32)
        rows_u = pad_u[index].astype(jnp.float32)
        rows_dy = rounded(scale[:, :, None] * pad_c[index].astype(jnp.float32))
        w_first = w_in[expert].astype(jnp.float32)
        v_first = v_in[expert].astype(jnp.float32)
        w_second = w_out[expert].astype(jnp.float32)
        v_second = v_out[expert].astype(jnp.float32)
        pre = jnp.einsum("prd,gfd->prgf", rows_x, w_first)
        pre_dot = jnp.einsum("prd,gfd->prgf", rows_u, w_first) + jnp.einsum("prd,gfd->prgf", rows_x, v_first)
        gate_pre, up_val = pre[:, :, 0], pre[:, :, 1]
        gate_dot, up_dot = pre_dot[:, :, 0], pre_dot[:, :, 1]
        back = jnp.einsum("prd,fd->prf", rows_dy, w_second)
        back_dot = jnp.einsum("prd,fd->prf", rows_dy, v_second)
        sigma = jax.nn.sigmoid(gate_pre)
        silu_val = gate_pre * sigma
        first = sigma * (1.0 + gate_pre * (1.0 - sigma))
        second = sigma * (1.0 - sigma) * (2.0 + gate_pre * (1.0 - 2.0 * sigma))
        grad_a = back * up_val * first
        grad_b = back * silu_val
        tang_a = back_dot * up_val * first + back * up_dot * first + back * up_val * second * gate_dot
        tang_b = back_dot * silu_val + back * first * gate_dot
        grads = rounded(jnp.stack([grad_a, grad_b], axis=2))
        tangs = rounded(jnp.stack([tang_a, tang_b], axis=2))
        hidden_dot = rounded(first * gate_dot * up_val + silu_val * up_dot)
        partial_value = jnp.einsum("prgf,gfd->prd", tangs, w_first) + jnp.einsum("prgf,gfd->prd", grads, v_first)
        partial_value = rounded(partial_value)
        carry = carry.at[index.reshape(-1)].add(partial_value.reshape(-1, D))
        part_in = jnp.einsum("prd,prgf->pgfd", rows_u, grads) + jnp.einsum("prd,prgf->pgfd", rows_x, tangs)
        part_out = jnp.einsum("prf,prd->pfd", hidden_dot, rows_dy)
        return carry, (jnp.sum(rounded(part_in), axis=0), jnp.sum(rounded(part_out), axis=0))

    start = jnp.zeros((TOKENS + 1, D), jnp.float32)
    total, results = lax.scan(one_expert, start, jnp.arange(EXPERTS, dtype=jnp.int32))
    return total[:TOKENS], results[0], results[1]
```

```python
import functools

import jax
import jax.numpy as jnp
from jax import lax
from jax.experimental import pallas as pl
from jax.experimental.pallas import tpu as pltpu
from jax.sharding import PartitionSpec as P


BF = jnp.bfloat16
F32 = jnp.float32
MESH = pl.DeviceIdType.MESH


def dot_nt(x, w):
    return lax.dot_general(x, w, (((1,), (1,)), ((), ())), preferred_element_type=F32)


def dot_nn(x, w):
    return lax.dot_general(x, w, (((1,), (0,)), ((), ())), preferred_element_type=F32)


def dot_tn(x, w):
    return lax.dot_general(x, w, (((0,), (0,)), ((), ())), preferred_element_type=F32)


def sum_over(own, axis, sent, ahead=None):
    n = lax.axis_size(axis)
    if n & (n - 1):
        return lax.psum(own.astype(BF), axis).astype(F32)
    step = 1
    while step < n:
        give = own.astype(BF)
        if step == 1:
            sent.append(give)
        got = lax.ppermute(give, axis, [(i, i ^ step) for i in range(n)])
        if ahead is not None:
            got, ahead = lax.optimization_barrier((got, ahead))
        own = own + got.astype(F32)
        step *= 2
    return own


def hidden_terms(pre, pre_dot, backs):
    half = pre.shape[1] // 2
    gate_pre, up_val = pre[:, :half], pre[:, half:]
    gate_dot, up_dot = pre_dot[:, :half], pre_dot[:, half:]
    back, back_dot = backs[:, :half], backs[:, half:]
    sigma = jax.nn.sigmoid(gate_pre)
    silu_val = gate_pre * sigma
    first = sigma * (1.0 + gate_pre * (1.0 - sigma))
    second = sigma * (1.0 - sigma) * (2.0 + gate_pre * (1.0 - 2.0 * sigma))
    grad_a = back * up_val * first
    grad_b = back * silu_val
    tang_a = back_dot * up_val * first + back * up_dot * first + back * up_val * second * gate_dot
    tang_b = back_dot * silu_val + back * first * gate_dot
    hidden_dot = first * gate_dot * up_val + silu_val * up_dot
    grads = jnp.concatenate([grad_a, grad_b], axis=1).astype(BF)
    tangs = jnp.concatenate([tang_a, tang_b], axis=1).astype(BF)
    return grads, tangs, hidden_dot.astype(BF)


def plain_shards(tokens, tangent, cotangent, expert_ids, gates, w_in, v_in, w_out, v_out):
    n_tensor = lax.axis_size("tensor")
    n_expert = lax.axis_size("expert")
    n_dp = lax.axis_size("dp")
    rank, core = lax.axis_index("tensor"), lax.axis_index("expert")
    held, _, ff, part = w_in.shape
    all_experts = held * n_tensor * n_expert
    rows, width = tokens.shape
    topk = expert_ids.shape[1]
    cap = min(rows, 3 * rows * topk // (2 * all_experts))

    around = [
        [((i + r) % n_expert, i) for i in range(n_expert)] for r in range(n_expert)
    ]

    def from_cores(v):
        return [v] + [lax.ppermute(v, "expert", around[r]) for r in range(1, n_expert)]

    fields = (tokens, tangent, cotangent)
    if n_dp == 2:
        low_half = [v[:, :part] for v in fields]
        high_half = [v[:, part:] for v in fields]
        first = lax.axis_index("dp") == 0
        give = jnp.where(first, jnp.concatenate(high_half, axis=1), jnp.concatenate(low_half, axis=1))
        keep = jnp.where(first, jnp.concatenate(low_half, axis=1), jnp.concatenate(high_half, axis=1))
        other = lax.ppermute(give, "dp", [(0, 1), (1, 0)])
        keeps, others = jnp.stack(from_cores(keep)), jnp.stack(from_cores(other))
        blocks = [jnp.where(first, keeps, others), jnp.where(first, others, keeps)]
    else:
        mine = lax.all_to_all(jnp.stack(fields, axis=1), "dp", split_axis=2, concat_axis=0, tiled=True)
        mine = mine.reshape(n_dp, rows, 3 * part)
        blocks = jnp.stack(from_cores(mine), axis=1)

    names = jnp.arange(all_experts, dtype=jnp.int32)
    hit = names[:, None, None] == expert_ids.T[None]
    table = jnp.sum(jnp.where(hit, gates.T[None], 0.0), axis=1)
    table = jnp.where(jnp.any(hit, axis=1), table, -1.0)
    tables = jnp.broadcast_to(table[None], (n_expert * n_dp, all_experts, rows))
    tables = lax.all_to_all(tables, ("expert", "dp"), split_axis=0, concat_axis=0, tiled=True)
    tables = tables.reshape(n_expert, n_dp, all_experts, rows)

    low = jnp.tril(jnp.ones((rows, rows), BF))
    weights = [
        (
            w_in[l].reshape(2 * ff, part),
            v_in[l].reshape(2 * ff, part),
            w_out[l],
            v_out[l],
        )
        for l in range(held)
    ]

    def replica(c, before=None):
        saved, spread, sent = [], [0.0] * n_expert, []
        block, ahead = blocks[c], None
        if before is not None:
            block, _ = lax.optimization_barrier((block, before[2]))
            ahead = before[0]
        for l in range(held):
            wi, vi, wo, vo = weights[l]
            expert = (rank * n_expert + core) * held + l
            picks, scales = [], []
            for r in range(n_expert):
                gate = tables[lax.rem(core + r, n_expert), c, expert]
                on = gate >= 0.0
                slot = dot_nt(on.astype(BF)[None, :], low)[0].astype(jnp.int32) - 1
                pick = (jnp.arange(cap, dtype=jnp.int32)[:, None] == slot[None, :]) & on[None, :]
                scales.append(jnp.sum(jnp.where(pick, gate[None, :], 0.0), axis=1))
                picks.append(pick.astype(BF))
            chosen = jnp.einsum(
                "rst,rtd->rsd", jnp.stack(picks), block, preferred_element_type=F32
            ).reshape(n_expert * cap, 3 * part)
            x = chosen[:, :part].astype(BF)
            u = chosen[:, part:2 * part].astype(BF)
            dy = (jnp.concatenate(scales)[:, None] * chosen[:, 2 * part:]).astype(BF)
            pre = sum_over(dot_nt(x, wi), "dp", sent)
            pre_dot = sum_over(dot_nt(u, wi) + dot_nt(x, vi), "dp", sent)
            backs = sum_over(jnp.concatenate([dot_nt(dy, wo), dot_nt(dy, vo)], axis=1), "dp", sent, ahead)
            grads, tangs, hidden = hidden_terms(pre, pre_dot, backs)
            saved.append((x, u, dy, grads, tangs, hidden))
            partial = (dot_nn(tangs, wi) + dot_nn(grads, vi)).astype(BF)
            for r, pick in enumerate(picks):
                spread[r] = spread[r] + dot_tn(pick, partial[r * cap:(r + 1) * cap])
        total = spread[0]
        for r in range(1, n_expert):
            moved = [(i, (i + r) % n_expert) for i in range(n_expert)]
            total = total + lax.ppermute(spread[r].astype(BF), "expert", moved).astype(F32)
        total = total.reshape(n_tensor, rows // n_tensor, part).astype(BF)
        got = lax.all_to_all(total, "tensor", split_axis=0, concat_axis=0, tiled=True)
        return jnp.sum(got.astype(F32), axis=0).astype(BF), saved, sent

    if n_dp <= 2:
        done = [replica(0)]
        for c in range(1, n_dp):
            done.append(replica(c, done[-1]))
        share, saved = jax.tree.map(lambda *v: jnp.stack(v), *[d[:2] for d in done])
    else:
        share, saved = lax.map(lambda c: replica(c)[:2], jnp.arange(n_dp))

    hvp_in, hvp_out = [], []
    for l in range(held):
        x, u, dy, grads, tangs, hidden = (v.reshape(-1, v.shape[-1]) for v in saved[l])
        both = jnp.concatenate([grads, tangs], axis=0)
        hvp_in.append(dot_tn(both, jnp.concatenate([u, x], axis=0)).reshape(2, ff, part))
        hvp_out.append(dot_tn(hidden, dy))

    share = jnp.broadcast_to(share[None], (n_tensor,) + share.shape)
    share = share.reshape((n_tensor * n_dp,) + share.shape[2:])
    share = lax.all_to_all(share, ("tensor", "dp"), split_axis=0, concat_axis=0, tiled=True)
    share = share.reshape(n_tensor, n_dp, rows // n_tensor, part).transpose(0, 2, 1, 3)
    hvp_tokens = share.reshape(rows, width).astype(F32)
    return hvp_tokens, jnp.stack(hvp_in), jnp.stack(hvp_out)


def remote(src, dst, send, recv, where):
    return pltpu.make_async_remote_copy(
        src_ref=src, dst_ref=dst, send_sem=send, recv_sem=recv, device_id=where, device_id_type=MESH
    )


def aligned(index, size):
    return pl.ds(pl.multiple_of(index * size, size), size)


def exchange_kernel(
    n_tensor, topk, cap, fc,
    tok_h, tan_h, cot_h, info_v, w_h, v_h, wo_h, vo_h,
    rows_o, fing_o, finh_o, tok_o,
    w_s, v_s, o_s, tok_s, info_s, pick_s, rows_s, send_s, recv_s, fing_s, finh_s,
    part_s, own_s, give_s, core_s, sum_s, slice_s, share_s, out_s,
    wsem, lsem, osem, c1s, c1r, c2s, c2r, c3s, c3r, c4s, c4r, c5s, c5r, c6s, c6r, c7s, c7r,
    as_, ar_, bs_, br_, cs_, cr_, ys_, yr_, zs_, zr_,
):
    t, e, p = lax.axis_index("tensor"), lax.axis_index("expert"), lax.axis_index("dp")
    q = 1 - p
    core, over = {"expert": 1 - e}, {"dp": q}
    rows, part = tok_s.shape[3], tok_s.shape[4]
    nch = w_s.shape[0]
    few = rows // n_tensor
    width = 2 * topk
    mine, theirs = aligned(p, part), aligned(q, part)
    fields = (tok_h, tan_h, cot_h)
    plane = [{"tensor": lax.rem(t + k, n_tensor)} for k in range(1, n_tensor)]
    peers = [lax.rem(t + k, n_tensor) for k in range(1, n_tensor)]
    slice_t = aligned(t, few)
    own_info = aligned(e, width)

    local = [pltpu.make_async_copy(h.at[:, mine], tok_s.at[0, e, i], lsem.at[i]) for i, h in enumerate(fields)]
    for c in local:
        c.start()

    def weight_copies(f):
        part_f = aligned(f, fc)
        return [
            pltpu.make_async_copy(w_h.at[0, :, part_f, :], w_s.at[f], wsem.at[0, f]),
            pltpu.make_async_copy(v_h.at[0, :, part_f, :], v_s.at[f], wsem.at[1, f]),
            pltpu.make_async_copy(wo_h.at[0, part_f, :], o_s.at[f, 0], wsem.at[2, f]),
            pltpu.make_async_copy(vo_h.at[0, part_f, :], o_s.at[f, 1], wsem.at[3, f]),
        ]

    def load_weights(f, _):
        for c in weight_copies(f):
            c.start()
        return 0

    lax.fori_loop(0, nch, load_weights, 0)

    barrier = pltpu.get_barrier_semaphore()
    for where in [core, over] + plane:
        pl.semaphore_signal(barrier, inc=1, device_id=where, device_id_type=MESH)
    info_s[0, own_info, :] = info_v[...]
    for rep in range(2):
        info_s[rep, 2 * width:, :] = jnp.zeros((info_s.shape[1] - 2 * width, rows), F32)
    pl.semaphore_wait(barrier, 2 + len(plane))

    first = [remote(h.at[:, mine], tok_s.at[0, e, i], c1s.at[i], c1r.at[i], core) for i, h in enumerate(fields)]
    first.append(remote(info_v, info_s.at[0, own_info], c1s.at[3], c1r.at[3], core))
    cross = [
        remote(h.at[slice_t, theirs], tok_s.at[1, e, i, slice_t], c2s.at[i], c2r.at[i], over)
        for i, h in enumerate(fields)
    ]
    cross.append(remote(info_v, info_s.at[1, own_info], c2s.at[3], c2r.at[3], over))
    for c in first + cross:
        c.start()

    expert = (t * 2 + e).astype(F32)
    low = (
        lax.broadcasted_iota(jnp.int32, (rows, rows), 0) > lax.broadcasted_iota(jnp.int32, (rows, rows), 1)
    ).astype(F32).astype(BF)
    lane = lax.broadcasted_iota(jnp.int32, (rows, rows), 1).astype(F32)

    def gather(rep):
        info = info_s[rep].T
        for s in range(2):
            ids = info[:, s * width:s * width + topk]
            gates = info[:, s * width + topk:(s + 1) * width]
            hit = ids == expert
            on = jnp.sum(jnp.where(hit, 1.0, 0.0), axis=1, keepdims=True)
            gate = jnp.sum(jnp.where(hit, gates, 0.0), axis=1, keepdims=True)
            on = jnp.broadcast_to(on, (rows, rows))
            slot = dot_nn(low, on.astype(BF))
            pick = jnp.where((slot == lane) & (on > 0.5), 1.0, 0.0)
            pick_s[rep, s] = pick.astype(BF)
            pick = pick.T.astype(BF)[:cap]
            x = dot_nn(pick, tok_s[rep, s, 0]).astype(BF)
            u = dot_nn(pick, tok_s[rep, s, 1]).astype(BF)
            scaled = (gate * tok_s[rep, s, 2].astype(F32)).astype(BF)
            dy = dot_nn(pick, scaled).astype(BF)
            for i, v in enumerate((x, u, dy)):
                rows_s[rep, i, s * cap:(s + 1) * cap, :] = v

    def products(rep, f):
        w = w_s[f].reshape(2 * fc, part)
        v = v_s[f].reshape(2 * fc, part)
        o = o_s[f].reshape(2 * fc, part)
        x, u, dy = rows_s[rep, 0], rows_s[rep, 1], rows_s[rep, 2]
        return dot_nt(x, w), dot_nt(u, w) + dot_nt(x, v), dot_nt(dy, o)

    for c in local:
        c.wait()
    for c in first:
        c.wait_recv()
    gather(0)
    rows_out = [pltpu.make_async_copy(rows_s.at[rep], rows_o.at[rep], osem.at[rep]) for rep in range(2)]
    rows_out[0].start()

    def chunk_copy(f):
        return remote(send_s.at[f], recv_s.at[f], c5s.at[f], c5r.at[f], over)

    def send_chunk(f, _):
        for c in weight_copies(f):
            c.wait()
        pre, pre_dot, back = products(0, f)
        send_s[f, :, :2 * fc] = pre.astype(BF)
        send_s[f, :, 2 * fc:4 * fc] = pre_dot.astype(BF)
        send_s[f, :, 4 * fc:] = back.astype(BF)
        chunk_copy(f).start()
        return 0

    lax.fori_loop(0, 1, send_chunk, 0)

    for c in cross:
        c.wait_recv()
    shared = [
        remote(tok_s.at[1, e, :, slice_t], tok_s.at[1, e, :, slice_t], c3s.at[k], c3r.at[k], where)
        for k, where in enumerate(plane)
    ]
    for c in shared:
        c.start()
    lax.fori_loop(1, nch, send_chunk, 0)
    for c in shared:
        c.wait_recv()
    passed = [
        remote(tok_s.at[1, e], tok_s.at[1, e], c4s.at[0], c4r.at[0], core),
        remote(info_s.at[1, own_info], info_s.at[1, own_info], c4s.at[1], c4r.at[1], core),
    ]
    for c in passed:
        c.start()
    for c in passed:
        c.wait_recv()
    gather(1)
    rows_out[1].start()

    def back_rows(rep, f):
        w = w_s[f].reshape(2 * fc, part)
        v = v_s[f].reshape(2 * fc, part)
        g = fing_s[rep, f]
        return dot_nn(g[:, 2 * fc:], w) + dot_nn(g[:, :2 * fc], v)

    def grads_copy(f):
        return remote(fing_s.at[1, f], fing_s.at[0, f], c6s.at[f], c6r.at[f], over)

    part_s[...] = jnp.zeros_like(part_s)

    def finish_chunk(f, _):
        pre, pre_dot, back = products(1, f)
        chunk_copy(f).wait_recv()
        pre = pre + recv_s[f, :, :2 * fc].astype(F32)
        pre_dot = pre_dot + recv_s[f, :, 2 * fc:4 * fc].astype(F32)
        back = back + recv_s[f, :, 4 * fc:].astype(F32)
        grads, tangs, hidden = hidden_terms(pre, pre_dot, back)
        fing_s[1, f, :, :2 * fc] = grads
        fing_s[1, f, :, 2 * fc:] = tangs
        finh_s[1, f] = hidden
        grads_copy(f).start()
        part_s[1] += back_rows(1, f)
        return 0

    lax.fori_loop(0, nch, finish_chunk, 0)
    hidden_copy = remote(finh_s.at[1], finh_s.at[0], c7s, c7r, over)
    hidden_copy.start()
    fing_out = [pltpu.make_async_copy(fing_s.at[rep], fing_o.at[rep], osem.at[2 + rep]) for rep in range(2)]
    finh_out = [pltpu.make_async_copy(finh_s.at[rep], finh_o.at[rep], osem.at[4 + rep]) for rep in range(2)]
    fing_out[1].start()
    finh_out[1].start()

    def spread(rep, s):
        return dot_nn(pick_s[rep, s][:, :cap], part_s[rep, aligned(s, cap), :].astype(BF))

    def core_copy(rep):
        return remote(give_s.at[rep], core_s.at[rep], as_.at[rep], ar_.at[rep], core)

    def slice_copies(rep):
        return [
            remote(sum_s.at[rep, aligned(peer, few)], slice_s.at[rep, k], bs_.at[rep, k], br_.at[rep, k], where)
            for k, (peer, where) in enumerate(zip(peers, plane))
        ]

    def over_experts(rep):
        give_s[rep] = spread(rep, 1 - e).astype(BF)
        core_copy(rep).start()
        own_s[...] = spread(rep, e)
        core_copy(rep).wait_recv()
        sum_s[rep] = (own_s[...] + core_s[rep].astype(F32)).astype(BF)
        for c in slice_copies(rep):
            c.start()
        for c in slice_copies(rep):
            c.wait_recv()
        total = sum_s[rep, slice_t].astype(F32)
        for k in range(n_tensor - 1):
            total = total + slice_s[rep, k].astype(F32)
        return total.astype(BF)

    def out_copies(half, sends, recvs):
        return [
            remote(out_s.at[half, slice_t], out_s.at[half, slice_t], sends.at[k], recvs.at[k], where)
            for k, where in enumerate(plane)
        ]

    share_s[...] = over_experts(1)
    share_copy = remote(share_s, out_s.at[1, slice_t], ys_, yr_, over)
    share_copy.start()

    def take_back(f, _):
        grads_copy(f).wait_recv()
        part_s[0] += back_rows(0, f)
        return 0

    lax.fori_loop(0, nch, take_back, 0)
    fing_out[0].start()
    share_copy.wait_recv()
    second = out_copies(1, zs_, zr_)
    for c in second:
        c.start()
    out_s[0, slice_t] = over_experts(0)
    third = out_copies(0, cs_, cr_)
    for c in third:
        c.start()
    hidden_copy.wait_recv()
    finh_out[0].start()
    for c in second + third:
        c.wait_recv()
    tok_o[:, mine] = out_s[0]
    tok_o[:, theirs] = out_s[1]

    for c in first + cross + shared + passed + second + third + [hidden_copy, share_copy]:
        c.wait_send()
    for rep in range(2):
        core_copy(rep).wait_send()
        for c in slice_copies(rep):
            c.wait_send()

    def drain(f, _):
        chunk_copy(f).wait_send()
        grads_copy(f).wait_send()
        return 0

    lax.fori_loop(0, nch, drain, 0)
    for c in rows_out + fing_out + finh_out:
        c.wait()


def exchange(tokens, tangent, cotangent, info, w_in, v_in, w_out, v_out, cap, fc, topk):
    n_tensor = lax.axis_size("tensor")
    rows, width = tokens.shape
    _, _, ff, part = w_in.shape
    nch, few, peers = ff // fc, rows // n_tensor, n_tensor - 1
    dma = pltpu.SemaphoreType.DMA
    anyspace = pl.BlockSpec(memory_space=pl.ANY)
    vmem = pl.BlockSpec(memory_space=pltpu.VMEM)
    return pl.pallas_call(
        functools.partial(exchange_kernel, n_tensor, topk, cap, fc),
        name="exchange",
        out_shape=[
            jax.ShapeDtypeStruct((2, 3, 2 * cap, part), BF),
            jax.ShapeDtypeStruct((2, nch, 2 * cap, 4 * fc), BF),
            jax.ShapeDtypeStruct((2, nch, 2 * cap, fc), BF),
            jax.ShapeDtypeStruct((rows, width), BF),
        ],
        in_specs=[anyspace] * 3 + [vmem] + [anyspace] * 4,
        out_specs=[anyspace] * 3 + [vmem],
        scratch_shapes=[
            pltpu.VMEM((nch, 2, fc, part), BF),
            pltpu.VMEM((nch, 2, fc, part), BF),
            pltpu.VMEM((nch, 2, fc, part), BF),
            pltpu.VMEM((2, 2, 3, rows, part), BF),
            pltpu.VMEM((2, rows, rows), F32),
            pltpu.VMEM((2, 2, rows, rows), BF),
            pltpu.VMEM((2, 3, 2 * cap, part), BF),
            pltpu.VMEM((nch, 2 * cap, 6 * fc), BF),
            pltpu.VMEM((nch, 2 * cap, 6 * fc), BF),
            pltpu.VMEM((2, nch, 2 * cap, 4 * fc), BF),
            pltpu.VMEM((2, nch, 2 * cap, fc), BF),
            pltpu.VMEM((2, 2 * cap, part), F32),
            pltpu.VMEM((rows, part), F32),
            pltpu.VMEM((2, rows, part), BF),
            pltpu.VMEM((2, rows, part), BF),
            pltpu.VMEM((2, rows, part), BF),
            pltpu.VMEM((2, peers, few, part), BF),
            pltpu.VMEM((few, part), BF),
            pltpu.VMEM((2, rows, part), BF),
            dma((4, nch)), dma((3,)), dma((6,)),
            dma((4,)), dma((4,)), dma((4,)), dma((4,)),
            dma((peers,)), dma((peers,)), dma((2,)), dma((2,)),
            dma((nch,)), dma((nch,)), dma((nch,)), dma((nch,)), dma, dma,
            dma((2,)), dma((2,)), dma((2, peers)), dma((2, peers)),
            dma((peers,)), dma((peers,)), dma, dma, dma((peers,)), dma((peers,)),
        ],
        compiler_params=pltpu.CompilerParams(
            collective_id=0, has_side_effects=True, vmem_limit_bytes=60 * 1024 * 1024
        ),
    )(tokens, tangent, cotangent, info, w_in, v_in, w_out, v_out)


def weights_kernel(rows_ref, fing_ref, finh_ref, in_ref, out_ref):
    fc, part = in_ref.shape[2], in_ref.shape[3]
    total_in = total_out = 0.0
    for rep in range(2):
        g = fing_ref[rep, 0]
        x, u, dy = rows_ref[rep, 0], rows_ref[rep, 1], rows_ref[rep, 2]
        total_in = total_in + dot_tn(g[:, :2 * fc], u) + dot_tn(g[:, 2 * fc:], x)
        total_out = total_out + dot_tn(finh_ref[rep, 0], dy)
    in_ref[0] = total_in.reshape(2, fc, part)
    out_ref[0] = total_out


def weight_results(rows, fing, finh, ff, fc):
    _, _, many, part = rows.shape
    nch = ff // fc
    return pl.pallas_call(
        weights_kernel,
        name="weights",
        grid=(nch,),
        out_shape=[
            jax.ShapeDtypeStruct((1, 2, ff, part), F32),
            jax.ShapeDtypeStruct((1, ff, part), F32),
        ],
        in_specs=[
            pl.BlockSpec(rows.shape, lambda f: (0, 0, 0, 0)),
            pl.BlockSpec((2, 1, many, 4 * fc), lambda f: (0, f, 0, 0)),
            pl.BlockSpec((2, 1, many, fc), lambda f: (0, f, 0, 0)),
        ],
        out_specs=[
            pl.BlockSpec((1, 2, fc, part), lambda f: (0, 0, f, 0)),
            pl.BlockSpec((1, fc, part), lambda f: (0, f, 0)),
        ],
        cost_estimate=pl.CostEstimate(
            flops=2 * 2 * many * 5 * ff * part, bytes_accessed=12 * ff * part, transcendentals=0
        ),
    )(rows, fing, finh)


def kernel_shards(tokens, tangent, cotangent, expert_ids, gates, w_in, v_in, w_out, v_out):
    rows, _ = tokens.shape
    topk = expert_ids.shape[1]
    ff = w_in.shape[2]
    all_experts = lax.axis_size("tensor") * lax.axis_size("expert")
    cap = min(rows, 3 * rows * topk // (2 * all_experts))
    fc = 128
    info = jnp.concatenate([expert_ids.T.astype(F32), gates.T], axis=0)
    kept, fing, finh, out = exchange(
        tokens, tangent, cotangent, info, w_in, v_in, w_out, v_out, cap, fc, topk
    )
    hvp_in, hvp_out = weight_results(kept, fing, finh, ff, fc)
    return out.astype(F32), hvp_in, hvp_out


def shards(*args):
    tokens, expert_ids, w_in = args[0], args[3], args[5]
    n_tensor = lax.axis_size("tensor")
    rows, topk = expert_ids.shape
    fits = (
        lax.axis_size("expert") == 2 and lax.axis_size("dp") == 2 and w_in.shape[0] == 1
        and tokens.shape[1] == 2 * w_in.shape[3] and w_in.shape[3] % 128 == 0 and w_in.shape[2] % 128 == 0
        and rows == 128 and n_tensor > 1 and rows % (16 * n_tensor) == 0
        and topk % 4 == 0 and 4 * topk < rows and (3 * rows * topk) % (64 * n_tensor) == 0
    )
    return (kernel_shards if fits else plain_shards)(*args)


def solution(mesh):
    rows = P(("expert", "dp"), None)
    wide = P(("tensor", "expert"), None, None, "dp")
    tall = P(("tensor", "expert"), None, "dp")
    return jax.shard_map(
        shards,
        mesh=mesh,
        in_specs=(rows, rows, rows, rows, rows, wide, wide, tall, tall),
        out_specs=(rows, wide, tall),
        check_vma=False,
    )
```

```python
import functools

import jax
import jax.numpy as jnp
from jax import lax
from jax.experimental import pallas as pl
from jax.experimental.pallas import tpu as pltpu
from jax.sharding import PartitionSpec as P


BF = jnp.bfloat16
F32 = jnp.float32
MESH = pl.DeviceIdType.MESH


def dot_nt(x, w):
    return lax.dot_general(x, w, (((1,), (1,)), ((), ())), preferred_element_type=F32)


def dot_nn(x, w):
    return lax.dot_general(x, w, (((1,), (0,)), ((), ())), preferred_element_type=F32)


def dot_tn(x, w):
    return lax.dot_general(x, w, (((0,), (0,)), ((), ())), preferred_element_type=F32)


def sum_over(own, axis, sent, ahead=None):
    n = lax.axis_size(axis)
    if n & (n - 1):
        return lax.psum(own.astype(BF), axis).astype(F32)
    step = 1
    while step < n:
        give = own.astype(BF)
        if step == 1:
            sent.append(give)
        got = lax.ppermute(give, axis, [(i, i ^ step) for i in range(n)])
        if ahead is not None:
            got, ahead = lax.optimization_barrier((got, ahead))
        own = own + got.astype(F32)
        step *= 2
    return own


def hidden_terms(pre, pre_dot, backs):
    half = pre.shape[1] // 2
    gate_pre, up_val = pre[:, :half], pre[:, half:]
    gate_dot, up_dot = pre_dot[:, :half], pre_dot[:, half:]
    back, back_dot = backs[:, :half], backs[:, half:]
    sigma = jax.nn.sigmoid(gate_pre)
    silu_val = gate_pre * sigma
    first = sigma * (1.0 + gate_pre * (1.0 - sigma))
    second = sigma * (1.0 - sigma) * (2.0 + gate_pre * (1.0 - 2.0 * sigma))
    grad_a = back * up_val * first
    grad_b = back * silu_val
    tang_a = back_dot * up_val * first + back * up_dot * first + back * up_val * second * gate_dot
    tang_b = back_dot * silu_val + back * first * gate_dot
    hidden_dot = first * gate_dot * up_val + silu_val * up_dot
    grads = jnp.concatenate([grad_a, grad_b], axis=1).astype(BF)
    tangs = jnp.concatenate([tang_a, tang_b], axis=1).astype(BF)
    return grads, tangs, hidden_dot.astype(BF)


def plain_shards(tokens, tangent, cotangent, expert_ids, gates, w_in, v_in, w_out, v_out):
    n_tensor = lax.axis_size("tensor")
    n_expert = lax.axis_size("expert")
    n_dp = lax.axis_size("dp")
    rank, core = lax.axis_index("tensor"), lax.axis_index("expert")
    held, _, ff, part = w_in.shape
    all_experts = held * n_tensor * n_expert
    rows, width = tokens.shape
    topk = expert_ids.shape[1]
    cap = min(rows, 3 * rows * topk // (2 * all_experts))

    around = [
        [((i + r) % n_expert, i) for i in range(n_expert)] for r in range(n_expert)
    ]

    def from_cores(v):
        return [v] + [lax.ppermute(v, "expert", around[r]) for r in range(1, n_expert)]

    fields = (tokens, tangent, cotangent)
    if n_dp == 2:
        low_half = [v[:, :part] for v in fields]
        high_half = [v[:, part:] for v in fields]
        first = lax.axis_index("dp") == 0
        give = jnp.where(first, jnp.concatenate(high_half, axis=1), jnp.concatenate(low_half, axis=1))
        keep = jnp.where(first, jnp.concatenate(low_half, axis=1), jnp.concatenate(high_half, axis=1))
        other = lax.ppermute(give, "dp", [(0, 1), (1, 0)])
        keeps, others = jnp.stack(from_cores(keep)), jnp.stack(from_cores(other))
        blocks = [jnp.where(first, keeps, others), jnp.where(first, others, keeps)]
    else:
        mine = lax.all_to_all(jnp.stack(fields, axis=1), "dp", split_axis=2, concat_axis=0, tiled=True)
        mine = mine.reshape(n_dp, rows, 3 * part)
        blocks = jnp.stack(from_cores(mine), axis=1)

    names = jnp.arange(all_experts, dtype=jnp.int32)
    hit = names[:, None, None] == expert_ids.T[None]
    table = jnp.sum(jnp.where(hit, gates.T[None], 0.0), axis=1)
    table = jnp.where(jnp.any(hit, axis=1), table, -1.0)
    tables = jnp.broadcast_to(table[None], (n_expert * n_dp, all_experts, rows))
    tables = lax.all_to_all(tables, ("expert", "dp"), split_axis=0, concat_axis=0, tiled=True)
    tables = tables.reshape(n_expert, n_dp, all_experts, rows)

    low = jnp.tril(jnp.ones((rows, rows), BF))
    weights = [
        (
            w_in[l].reshape(2 * ff, part),
            v_in[l].reshape(2 * ff, part),
            w_out[l],
            v_out[l],
        )
        for l in range(held)
    ]

    def replica(c, before=None):
        saved, spread, sent = [], [0.0] * n_expert, []
        block, ahead = blocks[c], None
        if before is not None:
            block, _ = lax.optimization_barrier((block, before[2]))
            ahead = before[0]
        for l in range(held):
            wi, vi, wo, vo = weights[l]
            expert = (rank * n_expert + core) * held + l
            picks, scales = [], []
            for r in range(n_expert):
                gate = tables[lax.rem(core + r, n_expert), c, expert]
                on = gate >= 0.0
                slot = dot_nt(on.astype(BF)[None, :], low)[0].astype(jnp.int32) - 1
                pick = (jnp.arange(cap, dtype=jnp.int32)[:, None] == slot[None, :]) & on[None, :]
                scales.append(jnp.sum(jnp.where(pick, gate[None, :], 0.0), axis=1))
                picks.append(pick.astype(BF))
            chosen = jnp.einsum(
                "rst,rtd->rsd", jnp.stack(picks), block, preferred_element_type=F32
            ).reshape(n_expert * cap, 3 * part)
            x = chosen[:, :part].astype(BF)
            u = chosen[:, part:2 * part].astype(BF)
            dy = (jnp.concatenate(scales)[:, None] * chosen[:, 2 * part:]).astype(BF)
            pre = sum_over(dot_nt(x, wi), "dp", sent)
            pre_dot = sum_over(dot_nt(u, wi) + dot_nt(x, vi), "dp", sent)
            backs = sum_over(jnp.concatenate([dot_nt(dy, wo), dot_nt(dy, vo)], axis=1), "dp", sent, ahead)
            grads, tangs, hidden = hidden_terms(pre, pre_dot, backs)
            saved.append((x, u, dy, grads, tangs, hidden))
            partial = (dot_nn(tangs, wi) + dot_nn(grads, vi)).astype(BF)
            for r, pick in enumerate(picks):
                spread[r] = spread[r] + dot_tn(pick, partial[r * cap:(r + 1) * cap])
        total = spread[0]
        for r in range(1, n_expert):
            moved = [(i, (i + r) % n_expert) for i in range(n_expert)]
            total = total + lax.ppermute(spread[r].astype(BF), "expert", moved).astype(F32)
        total = total.reshape(n_tensor, rows // n_tensor, part).astype(BF)
        got = lax.all_to_all(total, "tensor", split_axis=0, concat_axis=0, tiled=True)
        return jnp.sum(got.astype(F32), axis=0).astype(BF), saved, sent

    if n_dp <= 2:
        done = [replica(0)]
        for c in range(1, n_dp):
            done.append(replica(c, done[-1]))
        share, saved = jax.tree.map(lambda *v: jnp.stack(v), *[d[:2] for d in done])
    else:
        share, saved = lax.map(lambda c: replica(c)[:2], jnp.arange(n_dp))

    hvp_in, hvp_out = [], []
    for l in range(held):
        x, u, dy, grads, tangs, hidden = (v.reshape(-1, v.shape[-1]) for v in saved[l])
        both = jnp.concatenate([grads, tangs], axis=0)
        hvp_in.append(dot_tn(both, jnp.concatenate([u, x], axis=0)).reshape(2, ff, part))
        hvp_out.append(dot_tn(hidden, dy))

    share = jnp.broadcast_to(share[None], (n_tensor,) + share.shape)
    share = share.reshape((n_tensor * n_dp,) + share.shape[2:])
    share = lax.all_to_all(share, ("tensor", "dp"), split_axis=0, concat_axis=0, tiled=True)
    share = share.reshape(n_tensor, n_dp, rows // n_tensor, part).transpose(0, 2, 1, 3)
    hvp_tokens = share.reshape(rows, width).astype(F32)
    return hvp_tokens, jnp.stack(hvp_in), jnp.stack(hvp_out)


def remote(src, dst, send, recv, where):
    return pltpu.make_async_remote_copy(
        src_ref=src, dst_ref=dst, send_sem=send, recv_sem=recv, device_id=where, device_id_type=MESH
    )


def aligned(index, size):
    return pl.ds(pl.multiple_of(index * size, size), size)


def exchange_kernel(
    n_tensor, topk, cap, fc,
    tok_h, tan_h, cot_h, ids_v, gates_v, w_h, v_h, wo_h, vo_h,
    in_o, out_o, tok_o,
    w_s, v_s, o_s, tok_s, info_s, pick_s, rows_s, send_s, recv_s, fing_s, finh_s,
    part_s, own_s, give_s, core_s, sum_s, slice_s, share_s, ready_s,
    hin_s, hout_s, in16_s, out16_s,
    wsem, lsem, osem, c1s, c1r, c2s, c2r, c3s, c3r, c4s, c4r, c5s, c5r, c6s, c6r, c7s, c7r,
    as_, ar_, bs_, br_, cs_, cr_, ys_, yr_, zs_, zr_,
):
    t, e, p = lax.axis_index("tensor"), lax.axis_index("expert"), lax.axis_index("dp")
    q, other = 1 - p, 1 - e
    core, over = {"expert": other}, {"dp": q}
    rows, part = tok_s.shape[3], tok_s.shape[4]
    nch = w_s.shape[0]
    half = nch // 2
    few = rows // n_tensor
    mine, theirs = aligned(p, part), aligned(q, part)
    fields = (tan_h, tok_h, cot_h)
    plane = [{"tensor": lax.rem(t + k, n_tensor)} for k in range(1, n_tensor)]
    peers = [lax.rem(t + k, n_tensor) for k in range(1, n_tensor)]
    slice_t = aligned(t, few)

    local = [pltpu.make_async_copy(h.at[:, mine], tok_s.at[0, e, i], lsem.at[i]) for i, h in enumerate(fields)]
    for c in local:
        c.start()

    def weight_copies(f):
        part_f = aligned(f, fc)
        return [
            pltpu.make_async_copy(w_h.at[0, :, part_f, :], w_s.at[f], wsem.at[0, f]),
            pltpu.make_async_copy(v_h.at[0, :, part_f, :], v_s.at[f], wsem.at[1, f]),
            pltpu.make_async_copy(wo_h.at[0, part_f, :], o_s.at[f, 0], wsem.at[2, f]),
            pltpu.make_async_copy(vo_h.at[0, part_f, :], o_s.at[f, 1], wsem.at[3, f]),
        ]

    def load_weights(f, _):
        for c in weight_copies(f):
            c.start()
        return 0

    lax.fori_loop(0, nch, load_weights, 0)

    barrier = pltpu.get_barrier_semaphore()
    for where in [core, over] + plane:
        pl.semaphore_signal(barrier, inc=1, device_id=where, device_id_type=MESH)
    info_s[0, e, :topk, :] = ids_v[...].astype(F32)
    info_s[0, e, topk:, :] = gates_v[...]

    expert = (t * 2 + e).astype(F32)
    low = (
        lax.broadcasted_iota(jnp.int32, (rows, rows), 0) > lax.broadcasted_iota(jnp.int32, (rows, rows), 1)
    ).astype(F32).astype(BF)
    lane = lax.broadcasted_iota(jnp.int32, (rows, rows), 1).astype(F32)

    def gather(rep, s):
        info = info_s[rep, s].T
        hit = info[:, :topk] == expert
        on = jnp.sum(jnp.where(hit, 1.0, 0.0), axis=1, keepdims=True)
        gate = jnp.sum(jnp.where(hit, info[:, topk:], 0.0), axis=1, keepdims=True)
        on = jnp.broadcast_to(on, (rows, rows))
        slot = dot_nn(low, on.astype(BF))
        pick = jnp.where((slot == lane) & (on > 0.5), 1.0, 0.0)
        pick_s[rep, s] = pick.astype(BF)
        pick = pick.T.astype(BF)[:cap]
        rows_s[rep, s, 0] = dot_nn(pick, tok_s[rep, s, 0]).astype(BF)
        rows_s[rep, s, 1] = dot_nn(pick, tok_s[rep, s, 1]).astype(BF)
        scaled = (gate * tok_s[rep, s, 2].astype(F32)).astype(BF)
        rows_s[rep, s, 2] = dot_nn(pick, scaled).astype(BF)

    def products(rep, s, f):
        w = w_s[f].reshape(2 * fc, part)
        v = v_s[f].reshape(2 * fc, part)
        o = o_s[f].reshape(2 * fc, part)
        both = dot_nt(rows_s[rep, s, 0:2].reshape(2 * cap, part), w)
        return both[cap:], both[:cap] + dot_nt(rows_s[rep, s, 1], v), dot_nt(rows_s[rep, s, 2], o)

    def chunk_copy(s, f):
        return remote(send_s.at[s, f], recv_s.at[s, f], c5s.at[s, f], c5r.at[s, f], over)

    def make_chunk(s, f):
        pre, pre_dot, back = products(0, s, f)
        send_s[s, f, :, :2 * fc] = pre.astype(BF)
        send_s[s, f, :, 2 * fc:4 * fc] = pre_dot.astype(BF)
        send_s[s, f, :, 4 * fc:] = back.astype(BF)

    for c in local:
        c.wait()
    gather(0, e)
    for c in weight_copies(0):
        c.wait()
    make_chunk(e, 0)
    pl.semaphore_wait(barrier, 2 + len(plane))

    cross = [
        remote(h.at[slice_t, theirs], tok_s.at[1, e, i, slice_t], c2s.at[i], c2r.at[i], over)
        for i, h in enumerate(fields)
    ]
    cross.append(remote(info_s.at[0, e], info_s.at[1, e], c2s.at[3], c2r.at[3], over))
    first = [remote(h.at[:, mine], tok_s.at[0, e, i], c1s.at[i], c1r.at[i], core) for i, h in enumerate(fields)]
    first.append(remote(info_s.at[0, e], info_s.at[0, e], c1s.at[3], c1r.at[3], core))
    for c in cross + first:
        c.start()
    chunk_copy(e, 0).start()

    def send_own(f, _):
        for c in weight_copies(f):
            c.wait()
        make_chunk(e, f)
        chunk_copy(e, f).start()
        return 0

    lax.fori_loop(1, nch, send_own, 0)
    for c in first:
        c.wait_recv()
    gather(0, other)

    for c in cross:
        c.wait_recv()
    shared = [
        remote(tok_s.at[1, e, :, slice_t], tok_s.at[1, e, :, slice_t], c3s.at[k], c3r.at[k], where)
        for k, where in enumerate(plane)
    ]
    for c in shared:
        c.start()

    def send_other(f, _):
        make_chunk(other, f)
        chunk_copy(other, f).start()
        return 0

    lax.fori_loop(0, nch, send_other, 0)
    for c in shared:
        c.wait_recv()
    passed = [
        remote(tok_s.at[1, e], tok_s.at[1, e], c4s.at[0], c4r.at[0], core),
        remote(info_s.at[1, e], info_s.at[1, e], c4s.at[1], c4r.at[1], core),
    ]
    for c in passed:
        c.start()
    gather(1, e)
    for c in passed:
        c.wait_recv()
    gather(1, other)

    def back_rows(rep, s, f):
        w = w_s[f].reshape(2 * fc, part)
        v = v_s[f].reshape(2 * fc, part)
        g = fing_s[rep, s, f]
        return dot_nn(g[cap:], w) + dot_nn(g[:cap], v)

    def grads_copy(s, f):
        return remote(fing_s.at[1, s, f], fing_s.at[0, s, f], c6s.at[s, f], c6r.at[s, f], over)

    part_s[...] = jnp.zeros_like(part_s)

    def finish_chunk(i, _):
        s, f = lax.rem(e + i // nch, 2), lax.rem(i, nch)
        pre, pre_dot, back = products(1, s, f)
        chunk_copy(s, f).wait_recv()
        pre = pre + recv_s[s, f, :, :2 * fc].astype(F32)
        pre_dot = pre_dot + recv_s[s, f, :, 2 * fc:4 * fc].astype(F32)
        back = back + recv_s[s, f, :, 4 * fc:].astype(F32)
        grads, tangs, hidden = hidden_terms(pre, pre_dot, back)
        fing_s[1, s, f, :cap] = grads
        fing_s[1, s, f, cap:] = tangs
        finh_s[1, s, f] = hidden

        @pl.when(s == 0)
        def _():
            grads_copy(0, f).start()

        part_s[1, s] += back_rows(1, s, f)
        return 0

    lax.fori_loop(0, 2 * nch, finish_chunk, 0)

    def give_back(f, _):
        grads_copy(1, f).start()
        return 0

    lax.fori_loop(0, half, give_back, 0)

    def spread(rep, s):
        return dot_nn(pick_s[rep, s][:, :cap], part_s[rep, s].astype(BF))

    def core_copy(rep):
        return remote(give_s.at[rep], core_s.at[rep], as_.at[rep], ar_.at[rep], core)

    def slice_copies(rep):
        return [
            remote(sum_s.at[rep, aligned(peer, few)], slice_s.at[rep, k], bs_.at[rep, k], br_.at[rep, k], where)
            for k, (peer, where) in enumerate(zip(peers, plane))
        ]

    def over_cores(rep):
        core_copy(rep).wait_recv()
        sum_s[rep] = (own_s[...] + core_s[rep].astype(F32)).astype(BF)
        for c in slice_copies(rep):
            c.start()

    def over_plane(rep):
        for c in slice_copies(rep):
            c.wait_recv()
        total = sum_s[rep, slice_t].astype(F32)
        for k in range(n_tensor - 1):
            total = total + slice_s[rep, k].astype(F32)
        return total.astype(BF)

    def out_copies(side, sends, recvs):
        return [
            remote(ready_s.at[side, slice_t], ready_s.at[side, slice_t], sends.at[k], recvs.at[k], where)
            for k, where in enumerate(plane)
        ]

    def in_term(rep, s, f):
        return dot_tn(fing_s[rep, s, f], rows_s[rep, s, 0:2].reshape(2 * cap, part))

    def out_term(rep, s, f):
        return dot_tn(finh_s[rep, s, f], rows_s[rep, s, 2])

    def start_weights(f, _):
        hin_s[f] = in_term(1, 0, f) + in_term(1, 1, f)
        hout_s[f] = out_term(1, 0, f) + out_term(1, 1, f)
        return 0

    give_s[1] = spread(1, other).astype(BF)
    core_copy(1).start()
    own_s[...] = spread(1, e)
    lax.fori_loop(0, half, start_weights, 0)
    over_cores(1)
    lax.fori_loop(half, nch, start_weights, 0)
    share_s[...] = over_plane(1)
    share_copy = remote(share_s, ready_s.at[1, slice_t], ys_, yr_, over)
    share_copy.start()
    lax.fori_loop(half, nch, give_back, 0)
    hidden_copy = remote(finh_s.at[1], finh_s.at[0], c7s, c7r, over)
    hidden_copy.start()

    def take_first(f, _):
        grads_copy(0, f).wait_recv()
        part_s[0, 0] += back_rows(0, 0, f)
        hin_s[f] += in_term(0, 0, f)
        return 0

    def take_second(f, _):
        grads_copy(1, f).wait_recv()
        part_s[0, 1] += back_rows(0, 1, f)
        return 0

    def to_owner(s):
        @pl.when(e != s)
        def _():
            give_s[0] = spread(0, s).astype(BF)
            core_copy(0).start()

        @pl.when(e == s)
        def _():
            own_s[...] = spread(0, s)

    third = out_copies(0, cs_, cr_)

    def owner_sums():
        over_cores(0)

    def owner_shares():
        ready_s[0, slice_t] = over_plane(0)
        for c in third:
            c.start()

    lax.fori_loop(0, nch, take_first, 0)
    to_owner(0)
    pl.when(e == 0)(owner_sums)
    pl.when(e == 0)(owner_shares)
    share_copy.wait_recv()
    second = out_copies(1, zs_, zr_)
    for c in second:
        c.start()
    lax.fori_loop(0, nch, take_second, 0)
    to_owner(1)

    def in_copy(f):
        return pltpu.make_async_copy(in16_s.at[f], in_o.at[0, :, aligned(f, fc), :], osem.at[0, f])

    def out_copy(f):
        return pltpu.make_async_copy(out16_s.at[f], out_o.at[0, aligned(f, fc), :], osem.at[1, f])

    def end_in(f, _):
        in16_s[f] = (hin_s[f] + in_term(0, 1, f)).astype(BF).reshape(2, fc, part)
        in_copy(f).start()
        return 0

    def end_out(f, _):
        out16_s[f] = (hout_s[f] + out_term(0, 0, f) + out_term(0, 1, f)).astype(BF)
        out_copy(f).start()
        return 0

    lax.fori_loop(0, 1, end_in, 0)
    pl.when(e == 1)(owner_sums)
    lax.fori_loop(1, nch, end_in, 0)
    pl.when(e == 1)(owner_shares)
    hidden_copy.wait_recv()
    lax.fori_loop(0, nch, end_out, 0)
    for c in second + third:
        c.wait_recv()
    tok_o[:, mine] = ready_s[0]
    tok_o[:, theirs] = ready_s[1]

    for c in first + cross + shared + passed + second + third + [hidden_copy, share_copy]:
        c.wait_send()
    for rep in range(2):
        core_copy(rep).wait_send()
        for c in slice_copies(rep):
            c.wait_send()

    def drain(f, _):
        for s in range(2):
            chunk_copy(s, f).wait_send()
            grads_copy(s, f).wait_send()
        in_copy(f).wait()
        out_copy(f).wait()
        return 0

    lax.fori_loop(0, nch, drain, 0)


def exchange(tokens, tangent, cotangent, ids, gates, w_in, v_in, w_out, v_out, cap, fc):
    n_tensor = lax.axis_size("tensor")
    rows, width = tokens.shape
    _, _, ff, part = w_in.shape
    topk = ids.shape[0]
    nch, few, peers = ff // fc, rows // n_tensor, n_tensor - 1
    dma = pltpu.SemaphoreType.DMA
    anyspace = pl.BlockSpec(memory_space=pl.ANY)
    vmem = pl.BlockSpec(memory_space=pltpu.VMEM)
    return pl.pallas_call(
        functools.partial(exchange_kernel, n_tensor, topk, cap, fc),
        name="exchange",
        out_shape=[
            jax.ShapeDtypeStruct((1, 2, ff, part), BF),
            jax.ShapeDtypeStruct((1, ff, part), BF),
            jax.ShapeDtypeStruct((rows, width), BF),
        ],
        in_specs=[anyspace] * 3 + [vmem] * 2 + [anyspace] * 4,
        out_specs=[anyspace] * 2 + [vmem],
        scratch_shapes=[
            pltpu.VMEM((nch, 2, fc, part), BF),
            pltpu.VMEM((nch, 2, fc, part), BF),
            pltpu.VMEM((nch, 2, fc, part), BF),
            pltpu.VMEM((2, 2, 3, rows, part), BF),
            pltpu.VMEM((2, 2, 2 * topk, rows), F32),
            pltpu.VMEM((2, 2, rows, rows), BF),
            pltpu.VMEM((2, 2, 3, cap, part), BF),
            pltpu.VMEM((2, nch, cap, 6 * fc), BF),
            pltpu.VMEM((2, nch, cap, 6 * fc), BF),
            pltpu.VMEM((2, 2, nch, 2 * cap, 2 * fc), BF),
            pltpu.VMEM((2, 2, nch, cap, fc), BF),
            pltpu.VMEM((2, 2, cap, part), F32),
            pltpu.VMEM((rows, part), F32),
            pltpu.VMEM((2, rows, part), BF),
            pltpu.VMEM((2, rows, part), BF),
            pltpu.VMEM((2, rows, part), BF),
            pltpu.VMEM((2, peers, few, part), BF),
            pltpu.VMEM((few, part), BF),
            pltpu.VMEM((2, rows, part), BF),
            pltpu.VMEM((nch, 2 * fc, part), F32),
            pltpu.VMEM((nch, fc, part), F32),
            pltpu.VMEM((nch, 2, fc, part), BF),
            pltpu.VMEM((nch, fc, part), BF),
            dma((4, nch)), dma((3,)), dma((2, nch)),
            dma((4,)), dma((4,)), dma((4,)), dma((4,)),
            dma((peers,)), dma((peers,)), dma((2,)), dma((2,)),
            dma((2, nch)), dma((2, nch)), dma((2, nch)), dma((2, nch)), dma, dma,
            dma((2,)), dma((2,)), dma((2, peers)), dma((2, peers)),
            dma((peers,)), dma((peers,)), dma, dma, dma((peers,)), dma((peers,)),
        ],
        compiler_params=pltpu.CompilerParams(
            collective_id=0, has_side_effects=True, vmem_limit_bytes=60 * 1024 * 1024
        ),
    )(tokens, tangent, cotangent, ids, gates, w_in, v_in, w_out, v_out)


def kernel_shards(tokens, tangent, cotangent, expert_ids, gates, w_in, v_in, w_out, v_out):
    rows, _ = tokens.shape
    topk = expert_ids.shape[1]
    all_experts = lax.axis_size("tensor") * lax.axis_size("expert")
    cap = min(rows, 3 * rows * topk // (2 * all_experts))
    hvp_in, hvp_out, out = exchange(
        tokens, tangent, cotangent, expert_ids.T, gates.T, w_in, v_in, w_out, v_out, cap, 128
    )
    return out.astype(F32), hvp_in.astype(F32), hvp_out.astype(F32)


def shards(*args):
    tokens, expert_ids, w_in = args[0], args[3], args[5]
    n_tensor = lax.axis_size("tensor")
    rows, topk = expert_ids.shape
    fits = (
        lax.axis_size("expert") == 2 and lax.axis_size("dp") == 2 and w_in.shape[0] == 1
        and tokens.shape[1] == 2 * w_in.shape[3] and w_in.shape[3] % 128 == 0 and w_in.shape[2] % 256 == 0
        and rows == 128 and n_tensor > 1 and rows % (16 * n_tensor) == 0
        and topk % 8 == 0 and (3 * rows * topk) % (64 * n_tensor) == 0
    )
    return (kernel_shards if fits else plain_shards)(*args)


def solution(mesh):
    rows = P(("expert", "dp"), None)
    wide = P(("tensor", "expert"), None, None, "dp")
    tall = P(("tensor", "expert"), None, "dp")
    return jax.shard_map(
        shards,
        mesh=mesh,
        in_specs=(rows, rows, rows, rows, rows, wide, wide, tall, tall),
        out_specs=(rows, wide, tall),
        check_vma=False,
    )
```

```python
import functools

import jax
import jax.numpy as jnp
from jax import lax
from jax.experimental import pallas as pl
from jax.experimental.pallas import tpu as pltpu
from jax.sharding import PartitionSpec as P


BF = jnp.bfloat16
F32 = jnp.float32
MESH = pl.DeviceIdType.MESH


def dot_nt(x, w):
    return lax.dot_general(x, w, (((1,), (1,)), ((), ())), preferred_element_type=F32)


def dot_nn(x, w):
    return lax.dot_general(x, w, (((1,), (0,)), ((), ())), preferred_element_type=F32)


def dot_tn(x, w):
    return lax.dot_general(x, w, (((0,), (0,)), ((), ())), preferred_element_type=F32)


def sum_over(own, axis, sent, ahead=None):
    n = lax.axis_size(axis)
    if n & (n - 1):
        return lax.psum(own.astype(BF), axis).astype(F32)
    step = 1
    while step < n:
        give = own.astype(BF)
        if step == 1:
            sent.append(give)
        got = lax.ppermute(give, axis, [(i, i ^ step) for i in range(n)])
        if ahead is not None:
            got, ahead = lax.optimization_barrier((got, ahead))
        own = own + got.astype(F32)
        step *= 2
    return own


def hidden_terms(pre, pre_dot, backs):
    half = pre.shape[1] // 2
    gate_pre, up_val = pre[:, :half], pre[:, half:]
    gate_dot, up_dot = pre_dot[:, :half], pre_dot[:, half:]
    back, back_dot = backs[:, :half], backs[:, half:]
    sigma = jax.nn.sigmoid(gate_pre)
    silu_val = gate_pre * sigma
    first = sigma * (1.0 + gate_pre * (1.0 - sigma))
    second = sigma * (1.0 - sigma) * (2.0 + gate_pre * (1.0 - 2.0 * sigma))
    grad_a = back * up_val * first
    grad_b = back * silu_val
    tang_a = back_dot * up_val * first + back * up_dot * first + back * up_val * second * gate_dot
    tang_b = back_dot * silu_val + back * first * gate_dot
    hidden_dot = first * gate_dot * up_val + silu_val * up_dot
    grads = jnp.concatenate([grad_a, grad_b], axis=1).astype(BF)
    tangs = jnp.concatenate([tang_a, tang_b], axis=1).astype(BF)
    return grads, tangs, hidden_dot.astype(BF)


def plain_shards(tokens, tangent, cotangent, expert_ids, gates, w_in, v_in, w_out, v_out):
    n_tensor = lax.axis_size("tensor")
    n_expert = lax.axis_size("expert")
    n_dp = lax.axis_size("dp")
    rank, core = lax.axis_index("tensor"), lax.axis_index("expert")
    held, _, ff, part = w_in.shape
    all_experts = held * n_tensor * n_expert
    rows, width = tokens.shape
    topk = expert_ids.shape[1]
    cap = min(rows, 3 * rows * topk // (2 * all_experts))

    around = [
        [((i + r) % n_expert, i) for i in range(n_expert)] for r in range(n_expert)
    ]

    def from_cores(v):
        return [v] + [lax.ppermute(v, "expert", around[r]) for r in range(1, n_expert)]

    fields = (tokens, tangent, cotangent)
    if n_dp == 2:
        low_half = [v[:, :part] for v in fields]
        high_half = [v[:, part:] for v in fields]
        first = lax.axis_index("dp") == 0
        give = jnp.where(first, jnp.concatenate(high_half, axis=1), jnp.concatenate(low_half, axis=1))
        keep = jnp.where(first, jnp.concatenate(low_half, axis=1), jnp.concatenate(high_half, axis=1))
        other = lax.ppermute(give, "dp", [(0, 1), (1, 0)])
        keeps, others = jnp.stack(from_cores(keep)), jnp.stack(from_cores(other))
        blocks = [jnp.where(first, keeps, others), jnp.where(first, others, keeps)]
    else:
        mine = lax.all_to_all(jnp.stack(fields, axis=1), "dp", split_axis=2, concat_axis=0, tiled=True)
        mine = mine.reshape(n_dp, rows, 3 * part)
        blocks = jnp.stack(from_cores(mine), axis=1)

    names = jnp.arange(all_experts, dtype=jnp.int32)
    hit = names[:, None, None] == expert_ids.T[None]
    table = jnp.sum(jnp.where(hit, gates.T[None], 0.0), axis=1)
    table = jnp.where(jnp.any(hit, axis=1), table, -1.0)
    tables = jnp.broadcast_to(table[None], (n_expert * n_dp, all_experts, rows))
    tables = lax.all_to_all(tables, ("expert", "dp"), split_axis=0, concat_axis=0, tiled=True)
    tables = tables.reshape(n_expert, n_dp, all_experts, rows)

    low = jnp.tril(jnp.ones((rows, rows), BF))
    weights = [
        (
            w_in[l].reshape(2 * ff, part),
            v_in[l].reshape(2 * ff, part),
            w_out[l],
            v_out[l],
        )
        for l in range(held)
    ]

    def replica(c, before=None):
        saved, spread, sent = [], [0.0] * n_expert, []
        block, ahead = blocks[c], None
        if before is not None:
            block, _ = lax.optimization_barrier((block, before[2]))
            ahead = before[0]
        for l in range(held):
            wi, vi, wo, vo = weights[l]
            expert = (rank * n_expert + core) * held + l
            picks, scales = [], []
            for r in range(n_expert):
                gate = tables[lax.rem(core + r, n_expert), c, expert]
                on = gate >= 0.0
                slot = dot_nt(on.astype(BF)[None, :], low)[0].astype(jnp.int32) - 1
                pick = (jnp.arange(cap, dtype=jnp.int32)[:, None] == slot[None, :]) & on[None, :]
                scales.append(jnp.sum(jnp.where(pick, gate[None, :], 0.0), axis=1))
                picks.append(pick.astype(BF))
            chosen = jnp.einsum(
                "rst,rtd->rsd", jnp.stack(picks), block, preferred_element_type=F32
            ).reshape(n_expert * cap, 3 * part)
            x = chosen[:, :part].astype(BF)
            u = chosen[:, part:2 * part].astype(BF)
            dy = (jnp.concatenate(scales)[:, None] * chosen[:, 2 * part:]).astype(BF)
            pre = sum_over(dot_nt(x, wi), "dp", sent)
            pre_dot = sum_over(dot_nt(u, wi) + dot_nt(x, vi), "dp", sent)
            backs = sum_over(jnp.concatenate([dot_nt(dy, wo), dot_nt(dy, vo)], axis=1), "dp", sent, ahead)
            grads, tangs, hidden = hidden_terms(pre, pre_dot, backs)
            saved.append((x, u, dy, grads, tangs, hidden))
            partial = (dot_nn(tangs, wi) + dot_nn(grads, vi)).astype(BF)
            for r, pick in enumerate(picks):
                spread[r] = spread[r] + dot_tn(pick, partial[r * cap:(r + 1) * cap])
        total = spread[0]
        for r in range(1, n_expert):
            moved = [(i, (i + r) % n_expert) for i in range(n_expert)]
            total = total + lax.ppermute(spread[r].astype(BF), "expert", moved).astype(F32)
        total = total.reshape(n_tensor, rows // n_tensor, part).astype(BF)
        got = lax.all_to_all(total, "tensor", split_axis=0, concat_axis=0, tiled=True)
        return jnp.sum(got.astype(F32), axis=0).astype(BF), saved, sent

    if n_dp <= 2:
        done = [replica(0)]
        for c in range(1, n_dp):
            done.append(replica(c, done[-1]))
        share, saved = jax.tree.map(lambda *v: jnp.stack(v), *[d[:2] for d in done])
    else:
        share, saved = lax.map(lambda c: replica(c)[:2], jnp.arange(n_dp))

    hvp_in, hvp_out = [], []
    for l in range(held):
        x, u, dy, grads, tangs, hidden = (v.reshape(-1, v.shape[-1]) for v in saved[l])
        both = jnp.concatenate([grads, tangs], axis=0)
        hvp_in.append(dot_tn(both, jnp.concatenate([u, x], axis=0)).reshape(2, ff, part))
        hvp_out.append(dot_tn(hidden, dy))

    share = jnp.broadcast_to(share[None], (n_tensor,) + share.shape)
    share = share.reshape((n_tensor * n_dp,) + share.shape[2:])
    share = lax.all_to_all(share, ("tensor", "dp"), split_axis=0, concat_axis=0, tiled=True)
    share = share.reshape(n_tensor, n_dp, rows // n_tensor, part).transpose(0, 2, 1, 3)
    hvp_tokens = share.reshape(rows, width).astype(F32)
    return hvp_tokens, jnp.stack(hvp_in), jnp.stack(hvp_out)


def remote(src, dst, send, recv, where):
    return pltpu.make_async_remote_copy(
        src_ref=src, dst_ref=dst, send_sem=send, recv_sem=recv, device_id=where, device_id_type=MESH
    )


def aligned(index, size):
    return pl.ds(pl.multiple_of(index * size, size), size)


def exchange_kernel(
    n_tensor, topk, cap, fc,
    tok_h, tan_h, cot_h, ids_h, gates_h, w_h, v_h, wo_h, vo_h,
    hin_o, hout_o, tok_o,
    w_s, v_s, o_s, tok_s, info_s, pick_s, rows_s, send_s, recv_s, fing_s, finh_s,
    part_s, own_s, give_s, core_s, sum_s, slice_s, share_s, ready_s, ids_s,
    wsem, lsem, c1s, c1r, c2s, c2r, c3s, c3r, c4s, c4r, c5s, c5r, c6s, c6r, c7s, c7r,
    as_, ar_, bs_, br_, cs_, cr_, ys_, yr_, zs_, zr_,
):
    t, e, p = lax.axis_index("tensor"), lax.axis_index("expert"), lax.axis_index("dp")
    q, other = 1 - p, 1 - e
    core, over = {"expert": other}, {"dp": q}
    rows, part = tok_s.shape[3], tok_s.shape[4]
    nch = w_s.shape[0]
    half = nch // 2
    few = rows // n_tensor
    mine, theirs = aligned(p, part), aligned(q, part)
    fields = (tan_h, tok_h, cot_h)
    plane = [{"tensor": lax.rem(t + k, n_tensor)} for k in range(1, n_tensor)]
    peers = [lax.rem(t + k, n_tensor) for k in range(1, n_tensor)]
    slice_t = aligned(t, few)

    barrier = pltpu.get_barrier_semaphore()
    for where in [core, over] + plane:
        pl.semaphore_signal(barrier, inc=1, device_id=where, device_id_type=MESH)

    local = [pltpu.make_async_copy(h.at[:, mine], tok_s.at[0, e, i], lsem.at[i]) for i, h in enumerate(fields)]
    local.append(pltpu.make_async_copy(ids_h, ids_s, lsem.at[3]))
    local.append(pltpu.make_async_copy(gates_h, info_s.at[0, e, pl.ds(topk, topk)], lsem.at[4]))
    for c in local:
        c.start()

    def weight_copies(f):
        part_f = aligned(f, fc)
        return [
            pltpu.make_async_copy(w_h.at[0, :, part_f, :], w_s.at[f], wsem.at[0, f]),
            pltpu.make_async_copy(v_h.at[0, :, part_f, :], v_s.at[f], wsem.at[1, f]),
            pltpu.make_async_copy(wo_h.at[0, part_f, :], o_s.at[f, 0], wsem.at[2, f]),
            pltpu.make_async_copy(vo_h.at[0, part_f, :], o_s.at[f, 1], wsem.at[3, f]),
        ]

    def load_weights(f, _):
        for c in weight_copies(f):
            c.start()
        return 0

    lax.fori_loop(0, nch, load_weights, 0)


    expert = (t * 2 + e).astype(F32)
    low = (
        lax.broadcasted_iota(jnp.int32, (rows, rows), 0) > lax.broadcasted_iota(jnp.int32, (rows, rows), 1)
    ).astype(F32).astype(BF)
    lane = lax.broadcasted_iota(jnp.int32, (rows, rows), 1).astype(F32)

    def gather(rep, s):
        info = info_s[rep, s].T
        hit = info[:, :topk] == expert
        on = jnp.sum(jnp.where(hit, 1.0, 0.0), axis=1, keepdims=True)
        gate = jnp.sum(jnp.where(hit, info[:, topk:], 0.0), axis=1, keepdims=True)
        on = jnp.broadcast_to(on, (rows, rows))
        slot = dot_nn(low, on.astype(BF))
        pick = jnp.where((slot == lane) & (on > 0.5), 1.0, 0.0)
        pick_s[rep, s] = pick.astype(BF)
        pick = pick.T.astype(BF)[:cap]
        rows_s[rep, s, 0] = dot_nn(pick, tok_s[rep, s, 0]).astype(BF)
        rows_s[rep, s, 1] = dot_nn(pick, tok_s[rep, s, 1]).astype(BF)
        scaled = (gate * tok_s[rep, s, 2].astype(F32)).astype(BF)
        rows_s[rep, s, 2] = dot_nn(pick, scaled).astype(BF)

    def products(rep, s, f):
        w = w_s[f].reshape(2 * fc, part)
        v = v_s[f].reshape(2 * fc, part)
        o = o_s[f].reshape(2 * fc, part)
        both = dot_nt(rows_s[rep, s, 0:2].reshape(2 * cap, part), w)
        return both[cap:], both[:cap] + dot_nt(rows_s[rep, s, 1], v), dot_nt(rows_s[rep, s, 2], o)

    def chunk_copy(s, f):
        return remote(send_s.at[s, f], recv_s.at[s, f], c5s.at[s, f], c5r.at[s, f], over)

    def make_chunk(s, f):
        pre, pre_dot, back = products(0, s, f)
        send_s[s, f, :, :2 * fc] = pre.astype(BF)
        send_s[s, f, :, 2 * fc:4 * fc] = pre_dot.astype(BF)
        send_s[s, f, :, 4 * fc:] = back.astype(BF)

    for c in local:
        c.wait()
    info_s[0, e, :topk, :] = ids_s[...].astype(F32)
    gather(0, e)
    for c in weight_copies(0):
        c.wait()
    make_chunk(e, 0)
    pl.semaphore_wait(barrier, 2 + len(plane))

    cross = [
        remote(h.at[slice_t, theirs], tok_s.at[1, e, i, slice_t], c2s.at[i], c2r.at[i], over)
        for i, h in enumerate(fields)
    ]
    cross.append(remote(info_s.at[0, e], info_s.at[1, e], c2s.at[3], c2r.at[3], over))
    first = [remote(h.at[:, mine], tok_s.at[0, e, i], c1s.at[i], c1r.at[i], core) for i, h in enumerate(fields)]
    first.append(remote(info_s.at[0, e], info_s.at[0, e], c1s.at[3], c1r.at[3], core))
    for c in cross + first:
        c.start()
    chunk_copy(e, 0).start()

    def send_own(f, _):
        for c in weight_copies(f):
            c.wait()
        make_chunk(e, f)
        chunk_copy(e, f).start()
        return 0

    lax.fori_loop(1, nch, send_own, 0)
    for c in first:
        c.wait_recv()
    gather(0, other)

    for c in cross:
        c.wait_recv()
    shared = [
        remote(tok_s.at[1, e, :, slice_t], tok_s.at[1, e, :, slice_t], c3s.at[k], c3r.at[k], where)
        for k, where in enumerate(plane)
    ]
    for c in shared:
        c.start()

    def send_other(f, _):
        make_chunk(other, f)
        chunk_copy(other, f).start()
        return 0

    lax.fori_loop(0, nch, send_other, 0)
    for c in shared:
        c.wait_recv()
    passed = [
        remote(tok_s.at[1, e], tok_s.at[1, e], c4s.at[0], c4r.at[0], core),
        remote(info_s.at[1, e], info_s.at[1, e], c4s.at[1], c4r.at[1], core),
    ]
    for c in passed:
        c.start()
    gather(1, e)
    for c in passed:
        c.wait_recv()
    gather(1, other)

    def back_rows(rep, s, f):
        w = w_s[f].reshape(2 * fc, part)
        v = v_s[f].reshape(2 * fc, part)
        g = fing_s[rep, s, f]
        return dot_nn(g[cap:], w) + dot_nn(g[:cap], v)

    def grads_copy(s, f):
        return remote(fing_s.at[1, s, f], fing_s.at[0, s, f], c6s.at[s, f], c6r.at[s, f], over)

    part_s[...] = jnp.zeros_like(part_s)

    def finish_chunk(i, _):
        s, f = lax.rem(e + i // nch, 2), lax.rem(i, nch)
        pre, pre_dot, back = products(1, s, f)
        chunk_copy(s, f).wait_recv()
        pre = pre + recv_s[s, f, :, :2 * fc].astype(F32)
        pre_dot = pre_dot + recv_s[s, f, :, 2 * fc:4 * fc].astype(F32)
        back = back + recv_s[s, f, :, 4 * fc:].astype(F32)
        grads, tangs, hidden = hidden_terms(pre, pre_dot, back)
        fing_s[1, s, f, :cap] = grads
        fing_s[1, s, f, cap:] = tangs
        finh_s[1, s, f] = hidden

        @pl.when(s == 0)
        def _():
            grads_copy(0, f).start()

        part_s[1, s] += back_rows(1, s, f)
        return 0

    lax.fori_loop(0, 2 * nch, finish_chunk, 0)

    def give_back(f, _):
        grads_copy(1, f).start()
        return 0

    lax.fori_loop(0, half, give_back, 0)

    def spread(rep, s):
        return dot_nn(pick_s[rep, s][:, :cap], part_s[rep, s].astype(BF))

    def core_copy(rep):
        return remote(give_s.at[rep], core_s.at[rep], as_.at[rep], ar_.at[rep], core)

    def slice_copies(rep):
        return [
            remote(sum_s.at[rep, aligned(peer, few)], slice_s.at[rep, k], bs_.at[rep, k], br_.at[rep, k], where)
            for k, (peer, where) in enumerate(zip(peers, plane))
        ]

    def over_cores(rep):
        core_copy(rep).wait_recv()
        sum_s[rep] = (own_s[...] + core_s[rep].astype(F32)).astype(BF)
        for c in slice_copies(rep):
            c.start()

    def over_plane(rep):
        for c in slice_copies(rep):
            c.wait_recv()
        total = sum_s[rep, slice_t].astype(F32)
        for k in range(n_tensor - 1):
            total = total + slice_s[rep, k].astype(F32)
        return total.astype(BF)

    def out_copies(side, sends, recvs):
        return [
            remote(ready_s.at[side, slice_t], ready_s.at[side, slice_t], sends.at[k], recvs.at[k], where)
            for k, where in enumerate(plane)
        ]

    def in_term(rep, s, f):
        return dot_tn(fing_s[rep, s, f], rows_s[rep, s, 0:2].reshape(2 * cap, part)).reshape(2, fc, part)

    def out_term(rep, s, f):
        return dot_tn(finh_s[rep, s, f], rows_s[rep, s, 2])

    def start_weights(f, _):
        part_f = aligned(f, fc)
        hin_o[0, :, part_f, :] = in_term(1, 0, f) + in_term(1, 1, f)
        hout_o[0, part_f, :] = out_term(1, 0, f) + out_term(1, 1, f)
        return 0

    give_s[1] = spread(1, other).astype(BF)
    core_copy(1).start()
    own_s[...] = spread(1, e)
    lax.fori_loop(0, half, start_weights, 0)
    over_cores(1)
    lax.fori_loop(half, nch, start_weights, 0)
    share_s[...] = over_plane(1)
    share_copy = remote(share_s, ready_s.at[1, slice_t], ys_, yr_, over)
    share_copy.start()
    lax.fori_loop(half, nch, give_back, 0)
    hidden = [remote(finh_s.at[1, s], finh_s.at[0, s], c7s.at[s], c7r.at[s], over) for s in range(2)]
    for c in hidden:
        c.start()

    def take_first(f, _):
        grads_copy(0, f).wait_recv()
        part_s[0, 0] += back_rows(0, 0, f)
        hin_o[0, :, aligned(f, fc), :] += in_term(0, 0, f)
        return 0

    def take_second(f, _):
        grads_copy(1, f).wait_recv()
        part_s[0, 1] += back_rows(0, 1, f)
        return 0

    def to_owner(s):
        @pl.when(e != s)
        def _():
            give_s[0] = spread(0, s).astype(BF)
            core_copy(0).start()

        @pl.when(e == s)
        def _():
            own_s[...] = spread(0, s)

    third = out_copies(0, cs_, cr_)

    def owner_sums():
        over_cores(0)

    def owner_shares():
        ready_s[0, slice_t] = over_plane(0)
        for c in third:
            c.start()

    lax.fori_loop(0, nch, take_first, 0)
    to_owner(0)
    pl.when(e == 0)(owner_sums)
    pl.when(e == 0)(owner_shares)
    share_copy.wait_recv()
    second = out_copies(1, zs_, zr_)
    for c in second:
        c.start()
    lax.fori_loop(0, nch, take_second, 0)
    to_owner(1)

    def end_in(f, _):
        hin_o[0, :, aligned(f, fc), :] += in_term(0, 1, f)
        return 0

    def end_out(s):
        def body(f, _):
            hout_o[0, aligned(f, fc), :] += out_term(0, s, f)
            return 0

        return body

    lax.fori_loop(0, 1, end_in, 0)
    pl.when(e == 1)(owner_sums)
    lax.fori_loop(1, nch, end_in, 0)
    pl.when(e == 1)(owner_shares)
    for s in range(2):
        hidden[s].wait_recv()
        lax.fori_loop(0, nch, end_out(s), 0)
    for c in second + third:
        c.wait_recv()
    tok_o[:, mine] = ready_s[0].astype(F32)
    tok_o[:, theirs] = ready_s[1].astype(F32)

    for c in first + cross + shared + passed + second + third + hidden + [share_copy]:
        c.wait_send()
    for rep in range(2):
        core_copy(rep).wait_send()
        for c in slice_copies(rep):
            c.wait_send()

    def drain(f, _):
        for s in range(2):
            chunk_copy(s, f).wait_send()
            grads_copy(s, f).wait_send()
        return 0

    lax.fori_loop(0, nch, drain, 0)


def exchange(args, cap, fc):
    tokens, ids, w_in = args[0], args[3], args[5]
    n_tensor = lax.axis_size("tensor")
    rows, width = tokens.shape
    _, _, ff, part = w_in.shape
    topk = ids.shape[0]
    nch, few, peers = ff // fc, rows // n_tensor, n_tensor - 1
    dma = pltpu.SemaphoreType.DMA
    hbm = pl.BlockSpec(memory_space=pltpu.HBM)
    vmem = pl.BlockSpec(memory_space=pltpu.VMEM)
    return pl.pallas_call(
        functools.partial(exchange_kernel, n_tensor, topk, cap, fc),
        name="exchange",
        out_shape=[
            pltpu.VMEM((1, 2, ff, part), F32),
            pltpu.VMEM((1, ff, part), F32),
            pltpu.VMEM((rows, width), F32),
        ],
        in_specs=[hbm] * 9,
        out_specs=[vmem] * 3,
        scratch_shapes=[
            pltpu.VMEM((nch, 2, fc, part), BF),
            pltpu.VMEM((nch, 2, fc, part), BF),
            pltpu.VMEM((nch, 2, fc, part), BF),
            pltpu.VMEM((2, 2, 3, rows, part), BF),
            pltpu.VMEM((2, 2, 2 * topk, rows), F32),
            pltpu.VMEM((2, 2, rows, rows), BF),
            pltpu.VMEM((2, 2, 3, cap, part), BF),
            pltpu.VMEM((2, nch, cap, 6 * fc), BF),
            pltpu.VMEM((2, nch, cap, 6 * fc), BF),
            pltpu.VMEM((2, 2, nch, 2 * cap, 2 * fc), BF),
            pltpu.VMEM((2, 2, nch, cap, fc), BF),
            pltpu.VMEM((2, 2, cap, part), F32),
            pltpu.VMEM((rows, part), F32),
            pltpu.VMEM((2, rows, part), BF),
            pltpu.VMEM((2, rows, part), BF),
            pltpu.VMEM((2, rows, part), BF),
            pltpu.VMEM((2, peers, few, part), BF),
            pltpu.VMEM((few, part), BF),
            pltpu.VMEM((2, rows, part), BF),
            pltpu.VMEM((topk, rows), jnp.int32),
            dma((4, nch)), dma((5,)),
            dma((4,)), dma((4,)), dma((4,)), dma((4,)),
            dma((peers,)), dma((peers,)), dma((2,)), dma((2,)),
            dma((2, nch)), dma((2, nch)), dma((2, nch)), dma((2, nch)), dma((2,)), dma((2,)),
            dma((2,)), dma((2,)), dma((2, peers)), dma((2, peers)),
            dma((peers,)), dma((peers,)), dma, dma, dma((peers,)), dma((peers,)),
        ],
        compiler_params=pltpu.CompilerParams(
            collective_id=0, has_side_effects=True, vmem_limit_bytes=44 * 1024 * 1024
        ),
    )(*[pltpu.with_memory_space_constraint(v, pltpu.HBM) for v in args])


def kernel_shards(tokens, tangent, cotangent, expert_ids, gates, w_in, v_in, w_out, v_out):
    rows, _ = tokens.shape
    topk = expert_ids.shape[1]
    all_experts = lax.axis_size("tensor") * lax.axis_size("expert")
    cap = min(rows, 3 * rows * topk // (2 * all_experts))
    args = (tokens, tangent, cotangent, expert_ids.T, gates.T, w_in, v_in, w_out, v_out)
    hvp_in, hvp_out, out = exchange(args, cap, 128)
    return out, hvp_in, hvp_out


def shards(*args):
    tokens, expert_ids, w_in = args[0], args[3], args[5]
    n_tensor = lax.axis_size("tensor")
    rows, topk = expert_ids.shape
    fits = (
        lax.axis_size("expert") == 2 and lax.axis_size("dp") == 2 and w_in.shape[0] == 1
        and tokens.shape[1] == 2 * w_in.shape[3] and w_in.shape[3] % 128 == 0 and w_in.shape[2] % 256 == 0
        and rows == 128 and n_tensor > 1 and rows % (16 * n_tensor) == 0
        and topk % 8 == 0 and (3 * rows * topk) % (64 * n_tensor) == 0
    )
    return (kernel_shards if fits else plain_shards)(*args)


def solution(mesh):
    rows = P(("expert", "dp"), None)
    wide = P(("tensor", "expert"), None, None, "dp")
    tall = P(("tensor", "expert"), None, "dp")
    return jax.shard_map(
        shards,
        mesh=mesh,
        in_specs=(rows, rows, rows, rows, rows, wide, wide, tall, tall),
        out_specs=(rows, wide, tall),
        check_vma=False,
    )
```

```python
import functools

import jax
import jax.numpy as jnp
from jax import lax
from jax.experimental import pallas as pl
from jax.experimental.pallas import tpu as pltpu
from jax.sharding import PartitionSpec as P


BF = jnp.bfloat16
F32 = jnp.float32
MESH = pl.DeviceIdType.MESH


def dot_nt(x, w):
    return lax.dot_general(x, w, (((1,), (1,)), ((), ())), preferred_element_type=F32)


def dot_nn(x, w):
    return lax.dot_general(x, w, (((1,), (0,)), ((), ())), preferred_element_type=F32)


def dot_tn(x, w):
    return lax.dot_general(x, w, (((0,), (0,)), ((), ())), preferred_element_type=F32)


def sum_over(own, axis, sent, ahead=None):
    n = lax.axis_size(axis)
    if n & (n - 1):
        return lax.psum(own.astype(BF), axis).astype(F32)
    step = 1
    while step < n:
        give = own.astype(BF)
        if step == 1:
            sent.append(give)
        got = lax.ppermute(give, axis, [(i, i ^ step) for i in range(n)])
        if ahead is not None:
            got, ahead = lax.optimization_barrier((got, ahead))
        own = own + got.astype(F32)
        step *= 2
    return own


def hidden_terms(pre, pre_dot, backs):
    half = pre.shape[1] // 2
    gate_pre, up_val = pre[:, :half], pre[:, half:]
    gate_dot, up_dot = pre_dot[:, :half], pre_dot[:, half:]
    back, back_dot = backs[:, :half], backs[:, half:]
    sigma = jax.nn.sigmoid(gate_pre)
    silu_val = gate_pre * sigma
    first = sigma * (1.0 + gate_pre * (1.0 - sigma))
    second = sigma * (1.0 - sigma) * (2.0 + gate_pre * (1.0 - 2.0 * sigma))
    grad_a = back * up_val * first
    grad_b = back * silu_val
    tang_a = back_dot * up_val * first + back * up_dot * first + back * up_val * second * gate_dot
    tang_b = back_dot * silu_val + back * first * gate_dot
    hidden_dot = first * gate_dot * up_val + silu_val * up_dot
    grads = jnp.concatenate([grad_a, grad_b], axis=1).astype(BF)
    tangs = jnp.concatenate([tang_a, tang_b], axis=1).astype(BF)
    return grads, tangs, hidden_dot.astype(BF)


def plain_shards(tokens, tangent, cotangent, expert_ids, gates, w_in, v_in, w_out, v_out):
    n_tensor = lax.axis_size("tensor")
    n_expert = lax.axis_size("expert")
    n_dp = lax.axis_size("dp")
    rank, core = lax.axis_index("tensor"), lax.axis_index("expert")
    held, _, ff, part = w_in.shape
    all_experts = held * n_tensor * n_expert
    rows, width = tokens.shape
    topk = expert_ids.shape[1]
    cap = min(rows, 3 * rows * topk // (2 * all_experts))

    around = [
        [((i + r) % n_expert, i) for i in range(n_expert)] for r in range(n_expert)
    ]

    def from_cores(v):
        return [v] + [lax.ppermute(v, "expert", around[r]) for r in range(1, n_expert)]

    fields = (tokens, tangent, cotangent)
    if n_dp == 2:
        low_half = [v[:, :part] for v in fields]
        high_half = [v[:, part:] for v in fields]
        first = lax.axis_index("dp") == 0
        give = jnp.where(first, jnp.concatenate(high_half, axis=1), jnp.concatenate(low_half, axis=1))
        keep = jnp.where(first, jnp.concatenate(low_half, axis=1), jnp.concatenate(high_half, axis=1))
        other = lax.ppermute(give, "dp", [(0, 1), (1, 0)])
        keeps, others = jnp.stack(from_cores(keep)), jnp.stack(from_cores(other))
        blocks = [jnp.where(first, keeps, others), jnp.where(first, others, keeps)]
    else:
        mine = lax.all_to_all(jnp.stack(fields, axis=1), "dp", split_axis=2, concat_axis=0, tiled=True)
        mine = mine.reshape(n_dp, rows, 3 * part)
        blocks = jnp.stack(from_cores(mine), axis=1)

    names = jnp.arange(all_experts, dtype=jnp.int32)
    hit = names[:, None, None] == expert_ids.T[None]
    table = jnp.sum(jnp.where(hit, gates.T[None], 0.0), axis=1)
    table = jnp.where(jnp.any(hit, axis=1), table, -1.0)
    tables = jnp.broadcast_to(table[None], (n_expert * n_dp, all_experts, rows))
    tables = lax.all_to_all(tables, ("expert", "dp"), split_axis=0, concat_axis=0, tiled=True)
    tables = tables.reshape(n_expert, n_dp, all_experts, rows)

    low = jnp.tril(jnp.ones((rows, rows), BF))
    weights = [
        (
            w_in[l].reshape(2 * ff, part),
            v_in[l].reshape(2 * ff, part),
            w_out[l],
            v_out[l],
        )
        for l in range(held)
    ]

    def replica(c, before=None):
        saved, spread, sent = [], [0.0] * n_expert, []
        block, ahead = blocks[c], None
        if before is not None:
            block, _ = lax.optimization_barrier((block, before[2]))
            ahead = before[0]
        for l in range(held):
            wi, vi, wo, vo = weights[l]
            expert = (rank * n_expert + core) * held + l
            picks, scales = [], []
            for r in range(n_expert):
                gate = tables[lax.rem(core + r, n_expert), c, expert]
                on = gate >= 0.0
                slot = dot_nt(on.astype(BF)[None, :], low)[0].astype(jnp.int32) - 1
                pick = (jnp.arange(cap, dtype=jnp.int32)[:, None] == slot[None, :]) & on[None, :]
                scales.append(jnp.sum(jnp.where(pick, gate[None, :], 0.0), axis=1))
                picks.append(pick.astype(BF))
            chosen = jnp.einsum(
                "rst,rtd->rsd", jnp.stack(picks), block, preferred_element_type=F32
            ).reshape(n_expert * cap, 3 * part)
            x = chosen[:, :part].astype(BF)
            u = chosen[:, part:2 * part].astype(BF)
            dy = (jnp.concatenate(scales)[:, None] * chosen[:, 2 * part:]).astype(BF)
            pre = sum_over(dot_nt(x, wi), "dp", sent)
            pre_dot = sum_over(dot_nt(u, wi) + dot_nt(x, vi), "dp", sent)
            backs = sum_over(jnp.concatenate([dot_nt(dy, wo), dot_nt(dy, vo)], axis=1), "dp", sent, ahead)
            grads, tangs, hidden = hidden_terms(pre, pre_dot, backs)
            saved.append((x, u, dy, grads, tangs, hidden))
            partial = (dot_nn(tangs, wi) + dot_nn(grads, vi)).astype(BF)
            for r, pick in enumerate(picks):
                spread[r] = spread[r] + dot_tn(pick, partial[r * cap:(r + 1) * cap])
        total = spread[0]
        for r in range(1, n_expert):
            moved = [(i, (i + r) % n_expert) for i in range(n_expert)]
            total = total + lax.ppermute(spread[r].astype(BF), "expert", moved).astype(F32)
        total = total.reshape(n_tensor, rows // n_tensor, part).astype(BF)
        got = lax.all_to_all(total, "tensor", split_axis=0, concat_axis=0, tiled=True)
        return jnp.sum(got.astype(F32), axis=0).astype(BF), saved, sent

    if n_dp <= 2:
        done = [replica(0)]
        for c in range(1, n_dp):
            done.append(replica(c, done[-1]))
        share, saved = jax.tree.map(lambda *v: jnp.stack(v), *[d[:2] for d in done])
    else:
        share, saved = lax.map(lambda c: replica(c)[:2], jnp.arange(n_dp))

    hvp_in, hvp_out = [], []
    for l in range(held):
        x, u, dy, grads, tangs, hidden = (v.reshape(-1, v.shape[-1]) for v in saved[l])
        both = jnp.concatenate([grads, tangs], axis=0)
        hvp_in.append(dot_tn(both, jnp.concatenate([u, x], axis=0)).reshape(2, ff, part))
        hvp_out.append(dot_tn(hidden, dy))

    share = jnp.broadcast_to(share[None], (n_tensor,) + share.shape)
    share = share.reshape((n_tensor * n_dp,) + share.shape[2:])
    share = lax.all_to_all(share, ("tensor", "dp"), split_axis=0, concat_axis=0, tiled=True)
    share = share.reshape(n_tensor, n_dp, rows // n_tensor, part).transpose(0, 2, 1, 3)
    hvp_tokens = share.reshape(rows, width).astype(F32)
    return hvp_tokens, jnp.stack(hvp_in), jnp.stack(hvp_out)


def remote(src, dst, send, recv, where):
    return pltpu.make_async_remote_copy(
        src_ref=src, dst_ref=dst, send_sem=send, recv_sem=recv, device_id=where, device_id_type=MESH
    )


def aligned(index, size):
    return pl.ds(pl.multiple_of(index * size, size), size)


def exchange_kernel(
    n_tensor, topk, cap, fc,
    tok_h, tan_h, cot_h, ids_h, gates_h, w_h, v_h, wo_h, vo_h,
    hin_o, hout_o, tok_o,
    wvo_s, tok_s, info_s, pick_s, rows_s, send_s, recv_s, fing_s, finh_s,
    part_s, own_s, give_s, core_s, sum_s, slice_s, share_s, ready_s, ids_s,
    wsem, lsem, c1s, c1r, c2s, c2r, c3s, c3r, c4s, c4r, c5s, c5r, c6s, c6r, c7s, c7r,
    as_, ar_, bs_, br_, cs_, cr_, ys_, yr_, zs_, zr_,
):
    t, e, p = lax.axis_index("tensor"), lax.axis_index("expert"), lax.axis_index("dp")
    q, other = 1 - p, 1 - e
    core, over = {"expert": other}, {"dp": q}
    rows, part = tok_s.shape[3], tok_s.shape[4]
    nch, parts = wvo_s.shape[0], own_s.shape[0]
    half = nch // 2
    few = rows // n_tensor
    mine, theirs = aligned(p, part), aligned(q, part)
    fields = (tan_h, tok_h, cot_h)
    plane = [{"tensor": lax.rem(t + k, n_tensor)} for k in range(1, n_tensor)]
    peers = [lax.rem(t + k, n_tensor) for k in range(1, n_tensor)]
    slice_t = aligned(t, few)

    barrier = pltpu.get_barrier_semaphore()
    for where in [core, over] + plane:
        pl.semaphore_signal(barrier, inc=1, device_id=where, device_id_type=MESH)

    local = [pltpu.make_async_copy(h.at[:, mine], tok_s.at[0, e, i], lsem.at[0]) for i, h in enumerate(fields)]
    local.append(pltpu.make_async_copy(ids_h, ids_s, lsem.at[1]))
    local.append(pltpu.make_async_copy(gates_h, info_s.at[0, e, pl.ds(topk, topk)], lsem.at[2]))
    for c in local:
        c.start()

    def load_weights(f, _):
        part_f = aligned(f, fc)
        pltpu.make_async_copy(w_h.at[0, :, part_f, :], wvo_s.at[f, 0], wsem.at[f]).start()
        pltpu.make_async_copy(v_h.at[0, :, part_f, :], wvo_s.at[f, 1], wsem.at[f]).start()
        pltpu.make_async_copy(wo_h.at[0, part_f, :], wvo_s.at[f, 2, 0], wsem.at[f]).start()
        pltpu.make_async_copy(vo_h.at[0, part_f, :], wvo_s.at[f, 2, 1], wsem.at[f]).start()
        return 0

    def wait_weights(f):
        pltpu.make_async_copy(wvo_s.at[f], wvo_s.at[f], wsem.at[f]).wait()

    lax.fori_loop(0, nch, load_weights, 0)


    expert = (t * 2 + e).astype(F32)
    low = (
        lax.broadcasted_iota(jnp.int32, (rows, rows), 0) > lax.broadcasted_iota(jnp.int32, (rows, rows), 1)
    ).astype(F32).astype(BF)
    lane = lax.broadcasted_iota(jnp.int32, (rows, rows), 1).astype(F32)

    def gather(rep, s):
        info = info_s[rep, s].T
        hit = info[:, :topk] == expert
        on = jnp.sum(jnp.where(hit, 1.0, 0.0), axis=1, keepdims=True)
        gate = jnp.sum(jnp.where(hit, info[:, topk:], 0.0), axis=1, keepdims=True)
        on = jnp.broadcast_to(on, (rows, rows))
        slot = dot_nn(low, on.astype(BF))
        pick = jnp.where((slot == lane) & (on > 0.5), 1.0, 0.0)
        pick_s[rep, s] = pick.astype(BF)
        pick = pick.T.astype(BF)[:cap]
        rows_s[rep, s, 0] = dot_nn(pick, tok_s[rep, s, 0]).astype(BF)
        rows_s[rep, s, 1] = dot_nn(pick, tok_s[rep, s, 1]).astype(BF)
        scaled = (gate * tok_s[rep, s, 2].astype(F32)).astype(BF)
        rows_s[rep, s, 2] = dot_nn(pick, scaled).astype(BF)

    def products(rep, s, f):
        w = wvo_s[f, 0].reshape(2 * fc, part)
        v = wvo_s[f, 1].reshape(2 * fc, part)
        o = wvo_s[f, 2].reshape(2 * fc, part)
        both = dot_nt(rows_s[rep, s, 0:2].reshape(2 * cap, part), w)
        return both[cap:], both[:cap] + dot_nt(rows_s[rep, s, 1], v), dot_nt(rows_s[rep, s, 2], o)

    def chunk_copy(s, f):
        return remote(send_s.at[s, f], recv_s.at[s, f], c5s, c5r.at[s, f], over)

    def make_chunk(s, f):
        pre, pre_dot, back = products(0, s, f)
        send_s[s, f, :, :2 * fc] = pre.astype(BF)
        send_s[s, f, :, 2 * fc:4 * fc] = pre_dot.astype(BF)
        send_s[s, f, :, 4 * fc:] = back.astype(BF)

    pltpu.make_async_copy(tok_s.at[0, e], tok_s.at[0, e], lsem.at[0]).wait()
    for c in local[3:]:
        c.wait()
    info_s[0, e, :topk, :] = ids_s[...].astype(F32)
    gather(0, e)
    wait_weights(0)
    make_chunk(e, 0)
    pl.semaphore_wait(barrier, 2 + len(plane))

    cross = [
        remote(h.at[slice_t, theirs], tok_s.at[1, e, i, slice_t], c2s.at[0], c2r.at[0], over)
        for i, h in enumerate(fields)
    ]
    cross.append(remote(info_s.at[0, e], info_s.at[1, e], c2s.at[1], c2r.at[1], over))
    first = [remote(h.at[:, mine], tok_s.at[0, e, i], c1s.at[0], c1r.at[0], core) for i, h in enumerate(fields)]
    first.append(remote(info_s.at[0, e], info_s.at[0, e], c1s.at[1], c1r.at[1], core))
    for c in cross + first:
        c.start()
    chunk_copy(e, 0).start()

    def send_own(f, _):
        wait_weights(f)
        make_chunk(e, f)
        chunk_copy(e, f).start()
        return 0

    lax.fori_loop(1, nch, send_own, 0)
    firsts = [remote(tok_s.at[0, other], tok_s.at[0, other], c1s.at[0], c1r.at[0], core), first[3]]
    for c in firsts:
        c.wait_recv()
    gather(0, other)

    tok_slice = tok_s.at[1, e, :, slice_t]
    crosses = [remote(tok_slice, tok_slice, c2s.at[0], c2r.at[0], over), cross[3]]
    for c in crosses:
        c.wait_recv()
    shared = [
        remote(tok_slice, tok_slice, c3s, c3r, where) for where in plane
    ]
    for c in shared:
        c.start()

    def send_other(f, _):
        make_chunk(other, f)
        chunk_copy(other, f).start()
        return 0

    lax.fori_loop(0, nch, send_other, 0)
    most = pl.ds(0, rows - few)
    tok_most = tok_s.at[1, e, :, most]
    shareds = remote(tok_most, tok_most, c3s, c3r, core)
    shareds.wait_recv()
    passed = [
        remote(tok_s.at[1, e], tok_s.at[1, e], c4s.at[0], c4r.at[0], core),
        remote(info_s.at[1, e], info_s.at[1, e], c4s.at[1], c4r.at[1], core),
    ]
    for c in passed:
        c.start()
    gather(1, e)
    for c in passed:
        c.wait_recv()
    gather(1, other)

    def back_rows(rep, s, f):
        w = wvo_s[f, 0].reshape(2 * fc, part)
        v = wvo_s[f, 1].reshape(2 * fc, part)
        g = fing_s[rep, s, f]
        return dot_nn(g[cap:], w) + dot_nn(g[:cap], v)

    def grads_copy(s, f):
        return remote(fing_s.at[1, s, f], fing_s.at[0, s, f], c6s, c6r.at[s, f], over)

    part_s[...] = jnp.zeros_like(part_s)

    def finish_chunk(i, _):
        s, f = lax.rem(e + i // nch, 2), lax.rem(i, nch)
        pre, pre_dot, back = products(1, s, f)
        chunk_copy(s, f).wait_recv()
        pre = pre + recv_s[s, f, :, :2 * fc].astype(F32)
        pre_dot = pre_dot + recv_s[s, f, :, 2 * fc:4 * fc].astype(F32)
        back = back + recv_s[s, f, :, 4 * fc:].astype(F32)
        grads, tangs, hidden = hidden_terms(pre, pre_dot, back)
        fing_s[1, s, f, :cap] = grads
        fing_s[1, s, f, cap:] = tangs
        finh_s[1, s, f] = hidden

        @pl.when(s == 0)
        def _():
            grads_copy(0, f).start()

        part_s[1, s] += back_rows(1, s, f)
        return 0

    lax.fori_loop(0, 2 * nch, finish_chunk, 0)

    def give_back(f, _):
        grads_copy(1, f).start()
        return 0

    lax.fori_loop(0, half, give_back, 0)

    def spread(rep, s, h):
        pc = part // parts
        return dot_nn(pick_s[rep, s][:, :cap], part_s[rep, s, :, h * pc:(h + 1) * pc].astype(BF))

    def core_copy(rep, h):
        return remote(give_s.at[rep, h], core_s.at[rep, h], as_.at[rep, h], ar_.at[rep, h], core)

    def give_core(rep, s):
        for h in range(parts):
            give_s[rep, h] = spread(rep, s, h).astype(BF)
            core_copy(rep, h).start()

    def keep_own(rep, s):
        for h in range(parts):
            own_s[h] = spread(rep, s, h)

    def over_cores(rep):
        for h in range(parts):
            core_copy(rep, h).wait_recv()
            sum_s[rep, h] = (own_s[h] + core_s[rep, h].astype(F32)).astype(BF)
            for k, (peer, where) in enumerate(zip(peers, plane)):
                remote(
                    sum_s.at[rep, h, aligned(peer, few)], slice_s.at[rep, h, k], bs_.at[rep], br_.at[rep, h], where
                ).start()

    def over_plane(rep, h):
        remote(slice_s.at[rep, h], slice_s.at[rep, h], bs_.at[rep], br_.at[rep, h], core).wait_recv()
        total = sum_s[rep, h, slice_t].astype(F32)
        for k in range(n_tensor - 1):
            total = total + slice_s[rep, h, k].astype(F32)
        return total.astype(BF)

    def in_term(rep, s, f):
        return dot_tn(fing_s[rep, s, f], rows_s[rep, s, 0:2].reshape(2 * cap, part)).reshape(2, fc, part)

    def out_term(rep, s, f):
        return dot_tn(finh_s[rep, s, f], rows_s[rep, s, 2])

    def start_weights(f, _):
        part_f = aligned(f, fc)
        hin_o[0, :, part_f, :] = in_term(1, 0, f) + in_term(1, 1, f)
        hout_o[0, part_f, :] = out_term(1, 0, f) + out_term(1, 1, f)
        return 0

    give_core(1, other)
    keep_own(1, e)
    lax.fori_loop(0, half, start_weights, 0)
    over_cores(1)
    lax.fori_loop(half, nch, start_weights, 0)
    for h in range(parts):
        share_s[h] = over_plane(1, h)
    share_copy = remote(share_s, ready_s.at[1, :, slice_t], ys_, yr_, over)
    share_copy.start()
    lax.fori_loop(half, nch, give_back, 0)
    hidden = [remote(finh_s.at[1, s], finh_s.at[0, s], c7s, c7r.at[s], over) for s in range(2)]
    for c in hidden:
        c.start()

    def take_first(f, _):
        grads_copy(0, f).wait_recv()
        part_s[0, 0] += back_rows(0, 0, f)
        hin_o[0, :, aligned(f, fc), :] += in_term(0, 0, f)
        return 0

    def take_second(f, _):
        grads_copy(1, f).wait_recv()
        part_s[0, 1] += back_rows(0, 1, f)
        return 0

    def to_owner(s):
        @pl.when(e != s)
        def _():
            give_core(0, s)

        @pl.when(e == s)
        def _():
            keep_own(0, s)

    def owner_sums():
        over_cores(0)

    def owner_shares():
        for h in range(parts):
            ready_s[0, h, slice_t] = over_plane(0, h)
            for where in plane:
                mid = ready_s.at[0, h, slice_t]
                remote(mid, mid, cs_, cr_, where).start()

    lax.fori_loop(0, nch, take_first, 0)
    to_owner(0)
    pl.when(e == 0)(owner_sums)
    pl.when(e == 0)(owner_shares)
    share_copy.wait_recv()
    for where in plane:
        mid = ready_s.at[1, :, slice_t]
        remote(mid, mid, zs_, zr_, where).start()
    lax.fori_loop(0, nch, take_second, 0)
    to_owner(1)

    def end_in(f, _):
        hin_o[0, :, aligned(f, fc), :] += in_term(0, 1, f)
        return 0

    def end_out(s):
        def body(f, _):
            hout_o[0, aligned(f, fc), :] += out_term(0, s, f)
            return 0

        return body

    lax.fori_loop(0, 1, end_in, 0)
    pl.when(e == 1)(owner_sums)
    lax.fori_loop(1, nch, end_in, 0)
    pl.when(e == 1)(owner_shares)
    for s in range(2):
        hidden[s].wait_recv()
        lax.fori_loop(0, nch, end_out(s), 0)
    plane_out = [
        remote(ready_s.at[1, :, most], ready_s.at[1, :, most], zs_, zr_, core),
        remote(ready_s.at[0, :, most], ready_s.at[0, :, most], cs_, cr_, core),
    ]
    for c in plane_out:
        c.wait_recv()
    for h in range(parts):
        pc = part // parts
        tok_o[:, pl.ds(pl.multiple_of(p * part + h * pc, pc), pc)] = ready_s[0, h].astype(F32)
        tok_o[:, pl.ds(pl.multiple_of(q * part + h * pc, pc), pc)] = ready_s[1, h].astype(F32)

    for c in firsts + crosses + [shareds] + passed + plane_out + [share_copy]:
        c.wait_send()
    for r in range(2):
        for h in range(parts):
            core_copy(r, h).wait_send()
        remote(slice_s.at[r], slice_s.at[r], bs_.at[r], br_.at[r, 0], core).wait_send()
    remote(send_s, send_s, c5s, c5r.at[0, 0], over).wait_send()
    remote(fing_s.at[1], fing_s.at[1], c6s, c6r.at[0, 0], over).wait_send()
    remote(finh_s.at[1], finh_s.at[1], c7s, c7r.at[0], over).wait_send()


def exchange(args, cap, fc):
    tokens, ids, w_in = args[0], args[3], args[5]
    n_tensor = lax.axis_size("tensor")
    rows, width = tokens.shape
    _, _, ff, part = w_in.shape
    topk = ids.shape[0]
    nch, few, peers = ff // fc, rows // n_tensor, n_tensor - 1
    parts = 2
    pc = part // parts
    dma = pltpu.SemaphoreType.DMA
    hbm = pl.BlockSpec(memory_space=pltpu.HBM)
    vmem = pl.BlockSpec(memory_space=pltpu.VMEM)
    return pl.pallas_call(
        functools.partial(exchange_kernel, n_tensor, topk, cap, fc),
        name="exchange",
        out_shape=[
            pltpu.VMEM((1, 2, ff, part), F32),
            pltpu.VMEM((1, ff, part), F32),
            pltpu.VMEM((rows, width), F32),
        ],
        in_specs=[hbm] * 9,
        out_specs=[vmem] * 3,
        scratch_shapes=[
            pltpu.VMEM((nch, 3, 2, fc, part), BF),
            pltpu.VMEM((2, 2, 3, rows, part), BF),
            pltpu.VMEM((2, 2, 2 * topk, rows), F32),
            pltpu.VMEM((2, 2, rows, rows), BF),
            pltpu.VMEM((2, 2, 3, cap, part), BF),
            pltpu.VMEM((2, nch, cap, 6 * fc), BF),
            pltpu.VMEM((2, nch, cap, 6 * fc), BF),
            pltpu.VMEM((2, 2, nch, 2 * cap, 2 * fc), BF),
            pltpu.VMEM((2, 2, nch, cap, fc), BF),
            pltpu.VMEM((2, 2, cap, part), F32),
            pltpu.VMEM((parts, rows, pc), F32),
            pltpu.VMEM((2, parts, rows, pc), BF),
            pltpu.VMEM((2, parts, rows, pc), BF),
            pltpu.VMEM((2, parts, rows, pc), BF),
            pltpu.VMEM((2, parts, peers, few, pc), BF),
            pltpu.VMEM((parts, few, pc), BF),
            pltpu.VMEM((2, parts, rows, pc), BF),
            pltpu.VMEM((topk, rows), jnp.int32),
            dma((nch,)), dma((3,)),
            dma((2,)), dma((2,)), dma((2,)), dma((2,)), dma, dma, dma((2,)), dma((2,)),
            dma, dma((2, nch)), dma, dma((2, nch)), dma, dma((2,)),
            dma((2, parts)), dma((2, parts)), dma((2,)), dma((2, parts)),
            dma, dma, dma, dma, dma, dma,
        ],
        compiler_params=pltpu.CompilerParams(
            collective_id=0, has_side_effects=True, vmem_limit_bytes=44 * 1024 * 1024
        ),
    )(*[pltpu.with_memory_space_constraint(v, pltpu.HBM) for v in args])


def store_kernel(hin_v, hout_v, tok_v, hin_o, hout_o, tok_o, sem):
    ff = hin_v.shape[2]
    step = ff // 3
    copies = []
    for i in range(3):
        span = pl.ds(i * step, step)
        copies += [(hin_v.at[0, g, span], hin_o.at[0, g, span]) for g in range(2)]
        copies.append((hout_v.at[0, span], hout_o.at[0, span]))
    copies.append((tok_v, tok_o))
    copies = [pltpu.make_async_copy(src, dst, sem.at[i]) for i, (src, dst) in enumerate(copies)]
    for c in copies:
        c.start()
    for c in copies:
        c.wait()


def store(*results):
    return pl.pallas_call(
        store_kernel,
        name="store",
        out_shape=[pltpu.HBM(v.shape, v.dtype) for v in results],
        in_specs=[pl.BlockSpec(memory_space=pltpu.VMEM)] * 3,
        out_specs=[pl.BlockSpec(memory_space=pltpu.HBM)] * 3,
        scratch_shapes=[pltpu.SemaphoreType.DMA((10,))],
        compiler_params=pltpu.CompilerParams(vmem_limit_bytes=4 * 1024 * 1024),
    )(*[pltpu.with_memory_space_constraint(v, pltpu.VMEM) for v in results])


def kernel_shards(tokens, tangent, cotangent, expert_ids, gates, w_in, v_in, w_out, v_out):
    rows, _ = tokens.shape
    topk = expert_ids.shape[1]
    all_experts = lax.axis_size("tensor") * lax.axis_size("expert")
    cap = min(rows, 3 * rows * topk // (2 * all_experts))
    args = (tokens, tangent, cotangent, expert_ids.T, gates.T, w_in, v_in, w_out, v_out)
    hvp_in, hvp_out, out = exchange(args, cap, 128)
    hvp_in, hvp_out, out = store(hvp_in, hvp_out, out)
    return out, hvp_in, hvp_out


def shards(*args):
    tokens, expert_ids, w_in = args[0], args[3], args[5]
    n_tensor = lax.axis_size("tensor")
    rows, topk = expert_ids.shape
    fits = (
        lax.axis_size("expert") == 2 and lax.axis_size("dp") == 2 and w_in.shape[0] == 1
        and tokens.shape[1] == 2 * w_in.shape[3] and w_in.shape[3] % 128 == 0 and w_in.shape[2] % 256 == 0
        and rows == 128 and n_tensor > 1 and rows % (16 * n_tensor) == 0
        and topk % 8 == 0 and (3 * rows * topk) % (64 * n_tensor) == 0
    )
    return (kernel_shards if fits else plain_shards)(*args)


def solution(mesh):
    rows = P(("expert", "dp"), None)
    wide = P(("tensor", "expert"), None, None, "dp")
    tall = P(("tensor", "expert"), None, "dp")
    return jax.shard_map(
        shards,
        mesh=mesh,
        in_specs=(rows, rows, rows, rows, rows, wide, wide, tall, tall),
        out_specs=(rows, wide, tall),
        check_vma=False,
    )
```

```python
import functools

import jax
import jax.numpy as jnp
from jax import lax
from jax.experimental import pallas as pl
from jax.experimental.pallas import tpu as pltpu
from jax.sharding import PartitionSpec as P


BF = jnp.bfloat16
F32 = jnp.float32
MESH = pl.DeviceIdType.MESH


def dot_nt(x, w):
    return lax.dot_general(x, w, (((1,), (1,)), ((), ())), preferred_element_type=F32)


def dot_nn(x, w):
    return lax.dot_general(x, w, (((1,), (0,)), ((), ())), preferred_element_type=F32)


def dot_tn(x, w):
    return lax.dot_general(x, w, (((0,), (0,)), ((), ())), preferred_element_type=F32)


def sum_over(own, axis, sent, ahead=None):
    n = lax.axis_size(axis)
    if n & (n - 1):
        return lax.psum(own.astype(BF), axis).astype(F32)
    step = 1
    while step < n:
        give = own.astype(BF)
        if step == 1:
            sent.append(give)
        got = lax.ppermute(give, axis, [(i, i ^ step) for i in range(n)])
        if ahead is not None:
            got, ahead = lax.optimization_barrier((got, ahead))
        own = own + got.astype(F32)
        step *= 2
    return own


def hidden_terms(pre, pre_dot, backs):
    half = pre.shape[1] // 2
    gate_pre, up_val = pre[:, :half], pre[:, half:]
    gate_dot, up_dot = pre_dot[:, :half], pre_dot[:, half:]
    back, back_dot = backs[:, :half], backs[:, half:]
    sigma = jax.nn.sigmoid(gate_pre)
    silu_val = gate_pre * sigma
    first = sigma * (1.0 + gate_pre * (1.0 - sigma))
    second = sigma * (1.0 - sigma) * (2.0 + gate_pre * (1.0 - 2.0 * sigma))
    grad_a = back * up_val * first
    grad_b = back * silu_val
    tang_a = back_dot * up_val * first + back * up_dot * first + back * up_val * second * gate_dot
    tang_b = back_dot * silu_val + back * first * gate_dot
    hidden_dot = first * gate_dot * up_val + silu_val * up_dot
    grads = jnp.concatenate([grad_a, grad_b], axis=1).astype(BF)
    tangs = jnp.concatenate([tang_a, tang_b], axis=1).astype(BF)
    return grads, tangs, hidden_dot.astype(BF)


def plain_shards(tokens, tangent, cotangent, expert_ids, gates, w_in, v_in, w_out, v_out):
    n_tensor = lax.axis_size("tensor")
    n_expert = lax.axis_size("expert")
    n_dp = lax.axis_size("dp")
    rank, core = lax.axis_index("tensor"), lax.axis_index("expert")
    held, _, ff, part = w_in.shape
    all_experts = held * n_tensor * n_expert
    rows, width = tokens.shape
    topk = expert_ids.shape[1]
    cap = min(rows, 3 * rows * topk // (2 * all_experts))

    around = [
        [((i + r) % n_expert, i) for i in range(n_expert)] for r in range(n_expert)
    ]

    def from_cores(v):
        return [v] + [lax.ppermute(v, "expert", around[r]) for r in range(1, n_expert)]

    fields = (tokens, tangent, cotangent)
    if n_dp == 2:
        low_half = [v[:, :part] for v in fields]
        high_half = [v[:, part:] for v in fields]
        first = lax.axis_index("dp") == 0
        give = jnp.where(first, jnp.concatenate(high_half, axis=1), jnp.concatenate(low_half, axis=1))
        keep = jnp.where(first, jnp.concatenate(low_half, axis=1), jnp.concatenate(high_half, axis=1))
        other = lax.ppermute(give, "dp", [(0, 1), (1, 0)])
        keeps, others = jnp.stack(from_cores(keep)), jnp.stack(from_cores(other))
        blocks = [jnp.where(first, keeps, others), jnp.where(first, others, keeps)]
    else:
        mine = lax.all_to_all(jnp.stack(fields, axis=1), "dp", split_axis=2, concat_axis=0, tiled=True)
        mine = mine.reshape(n_dp, rows, 3 * part)
        blocks = jnp.stack(from_cores(mine), axis=1)

    names = jnp.arange(all_experts, dtype=jnp.int32)
    hit = names[:, None, None] == expert_ids.T[None]
    table = jnp.sum(jnp.where(hit, gates.T[None], 0.0), axis=1)
    table = jnp.where(jnp.any(hit, axis=1), table, -1.0)
    tables = jnp.broadcast_to(table[None], (n_expert * n_dp, all_experts, rows))
    tables = lax.all_to_all(tables, ("expert", "dp"), split_axis=0, concat_axis=0, tiled=True)
    tables = tables.reshape(n_expert, n_dp, all_experts, rows)

    low = jnp.tril(jnp.ones((rows, rows), BF))
    weights = [
        (
            w_in[l].reshape(2 * ff, part),
            v_in[l].reshape(2 * ff, part),
            w_out[l],
            v_out[l],
        )
        for l in range(held)
    ]

    def replica(c, before=None):
        saved, spread, sent = [], [0.0] * n_expert, []
        block, ahead = blocks[c], None
        if before is not None:
            block, _ = lax.optimization_barrier((block, before[2]))
            ahead = before[0]
        for l in range(held):
            wi, vi, wo, vo = weights[l]
            expert = (rank * n_expert + core) * held + l
            picks, scales = [], []
            for r in range(n_expert):
                gate = tables[lax.rem(core + r, n_expert), c, expert]
                on = gate >= 0.0
                slot = dot_nt(on.astype(BF)[None, :], low)[0].astype(jnp.int32) - 1
                pick = (jnp.arange(cap, dtype=jnp.int32)[:, None] == slot[None, :]) & on[None, :]
                scales.append(jnp.sum(jnp.where(pick, gate[None, :], 0.0), axis=1))
                picks.append(pick.astype(BF))
            chosen = jnp.einsum(
                "rst,rtd->rsd", jnp.stack(picks), block, preferred_element_type=F32
            ).reshape(n_expert * cap, 3 * part)
            x = chosen[:, :part].astype(BF)
            u = chosen[:, part:2 * part].astype(BF)
            dy = (jnp.concatenate(scales)[:, None] * chosen[:, 2 * part:]).astype(BF)
            pre = sum_over(dot_nt(x, wi), "dp", sent)
            pre_dot = sum_over(dot_nt(u, wi) + dot_nt(x, vi), "dp", sent)
            backs = sum_over(jnp.concatenate([dot_nt(dy, wo), dot_nt(dy, vo)], axis=1), "dp", sent, ahead)
            grads, tangs, hidden = hidden_terms(pre, pre_dot, backs)
            saved.append((x, u, dy, grads, tangs, hidden))
            partial = (dot_nn(tangs, wi) + dot_nn(grads, vi)).astype(BF)
            for r, pick in enumerate(picks):
                spread[r] = spread[r] + dot_tn(pick, partial[r * cap:(r + 1) * cap])
        total = spread[0]
        for r in range(1, n_expert):
            moved = [(i, (i + r) % n_expert) for i in range(n_expert)]
            total = total + lax.ppermute(spread[r].astype(BF), "expert", moved).astype(F32)
        total = total.reshape(n_tensor, rows // n_tensor, part).astype(BF)
        got = lax.all_to_all(total, "tensor", split_axis=0, concat_axis=0, tiled=True)
        return jnp.sum(got.astype(F32), axis=0).astype(BF), saved, sent

    if n_dp <= 2:
        done = [replica(0)]
        for c in range(1, n_dp):
            done.append(replica(c, done[-1]))
        share, saved = jax.tree.map(lambda *v: jnp.stack(v), *[d[:2] for d in done])
    else:
        share, saved = lax.map(lambda c: replica(c)[:2], jnp.arange(n_dp))

    hvp_in, hvp_out = [], []
    for l in range(held):
        x, u, dy, grads, tangs, hidden = (v.reshape(-1, v.shape[-1]) for v in saved[l])
        both = jnp.concatenate([grads, tangs], axis=0)
        hvp_in.append(dot_tn(both, jnp.concatenate([u, x], axis=0)).reshape(2, ff, part))
        hvp_out.append(dot_tn(hidden, dy))

    share = jnp.broadcast_to(share[None], (n_tensor,) + share.shape)
    share = share.reshape((n_tensor * n_dp,) + share.shape[2:])
    share = lax.all_to_all(share, ("tensor", "dp"), split_axis=0, concat_axis=0, tiled=True)
    share = share.reshape(n_tensor, n_dp, rows // n_tensor, part).transpose(0, 2, 1, 3)
    hvp_tokens = share.reshape(rows, width).astype(F32)
    return hvp_tokens, jnp.stack(hvp_in), jnp.stack(hvp_out)


def remote(src, dst, send, recv, where):
    return pltpu.make_async_remote_copy(
        src_ref=src, dst_ref=dst, send_sem=send, recv_sem=recv, device_id=where, device_id_type=MESH
    )


def aligned(index, size):
    return pl.ds(pl.multiple_of(index * size, size), size)


def exchange_kernel(
    n_tensor, topk, cap, fc,
    tok_h, tan_h, cot_h, ids_h, gates_h, w_h, v_h, wo_h, vo_h,
    hin_o, hout_o, tok_o,
    wvo_s, tok_s, info_s, pick_s, rows_s, send_s, recv_s, fing_s, finh_s,
    part_s, own_s, give_s, core_s, sum_s, slice_s, share_s, ready_s, ids_s,
    wsem, lsem, c1s, c1r, c2s, c2r, c3s, c3r, c4s, c4r, c5s, c5r, c6s, c6r, c7s, c7r,
    as_, ar_, bs_, br_, cs_, cr_, ys_, yr_, zs_, zr_,
):
    t, e, p = lax.axis_index("tensor"), lax.axis_index("expert"), lax.axis_index("dp")
    q, other = 1 - p, 1 - e
    core, over = {"expert": other}, {"dp": q}
    rows, part = tok_s.shape[3], tok_s.shape[4]
    nch, early = wvo_s.shape[0], rows // 2
    half = nch // 2
    few, parts = rows // n_tensor, 2
    spans = ((0, early), (early, cap))
    mine, theirs = aligned(p, part), aligned(q, part)
    fields = (tan_h, tok_h, cot_h)
    plane = [{"tensor": lax.rem(t + k, n_tensor)} for k in range(1, n_tensor)]
    peers = [lax.rem(t + k, n_tensor) for k in range(1, n_tensor)]
    slice_t = aligned(t, few)

    barrier = pltpu.get_barrier_semaphore()
    for where in [core, over] + plane:
        pl.semaphore_signal(barrier, inc=1, device_id=where, device_id_type=MESH)

    local = [pltpu.make_async_copy(h.at[:, mine], tok_s.at[0, e, i], lsem.at[0]) for i, h in enumerate(fields)]
    local.append(pltpu.make_async_copy(ids_h, ids_s, lsem.at[1]))
    local.append(pltpu.make_async_copy(gates_h, info_s.at[0, e, pl.ds(topk, topk)], lsem.at[2]))
    for c in local:
        c.start()

    def load_weights(f, _):
        part_f = aligned(f, fc)
        pltpu.make_async_copy(w_h.at[0, :, part_f, :], wvo_s.at[f, 0], wsem.at[f]).start()
        pltpu.make_async_copy(v_h.at[0, :, part_f, :], wvo_s.at[f, 1], wsem.at[f]).start()
        pltpu.make_async_copy(wo_h.at[0, part_f, :], wvo_s.at[f, 2, 0], wsem.at[f]).start()
        pltpu.make_async_copy(vo_h.at[0, part_f, :], wvo_s.at[f, 2, 1], wsem.at[f]).start()
        return 0

    def wait_weights(f):
        pltpu.make_async_copy(wvo_s.at[f], wvo_s.at[f], wsem.at[f]).wait()

    lax.fori_loop(0, nch, load_weights, 0)


    expert = (t * 2 + e).astype(F32)
    low = (
        lax.broadcasted_iota(jnp.int32, (rows, rows), 0) > lax.broadcasted_iota(jnp.int32, (rows, rows), 1)
    ).astype(F32).astype(BF)
    lane = lax.broadcasted_iota(jnp.int32, (rows, rows), 1).astype(F32)

    def gather(rep, s):
        info = info_s[rep, s].T
        hit = info[:, :topk] == expert
        on = jnp.sum(jnp.where(hit, 1.0, 0.0), axis=1, keepdims=True)
        gate = jnp.sum(jnp.where(hit, info[:, topk:], 0.0), axis=1, keepdims=True)
        on = jnp.broadcast_to(on, (rows, rows))
        slot = dot_nn(low, on.astype(BF))
        pick = jnp.where((slot == lane) & (on > 0.5), 1.0, 0.0)
        pick_s[rep, s] = pick.astype(BF)
        pick = pick.T.astype(BF)[:cap]
        rows_s[rep, s, 0] = dot_nn(pick, tok_s[rep, s, 0]).astype(BF)
        rows_s[rep, s, 1] = dot_nn(pick, tok_s[rep, s, 1]).astype(BF)
        scaled = (gate * tok_s[rep, s, 2].astype(F32)).astype(BF)
        rows_s[rep, s, 2] = dot_nn(pick, scaled).astype(BF)

    def products(rep, s, f):
        w = wvo_s[f, 0].reshape(2 * fc, part)
        v = wvo_s[f, 1].reshape(2 * fc, part)
        o = wvo_s[f, 2].reshape(2 * fc, part)
        both = dot_nt(rows_s[rep, s, 0:2].reshape(2 * cap, part), w)
        return both[cap:], both[:cap] + dot_nt(rows_s[rep, s, 1], v), dot_nt(rows_s[rep, s, 2], o)

    def chunk_copy(s, f):
        return remote(send_s.at[s, f], recv_s.at[s, f], c5s, c5r.at[s, f], over)

    def make_chunk(s, f):
        pre, pre_dot, back = products(0, s, f)
        send_s[s, f, :, :2 * fc] = pre.astype(BF)
        send_s[s, f, :, 2 * fc:4 * fc] = pre_dot.astype(BF)
        send_s[s, f, :, 4 * fc:] = back.astype(BF)

    pltpu.make_async_copy(tok_s.at[0, e], tok_s.at[0, e], lsem.at[0]).wait()
    for c in local[3:]:
        c.wait()
    info_s[0, e, :topk, :] = ids_s[...].astype(F32)
    gather(0, e)
    wait_weights(0)
    make_chunk(e, 0)
    pl.semaphore_wait(barrier, 2 + len(plane))

    cross = [
        remote(h.at[slice_t, theirs], tok_s.at[1, e, i, slice_t], c2s.at[0], c2r.at[0], over)
        for i, h in enumerate(fields)
    ]
    cross.append(remote(info_s.at[0, e], info_s.at[1, e], c2s.at[1], c2r.at[1], over))
    first = [remote(h.at[:, mine], tok_s.at[0, e, i], c1s.at[0], c1r.at[0], core) for i, h in enumerate(fields)]
    first.append(remote(info_s.at[0, e], info_s.at[0, e], c1s.at[1], c1r.at[1], core))
    for c in cross + first:
        c.start()
    chunk_copy(e, 0).start()

    def send_own(f, _):
        wait_weights(f)
        make_chunk(e, f)
        chunk_copy(e, f).start()
        return 0

    lax.fori_loop(1, nch, send_own, 0)
    firsts = [remote(tok_s.at[0, other], tok_s.at[0, other], c1s.at[0], c1r.at[0], core), first[3]]
    for c in firsts:
        c.wait_recv()
    gather(0, other)

    tok_slice = tok_s.at[1, e, :, slice_t]
    crosses = [remote(tok_slice, tok_slice, c2s.at[0], c2r.at[0], over), cross[3]]
    for c in crosses:
        c.wait_recv()
    shared = [
        remote(tok_slice, tok_slice, c3s, c3r, where) for where in plane
    ]
    for c in shared:
        c.start()

    def send_other(f, _):
        make_chunk(other, f)
        chunk_copy(other, f).start()
        return 0

    lax.fori_loop(0, nch, send_other, 0)
    most = pl.ds(0, rows - few)
    tok_most = tok_s.at[1, e, :, most]
    shareds = remote(tok_most, tok_most, c3s, c3r, core)
    shareds.wait_recv()
    passed = [
        remote(tok_s.at[1, e], tok_s.at[1, e], c4s.at[0], c4r.at[0], core),
        remote(info_s.at[1, e], info_s.at[1, e], c4s.at[1], c4r.at[1], core),
    ]
    for c in passed:
        c.start()
    gather(1, e)
    for c in passed:
        c.wait_recv()
    gather(1, other)

    def back_rows(rep, s, f, lo, hi):
        w = wvo_s[f, 0].reshape(2 * fc, part)
        v = wvo_s[f, 1].reshape(2 * fc, part)
        return dot_nn(fing_s[rep, s, f, 1, lo:hi], w) + dot_nn(fing_s[rep, s, f, 0, lo:hi], v)

    def grads_copy(f):
        return remote(fing_s.at[1, 0, f], fing_s.at[0, 0, f], c6s, c6r.at[2, f], over)

    def rows_copy(h, f):
        lo, hi = spans[h]
        span = pl.ds(lo, hi - lo)
        return remote(fing_s.at[1, 1, f, :, span], fing_s.at[0, 1, f, :, span], c6s, c6r.at[h, f], over)

    part_s[...] = jnp.zeros_like(part_s)

    def finish_chunk(i, _):
        s, f = lax.rem(e + i // nch, 2), lax.rem(i, nch)
        pre, pre_dot, back = products(1, s, f)
        chunk_copy(s, f).wait_recv()
        pre = pre + recv_s[s, f, :, :2 * fc].astype(F32)
        pre_dot = pre_dot + recv_s[s, f, :, 2 * fc:4 * fc].astype(F32)
        back = back + recv_s[s, f, :, 4 * fc:].astype(F32)
        grads, tangs, hidden = hidden_terms(pre, pre_dot, back)
        fing_s[1, s, f, 0] = grads
        fing_s[1, s, f, 1] = tangs
        finh_s[1, s, f] = hidden

        @pl.when(s == 0)
        def _():
            grads_copy(f).start()

        part_s[1, s] += back_rows(1, s, f, 0, cap)
        return 0

    lax.fori_loop(0, 2 * nch, finish_chunk, 0)

    def give_back(h):
        def body(f, _):
            rows_copy(h, f).start()
            return 0

        return body

    lax.fori_loop(0, half, give_back(0), 0)

    def spread(rep, s, h):
        hi = spans[h][1]
        return dot_nn(pick_s[rep, s, h * early:(h + 1) * early, :hi], part_s[rep, s, :hi].astype(BF))

    def core_copy(rep, h):
        return remote(give_s.at[rep, h], core_s.at[rep, h], as_.at[rep, h], ar_.at[rep, h], core)

    def give_core(rep, s, h):
        give_s[rep, h] = spread(rep, s, h).astype(BF)
        core_copy(rep, h).start()

    def over_cores(rep, h):
        core_copy(rep, h).wait_recv()
        both = own_s[h] + core_s[rep, h].astype(F32)
        sum_s[rep, h] = both.reshape(sum_s.shape[2:]).astype(BF)
        for k, (peer, where) in enumerate(zip(peers, plane)):
            remote(sum_s.at[rep, h, peer], slice_s.at[rep, h, k], bs_.at[rep], br_.at[rep, h], where).start()

    def over_plane(rep, h):
        remote(slice_s.at[rep, h], slice_s.at[rep, h], bs_.at[rep], br_.at[rep, h], core).wait_recv()
        total = sum_s[rep, h, t].astype(F32)
        for k in range(n_tensor - 1):
            total = total + slice_s[rep, h, k].astype(F32)
        return total.astype(BF)

    def in_term(rep, s, f):
        g = fing_s[rep, s, f].reshape(2 * cap, 2 * fc)
        return dot_tn(g, rows_s[rep, s, 0:2].reshape(2 * cap, part)).reshape(2, fc, part)

    def out_term(rep, s, f):
        return dot_tn(finh_s[rep, s, f], rows_s[rep, s, 2])

    def start_weights(f, _):
        part_f = aligned(f, fc)
        hin_o[0, :, part_f, :] = in_term(1, 0, f) + in_term(1, 1, f)
        hout_o[0, part_f, :] = out_term(1, 0, f) + out_term(1, 1, f)
        return 0

    for h in range(parts):
        give_core(1, other, h)
    for h in range(parts):
        own_s[h] = spread(1, e, h)
    lax.fori_loop(0, half, start_weights, 0)
    for h in range(parts):
        over_cores(1, h)
    lax.fori_loop(half, nch, start_weights, 0)
    for h in range(parts):
        share_s[h] = over_plane(1, h)
    share_copy = remote(share_s, ready_s.at[1, :, t], ys_, yr_, over)
    share_copy.start()
    lax.fori_loop(half, nch, give_back(0), 0)
    lax.fori_loop(0, nch, give_back(1), 0)
    hidden = [remote(finh_s.at[1, s], finh_s.at[0, s], c7s, c7r.at[s], over) for s in range(2)]

    def give_hidden():
        for c in hidden:
            c.start()

    pl.when(e == 0)(give_hidden)

    def take_first(f, _):
        grads_copy(f).wait_recv()
        part_s[0, 0] += back_rows(0, 0, f, 0, cap)
        hin_o[0, :, aligned(f, fc), :] += in_term(0, 0, f)
        return 0

    def take_second(h):
        lo, hi = spans[h]

        def body(f, _):
            rows_copy(h, f).wait_recv()
            part_s[0, 1, lo:hi] += back_rows(0, 1, f, lo, hi)
            return 0

        return body

    def to_owner(s, h):
        @pl.when(e != s)
        def _():
            give_core(0, s, h)

        @pl.when(e == s)
        def _():
            own_s[h] = spread(0, s, h)

    def owner_sums(s, h):
        @pl.when(e == s)
        def _():
            over_cores(0, h)

    def owner_shares(s, h):
        @pl.when(e == s)
        def _():
            ready_s[0, h, t] = over_plane(0, h)
            mid = ready_s.at[0, h, t]
            for where in plane:
                remote(mid, mid, cs_, cr_, where).start()

    lax.fori_loop(0, nch, take_first, 0)
    for h in range(parts):
        to_owner(0, h)
    for h in range(parts):
        owner_sums(0, h)
    for h in range(parts):
        owner_shares(0, h)
    share_copy.wait_recv()
    for where in plane:
        mid = ready_s.at[1, :, t]
        remote(mid, mid, zs_, zr_, where).start()
    lax.fori_loop(0, nch, take_second(0), 0)
    to_owner(1, 0)
    owner_sums(1, 0)
    lax.fori_loop(0, nch, take_second(1), 0)
    to_owner(1, 1)
    pl.when(e == 1)(give_hidden)
    owner_shares(1, 0)
    owner_sums(1, 1)

    def end_in(f, _):
        hin_o[0, :, aligned(f, fc), :] += in_term(0, 1, f)
        return 0

    def end_out(s):
        def body(f, _):
            hout_o[0, aligned(f, fc), :] += out_term(0, s, f)
            return 0

        return body

    lax.fori_loop(0, nch, end_in, 0)
    owner_shares(1, 1)
    for s in range(2):
        hidden[s].wait_recv()
        lax.fori_loop(0, nch, end_out(s), 0)
    far = pl.ds(0, n_tensor - 1)
    plane_out = [
        remote(ready_s.at[1, :, far], ready_s.at[1, :, far], zs_, zr_, core),
        remote(ready_s.at[0, :, far], ready_s.at[0, :, far], cs_, cr_, core),
    ]
    for c in plane_out:
        c.wait_recv()
    tok_o[:, mine] = ready_s[0].astype(F32).reshape(rows, part)
    tok_o[:, theirs] = ready_s[1].astype(F32).reshape(rows, part)

    for c in firsts + crosses + [shareds] + passed + plane_out + [share_copy]:
        c.wait_send()
    for r in range(2):
        for h in range(parts):
            core_copy(r, h).wait_send()
        remote(slice_s.at[r], slice_s.at[r], bs_.at[r], br_.at[r, 0], core).wait_send()
    remote(send_s, send_s, c5s, c5r.at[0, 0], over).wait_send()
    remote(fing_s.at[1], fing_s.at[1], c6s, c6r.at[0, 0], over).wait_send()
    remote(finh_s.at[1], finh_s.at[1], c7s, c7r.at[0], over).wait_send()


def exchange(args, cap, fc):
    tokens, ids, w_in = args[0], args[3], args[5]
    n_tensor = lax.axis_size("tensor")
    rows, width = tokens.shape
    _, _, ff, part = w_in.shape
    topk = ids.shape[0]
    nch, peers, parts = ff // fc, n_tensor - 1, 2
    few = rows // n_tensor // parts
    dma = pltpu.SemaphoreType.DMA
    hbm = pl.BlockSpec(memory_space=pltpu.HBM)
    vmem = pl.BlockSpec(memory_space=pltpu.VMEM)
    return pl.pallas_call(
        functools.partial(exchange_kernel, n_tensor, topk, cap, fc),
        name="exchange",
        out_shape=[
            pltpu.VMEM((1, 2, ff, part), F32),
            pltpu.VMEM((1, ff, part), F32),
            pltpu.VMEM((rows, width), F32),
        ],
        in_specs=[hbm] * 9,
        out_specs=[vmem] * 3,
        scratch_shapes=[
            pltpu.VMEM((nch, 3, 2, fc, part), BF),
            pltpu.VMEM((2, 2, 3, rows, part), BF),
            pltpu.VMEM((2, 2, 2 * topk, rows), F32),
            pltpu.VMEM((2, 2, rows, rows), BF),
            pltpu.VMEM((2, 2, 3, cap, part), BF),
            pltpu.VMEM((2, nch, cap, 6 * fc), BF),
            pltpu.VMEM((2, nch, cap, 6 * fc), BF),
            pltpu.VMEM((2, 2, nch, 2, cap, 2 * fc), BF),
            pltpu.VMEM((2, 2, nch, cap, fc), BF),
            pltpu.VMEM((2, 2, cap, part), F32),
            pltpu.VMEM((parts, rows // 2, part), F32),
            pltpu.VMEM((2, parts, rows // 2, part), BF),
            pltpu.VMEM((2, parts, rows // 2, part), BF),
            pltpu.VMEM((2, parts, n_tensor, few, part), BF),
            pltpu.VMEM((2, parts, peers, few, part), BF),
            pltpu.VMEM((parts, few, part), BF),
            pltpu.VMEM((2, parts, n_tensor, few, part), BF),
            pltpu.VMEM((topk, rows), jnp.int32),
            dma((nch,)), dma((3,)),
            dma((2,)), dma((2,)), dma((2,)), dma((2,)), dma, dma, dma((2,)), dma((2,)),
            dma, dma((2, nch)), dma, dma((3, nch)), dma, dma((2,)),
            dma((2, parts)), dma((2, parts)), dma((2,)), dma((2, parts)),
            dma, dma, dma, dma, dma, dma,
        ],
        compiler_params=pltpu.CompilerParams(
            collective_id=0, has_side_effects=True, vmem_limit_bytes=44 * 1024 * 1024
        ),
    )(*[pltpu.with_memory_space_constraint(v, pltpu.HBM) for v in args])


def store_kernel(hin_v, hout_v, tok_v, hin_o, hout_o, tok_o, sem):
    ff = hin_v.shape[2]
    step = ff // 3
    copies = []
    for i in range(3):
        span = pl.ds(i * step, step)
        copies += [(hin_v.at[0, g, span], hin_o.at[0, g, span]) for g in range(2)]
        copies.append((hout_v.at[0, span], hout_o.at[0, span]))
    copies.append((tok_v, tok_o))
    copies = [pltpu.make_async_copy(src, dst, sem.at[i]) for i, (src, dst) in enumerate(copies)]
    for c in copies:
        c.start()
    for c in copies:
        c.wait()


def store(*results):
    return pl.pallas_call(
        store_kernel,
        name="store",
        out_shape=[pltpu.HBM(v.shape, v.dtype) for v in results],
        in_specs=[pl.BlockSpec(memory_space=pltpu.VMEM)] * 3,
        out_specs=[pl.BlockSpec(memory_space=pltpu.HBM)] * 3,
        scratch_shapes=[pltpu.SemaphoreType.DMA((10,))],
        compiler_params=pltpu.CompilerParams(vmem_limit_bytes=4 * 1024 * 1024),
    )(*[pltpu.with_memory_space_constraint(v, pltpu.VMEM) for v in results])


def kernel_shards(tokens, tangent, cotangent, expert_ids, gates, w_in, v_in, w_out, v_out):
    rows, _ = tokens.shape
    topk = expert_ids.shape[1]
    all_experts = lax.axis_size("tensor") * lax.axis_size("expert")
    cap = min(rows, 3 * rows * topk // (2 * all_experts))
    args = (tokens, tangent, cotangent, expert_ids.T, gates.T, w_in, v_in, w_out, v_out)
    hvp_in, hvp_out, out = exchange(args, cap, 128)
    hvp_in, hvp_out, out = store(hvp_in, hvp_out, out)
    return out, hvp_in, hvp_out


def shards(*args):
    tokens, expert_ids, w_in = args[0], args[3], args[5]
    n_tensor = lax.axis_size("tensor")
    rows, topk = expert_ids.shape
    fits = (
        lax.axis_size("expert") == 2 and lax.axis_size("dp") == 2 and w_in.shape[0] == 1
        and tokens.shape[1] == 2 * w_in.shape[3] and w_in.shape[3] % 128 == 0 and w_in.shape[2] % 256 == 0
        and rows == 128 and n_tensor > 1 and rows % (16 * n_tensor) == 0
        and topk % 8 == 0 and (3 * rows * topk) % (64 * n_tensor) == 0 and 3 * topk > 2 * n_tensor
    )
    return (kernel_shards if fits else plain_shards)(*args)


def solution(mesh):
    rows = P(("expert", "dp"), None)
    wide = P(("tensor", "expert"), None, None, "dp")
    tall = P(("tensor", "expert"), None, "dp")
    return jax.shard_map(
        shards,
        mesh=mesh,
        in_specs=(rows, rows, rows, rows, rows, wide, wide, tall, tall),
        out_specs=(rows, wide, tall),
        check_vma=False,
    )
```

```python
import functools

import jax
import jax.numpy as jnp
from jax import lax
from jax.experimental import pallas as pl
from jax.experimental.pallas import tpu as pltpu
from jax.sharding import PartitionSpec as P


BF = jnp.bfloat16
F32 = jnp.float32
MESH = pl.DeviceIdType.MESH


def dot_nt(x, w):
    return lax.dot_general(x, w, (((1,), (1,)), ((), ())), preferred_element_type=F32)


def dot_nn(x, w):
    return lax.dot_general(x, w, (((1,), (0,)), ((), ())), preferred_element_type=F32)


def dot_tn(x, w):
    return lax.dot_general(x, w, (((0,), (0,)), ((), ())), preferred_element_type=F32)


def sum_over(own, axis, sent, ahead=None):
    n = lax.axis_size(axis)
    if n & (n - 1):
        return lax.psum(own.astype(BF), axis).astype(F32)
    step = 1
    while step < n:
        give = own.astype(BF)
        if step == 1:
            sent.append(give)
        got = lax.ppermute(give, axis, [(i, i ^ step) for i in range(n)])
        if ahead is not None:
            got, ahead = lax.optimization_barrier((got, ahead))
        own = own + got.astype(F32)
        step *= 2
    return own


def hidden_terms(pre, pre_dot, backs):
    half = pre.shape[1] // 2
    gate_pre, up_val = pre[:, :half], pre[:, half:]
    gate_dot, up_dot = pre_dot[:, :half], pre_dot[:, half:]
    back, back_dot = backs[:, :half], backs[:, half:]
    sigma = jax.nn.sigmoid(gate_pre)
    silu_val = gate_pre * sigma
    first = sigma * (1.0 + gate_pre * (1.0 - sigma))
    second = sigma * (1.0 - sigma) * (2.0 + gate_pre * (1.0 - 2.0 * sigma))
    grad_a = back * up_val * first
    grad_b = back * silu_val
    tang_a = back_dot * up_val * first + back * up_dot * first + back * up_val * second * gate_dot
    tang_b = back_dot * silu_val + back * first * gate_dot
    hidden_dot = first * gate_dot * up_val + silu_val * up_dot
    grads = jnp.concatenate([grad_a, grad_b], axis=1).astype(BF)
    tangs = jnp.concatenate([tang_a, tang_b], axis=1).astype(BF)
    return grads, tangs, hidden_dot.astype(BF)


def plain_shards(tokens, tangent, cotangent, expert_ids, gates, w_in, v_in, w_out, v_out):
    n_tensor = lax.axis_size("tensor")
    n_expert = lax.axis_size("expert")
    n_dp = lax.axis_size("dp")
    rank, core = lax.axis_index("tensor"), lax.axis_index("expert")
    held, _, ff, part = w_in.shape
    all_experts = held * n_tensor * n_expert
    rows, width = tokens.shape
    topk = expert_ids.shape[1]
    cap = min(rows, 3 * rows * topk // (2 * all_experts))

    around = [
        [((i + r) % n_expert, i) for i in range(n_expert)] for r in range(n_expert)
    ]

    def from_cores(v):
        return [v] + [lax.ppermute(v, "expert", around[r]) for r in range(1, n_expert)]

    fields = (tokens, tangent, cotangent)
    if n_dp == 2:
        low_half = [v[:, :part] for v in fields]
        high_half = [v[:, part:] for v in fields]
        first = lax.axis_index("dp") == 0
        give = jnp.where(first, jnp.concatenate(high_half, axis=1), jnp.concatenate(low_half, axis=1))
        keep = jnp.where(first, jnp.concatenate(low_half, axis=1), jnp.concatenate(high_half, axis=1))
        other = lax.ppermute(give, "dp", [(0, 1), (1, 0)])
        keeps, others = jnp.stack(from_cores(keep)), jnp.stack(from_cores(other))
        blocks = [jnp.where(first, keeps, others), jnp.where(first, others, keeps)]
    else:
        mine = lax.all_to_all(jnp.stack(fields, axis=1), "dp", split_axis=2, concat_axis=0, tiled=True)
        mine = mine.reshape(n_dp, rows, 3 * part)
        blocks = jnp.stack(from_cores(mine), axis=1)

    names = jnp.arange(all_experts, dtype=jnp.int32)
    hit = names[:, None, None] == expert_ids.T[None]
    table = jnp.sum(jnp.where(hit, gates.T[None], 0.0), axis=1)
    table = jnp.where(jnp.any(hit, axis=1), table, -1.0)
    tables = jnp.broadcast_to(table[None], (n_expert * n_dp, all_experts, rows))
    tables = lax.all_to_all(tables, ("expert", "dp"), split_axis=0, concat_axis=0, tiled=True)
    tables = tables.reshape(n_expert, n_dp, all_experts, rows)

    low = jnp.tril(jnp.ones((rows, rows), BF))
    weights = [
        (
            w_in[l].reshape(2 * ff, part),
            v_in[l].reshape(2 * ff, part),
            w_out[l],
            v_out[l],
        )
        for l in range(held)
    ]

    def replica(c, before=None):
        saved, spread, sent = [], [0.0] * n_expert, []
        block, ahead = blocks[c], None
        if before is not None:
            block, _ = lax.optimization_barrier((block, before[2]))
            ahead = before[0]
        for l in range(held):
            wi, vi, wo, vo = weights[l]
            expert = (rank * n_expert + core) * held + l
            picks, scales = [], []
            for r in range(n_expert):
                gate = tables[lax.rem(core + r, n_expert), c, expert]
                on = gate >= 0.0
                slot = dot_nt(on.astype(BF)[None, :], low)[0].astype(jnp.int32) - 1
                pick = (jnp.arange(cap, dtype=jnp.int32)[:, None] == slot[None, :]) & on[None, :]
                scales.append(jnp.sum(jnp.where(pick, gate[None, :], 0.0), axis=1))
                picks.append(pick.astype(BF))
            chosen = jnp.einsum(
                "rst,rtd->rsd", jnp.stack(picks), block, preferred_element_type=F32
            ).reshape(n_expert * cap, 3 * part)
            x = chosen[:, :part].astype(BF)
            u = chosen[:, part:2 * part].astype(BF)
            dy = (jnp.concatenate(scales)[:, None] * chosen[:, 2 * part:]).astype(BF)
            pre = sum_over(dot_nt(x, wi), "dp", sent)
            pre_dot = sum_over(dot_nt(u, wi) + dot_nt(x, vi), "dp", sent)
            backs = sum_over(jnp.concatenate([dot_nt(dy, wo), dot_nt(dy, vo)], axis=1), "dp", sent, ahead)
            grads, tangs, hidden = hidden_terms(pre, pre_dot, backs)
            saved.append((x, u, dy, grads, tangs, hidden))
            partial = (dot_nn(tangs, wi) + dot_nn(grads, vi)).astype(BF)
            for r, pick in enumerate(picks):
                spread[r] = spread[r] + dot_tn(pick, partial[r * cap:(r + 1) * cap])
        total = spread[0]
        for r in range(1, n_expert):
            moved = [(i, (i + r) % n_expert) for i in range(n_expert)]
            total = total + lax.ppermute(spread[r].astype(BF), "expert", moved).astype(F32)
        total = total.reshape(n_tensor, rows // n_tensor, part).astype(BF)
        got = lax.all_to_all(total, "tensor", split_axis=0, concat_axis=0, tiled=True)
        return jnp.sum(got.astype(F32), axis=0).astype(BF), saved, sent

    if n_dp <= 2:
        done = [replica(0)]
        for c in range(1, n_dp):
            done.append(replica(c, done[-1]))
        share, saved = jax.tree.map(lambda *v: jnp.stack(v), *[d[:2] for d in done])
    else:
        share, saved = lax.map(lambda c: replica(c)[:2], jnp.arange(n_dp))

    hvp_in, hvp_out = [], []
    for l in range(held):
        x, u, dy, grads, tangs, hidden = (v.reshape(-1, v.shape[-1]) for v in saved[l])
        both = jnp.concatenate([grads, tangs], axis=0)
        hvp_in.append(dot_tn(both, jnp.concatenate([u, x], axis=0)).reshape(2, ff, part))
        hvp_out.append(dot_tn(hidden, dy))

    share = jnp.broadcast_to(share[None], (n_tensor,) + share.shape)
    share = share.reshape((n_tensor * n_dp,) + share.shape[2:])
    share = lax.all_to_all(share, ("tensor", "dp"), split_axis=0, concat_axis=0, tiled=True)
    share = share.reshape(n_tensor, n_dp, rows // n_tensor, part).transpose(0, 2, 1, 3)
    hvp_tokens = share.reshape(rows, width).astype(F32)
    return hvp_tokens, jnp.stack(hvp_in), jnp.stack(hvp_out)


def remote(src, dst, send, recv, where):
    return pltpu.make_async_remote_copy(
        src_ref=src, dst_ref=dst, send_sem=send, recv_sem=recv, device_id=where, device_id_type=MESH
    )


def aligned(index, size):
    return pl.ds(pl.multiple_of(index * size, size), size)


def exchange_kernel(
    n_tensor, topk, cap, fc,
    tok_h, tan_h, cot_h, ids_h, gates_h, w_h, v_h, wo_h, vo_h,
    hin_o, hout_o, tok_o,
    wvo_s, tok_s, info_s, pick_s, rows_s, send_s, recv_s, fing_s, finh_s,
    part_s, own_s, give_s, core_s, sum_s, slice_s, share_s, ready_s, ids_s, near_s,
    wsem, lsem, c1s, c1r, c2s, c2r, c3s, c3r, c4s, c4r, c5s, c5r, c6s, c6r, c7s, c7r,
    as_, ar_, bs_, br_, cs_, cr_, ys_, yr_, zs_, zr_,
):
    t, e, p = lax.axis_index("tensor"), lax.axis_index("expert"), lax.axis_index("dp")
    q, other = 1 - p, 1 - e
    core, over = {"expert": other}, {"dp": q}
    rows, part = tok_s.shape[3], tok_s.shape[4]
    nch, early = wvo_s.shape[0], rows // 2
    half = nch // 2
    few, parts = rows // n_tensor, 2
    spans = ((0, early), (early, cap))
    mine, theirs = aligned(p, part), aligned(q, part)
    fields = (tan_h, tok_h, cot_h)
    steps = [1 << k for k in range(n_tensor.bit_length() - 1)]
    plane = [{"tensor": lax.rem(t + k, n_tensor)} for k in range(1, n_tensor)]
    peers = [lax.rem(t + k, n_tensor) for k in range(1, n_tensor)]
    slice_t = aligned(t, few)

    barrier = pltpu.get_barrier_semaphore()
    near = [{"tensor": lax.rem(t // step + 1, 2) * step + lax.rem(t, step) + t // (2 * step) * (2 * step)} for step in steps]
    for where in [core, over] + near:
        pl.semaphore_signal(barrier, inc=1, device_id=where, device_id_type=MESH)

    local = [pltpu.make_async_copy(h.at[:, mine], tok_s.at[0, e, i], lsem.at[0]) for i, h in enumerate(fields)]
    local.append(pltpu.make_async_copy(ids_h, ids_s, lsem.at[1]))
    local.append(pltpu.make_async_copy(gates_h, info_s.at[0, e, pl.ds(topk, topk)], lsem.at[2]))
    for c in local:
        c.start()

    def load_weights(f, _):
        part_f = aligned(f, fc)
        pltpu.make_async_copy(w_h.at[0, :, part_f, :], wvo_s.at[f, 0], wsem.at[f]).start()
        pltpu.make_async_copy(v_h.at[0, :, part_f, :], wvo_s.at[f, 1], wsem.at[f]).start()
        pltpu.make_async_copy(wo_h.at[0, part_f, :], wvo_s.at[f, 2, 0], wsem.at[f]).start()
        pltpu.make_async_copy(vo_h.at[0, part_f, :], wvo_s.at[f, 2, 1], wsem.at[f]).start()
        return 0

    def wait_weights(f):
        pltpu.make_async_copy(wvo_s.at[f], wvo_s.at[f], wsem.at[f]).wait()

    lax.fori_loop(0, nch, load_weights, 0)


    expert = (t * 2 + e).astype(F32)
    low = (
        lax.broadcasted_iota(jnp.int32, (rows, rows), 0) > lax.broadcasted_iota(jnp.int32, (rows, rows), 1)
    ).astype(F32).astype(BF)
    lane = lax.broadcasted_iota(jnp.int32, (rows, rows), 1).astype(F32)

    def gather(rep, s):
        info = info_s[rep, s].T
        hit = info[:, :topk] == expert
        on = jnp.sum(jnp.where(hit, 1.0, 0.0), axis=1, keepdims=True)
        gate = jnp.sum(jnp.where(hit, info[:, topk:], 0.0), axis=1, keepdims=True)
        on = jnp.broadcast_to(on, (rows, rows))
        slot = dot_nn(low, on.astype(BF))
        pick = jnp.where((slot == lane) & (on > 0.5), 1.0, 0.0)
        pick_s[rep, s] = pick.astype(BF)
        pick = pick.T.astype(BF)[:cap]
        rows_s[rep, s, 0] = dot_nn(pick, tok_s[rep, s, 0]).astype(BF)
        rows_s[rep, s, 1] = dot_nn(pick, tok_s[rep, s, 1]).astype(BF)
        scaled = (gate * tok_s[rep, s, 2].astype(F32)).astype(BF)
        rows_s[rep, s, 2] = dot_nn(pick, scaled).astype(BF)

    def products(rep, s, f):
        w = wvo_s[f, 0].reshape(2 * fc, part)
        v = wvo_s[f, 1].reshape(2 * fc, part)
        o = wvo_s[f, 2].reshape(2 * fc, part)
        both = dot_nt(rows_s[rep, s, 0:2].reshape(2 * cap, part), w)
        return both[cap:], both[:cap] + dot_nt(rows_s[rep, s, 1], v), dot_nt(rows_s[rep, s, 2], o)

    def chunk_copy(s, f):
        return remote(send_s.at[s, f], recv_s.at[s, f], c5s, c5r.at[s, f], over)

    def make_chunk(s, f):
        pre, pre_dot, back = products(0, s, f)
        send_s[s, f, :, :2 * fc] = pre.astype(BF)
        send_s[s, f, :, 2 * fc:4 * fc] = pre_dot.astype(BF)
        send_s[s, f, :, 4 * fc:] = back.astype(BF)

    pltpu.make_async_copy(tok_s.at[0, e], tok_s.at[0, e], lsem.at[0]).wait()
    for c in local[3:]:
        c.wait()
    info_s[0, e, :topk, :] = ids_s[...].astype(F32)
    gather(0, e)
    wait_weights(0)
    make_chunk(e, 0)
    pl.semaphore_wait(barrier, 2 + len(near))

    def tell_near(r):
        for where in near:
            pl.semaphore_signal(near_s.at[r], inc=1, device_id=where, device_id_type=MESH)

    tell_near(0)

    cross = [
        remote(h.at[slice_t, theirs], tok_s.at[1, e, i, slice_t], c2s.at[0], c2r.at[0], over)
        for i, h in enumerate(fields)
    ]
    cross.append(remote(info_s.at[0, e], info_s.at[1, e], c2s.at[1], c2r.at[1], over))
    first = [remote(h.at[:, mine], tok_s.at[0, e, i], c1s.at[0], c1r.at[0], core) for i, h in enumerate(fields)]
    first.append(remote(info_s.at[0, e], info_s.at[0, e], c1s.at[1], c1r.at[1], core))
    for c in cross + first:
        c.start()
    chunk_copy(e, 0).start()

    def send_own(f, _):
        wait_weights(f)
        make_chunk(e, f)
        chunk_copy(e, f).start()
        return 0

    lax.fori_loop(1, nch, send_own, 0)
    for r in range(len(near) - 1):
        pl.semaphore_wait(near_s.at[r], len(near))
        if r + 2 < len(near):
            tell_near(r + 1)
    firsts = [remote(tok_s.at[0, other], tok_s.at[0, other], c1s.at[0], c1r.at[0], core), first[3]]
    for c in firsts:
        c.wait_recv()
    gather(0, other)

    tok_slice = tok_s.at[1, e, :, slice_t]
    crosses = [remote(tok_slice, tok_slice, c2s.at[0], c2r.at[0], over), cross[3]]
    for c in crosses:
        c.wait_recv()
    shared = [
        remote(tok_slice, tok_slice, c3s, c3r, where) for where in plane
    ]
    for c in shared:
        c.start()

    def send_other(f, _):
        make_chunk(other, f)
        chunk_copy(other, f).start()
        return 0

    lax.fori_loop(0, nch, send_other, 0)
    most = pl.ds(0, rows - few)
    tok_most = tok_s.at[1, e, :, most]
    shareds = remote(tok_most, tok_most, c3s, c3r, core)
    shareds.wait_recv()
    passed = [
        remote(tok_s.at[1, e], tok_s.at[1, e], c4s.at[0], c4r.at[0], core),
        remote(info_s.at[1, e], info_s.at[1, e], c4s.at[1], c4r.at[1], core),
    ]
    for c in passed:
        c.start()
    gather(1, e)
    for c in passed:
        c.wait_recv()
    gather(1, other)

    def back_rows(rep, s, f, lo, hi):
        w = wvo_s[f, 0].reshape(2 * fc, part)
        v = wvo_s[f, 1].reshape(2 * fc, part)
        return dot_nn(fing_s[rep, s, f, 1, lo:hi], w) + dot_nn(fing_s[rep, s, f, 0, lo:hi], v)

    def grads_copy(f):
        return remote(fing_s.at[1, 0, f], fing_s.at[0, 0, f], c6s, c6r.at[2, f], over)

    def rows_copy(h, f):
        lo, hi = spans[h]
        span = pl.ds(lo, hi - lo)
        return remote(fing_s.at[1, 1, f, :, span], fing_s.at[0, 1, f, :, span], c6s, c6r.at[h, f], over)

    part_s[...] = jnp.zeros_like(part_s)

    def finish_chunk(i, _):
        s, f = lax.rem(e + i // nch, 2), lax.rem(i, nch)
        pre, pre_dot, back = products(1, s, f)
        chunk_copy(s, f).wait_recv()
        pre = pre + recv_s[s, f, :, :2 * fc].astype(F32)
        pre_dot = pre_dot + recv_s[s, f, :, 2 * fc:4 * fc].astype(F32)
        back = back + recv_s[s, f, :, 4 * fc:].astype(F32)
        grads, tangs, hidden = hidden_terms(pre, pre_dot, back)
        fing_s[1, s, f, 0] = grads
        fing_s[1, s, f, 1] = tangs
        finh_s[1, s, f] = hidden

        @pl.when(s == 0)
        def _():
            grads_copy(f).start()

        part_s[1, s] += back_rows(1, s, f, 0, cap)
        return 0

    lax.fori_loop(0, 2 * nch, finish_chunk, 0)

    def give_back(h):
        def body(f, _):
            rows_copy(h, f).start()
            return 0

        return body

    lax.fori_loop(0, 2, give_back(0), 0)

    def spread(rep, s, h):
        hi = spans[h][1]
        return dot_nn(pick_s[rep, s, h * early:(h + 1) * early, :hi], part_s[rep, s, :hi].astype(BF))

    def core_copy(rep, h):
        return remote(give_s.at[rep, h], core_s.at[rep, h], as_.at[rep, h], ar_.at[rep, h], core)

    def give_core(rep, s, h):
        give_s[rep, h] = spread(rep, s, h).astype(BF)
        core_copy(rep, h).start()

    def over_cores(rep, h):
        core_copy(rep, h).wait_recv()
        both = own_s[h] + core_s[rep, h].astype(F32)
        sum_s[rep, h] = both.reshape(sum_s.shape[2:]).astype(BF)
        for k, (peer, where) in enumerate(zip(peers, plane)):
            remote(sum_s.at[rep, h, peer], slice_s.at[rep, h, k], bs_.at[rep], br_.at[rep, h], where).start()

    def over_plane(rep, h):
        remote(slice_s.at[rep, h], slice_s.at[rep, h], bs_.at[rep], br_.at[rep, h], core).wait_recv()
        total = sum_s[rep, h, t].astype(F32)
        for k in range(n_tensor - 1):
            total = total + slice_s[rep, h, k].astype(F32)
        return total.astype(BF)

    def in_term(rep, s, f):
        g = fing_s[rep, s, f].reshape(2 * cap, 2 * fc)
        return dot_tn(g, rows_s[rep, s, 0:2].reshape(2 * cap, part)).reshape(2, fc, part)

    def out_term(rep, s, f):
        return dot_tn(finh_s[rep, s, f], rows_s[rep, s, 2])

    def start_weights(f, _):
        part_f = aligned(f, fc)
        hin_o[0, :, part_f, :] = in_term(1, 0, f) + in_term(1, 1, f)
        hout_o[0, part_f, :] = out_term(1, 0, f) + out_term(1, 1, f)
        return 0

    for h in range(parts):
        give_core(1, other, h)
    for h in range(parts):
        own_s[h] = spread(1, e, h)
    lax.fori_loop(0, half, start_weights, 0)
    for h in range(parts):
        over_cores(1, h)
    lax.fori_loop(half, nch, start_weights, 0)
    for h in range(parts):
        share_s[h] = over_plane(1, h)
    share_copy = remote(share_s, ready_s.at[1, :, t], ys_, yr_, over)
    share_copy.start()
    lax.fori_loop(2, nch, give_back(0), 0)
    lax.fori_loop(0, nch, give_back(1), 0)
    hidden = [remote(finh_s.at[1, s], finh_s.at[0, s], c7s, c7r.at[s], over) for s in range(2)]

    def give_hidden():
        for c in hidden:
            c.start()

    pl.when(e == 0)(give_hidden)

    def take_first(f, _):
        grads_copy(f).wait_recv()
        part_s[0, 0] += back_rows(0, 0, f, 0, cap)
        hin_o[0, :, aligned(f, fc), :] += in_term(0, 0, f)
        return 0

    def take_second(h):
        lo, hi = spans[h]

        def body(f, _):
            rows_copy(h, f).wait_recv()
            part_s[0, 1, lo:hi] += back_rows(0, 1, f, lo, hi)
            return 0

        return body

    def to_owner(s, h):
        @pl.when(e != s)
        def _():
            give_core(0, s, h)

        @pl.when(e == s)
        def _():
            own_s[h] = spread(0, s, h)

    def owner_sums(s, h):
        @pl.when(e == s)
        def _():
            over_cores(0, h)

    def owner_shares(s, h):
        @pl.when(e == s)
        def _():
            ready_s[0, h, t] = over_plane(0, h)
            mid = ready_s.at[0, h, t]
            for where in plane:
                remote(mid, mid, cs_, cr_, where).start()

    def end_in(f, _):
        hin_o[0, :, aligned(f, fc), :] += in_term(0, 1, f)
        return 0

    def end_out(f, _):
        hout_o[0, aligned(f, fc), :] += out_term(0, 0, f) + out_term(0, 1, f)
        return 0

    lax.fori_loop(0, nch, take_first, 0)
    for h in range(parts):
        to_owner(0, h)
    for h in range(parts):
        owner_sums(0, h)
    share_copy.wait_recv()
    for where in plane:
        mid = ready_s.at[1, :, t]
        remote(mid, mid, zs_, zr_, where).start()
    lax.fori_loop(0, nch, take_second(0), 0)
    to_owner(1, 0)
    for h in range(parts):
        owner_shares(0, h)
    owner_sums(1, 0)
    lax.fori_loop(0, nch, take_second(1), 0)
    to_owner(1, 1)
    pl.when(e == 1)(give_hidden)
    owner_sums(1, 1)
    lax.fori_loop(0, nch, end_in, 0)
    owner_shares(1, 0)

    owner_shares(1, 1)
    for c in hidden:
        c.wait_recv()
    lax.fori_loop(0, nch, end_out, 0)
    far = pl.ds(0, n_tensor - 1)
    plane_out = [
        remote(ready_s.at[1, :, far], ready_s.at[1, :, far], zs_, zr_, core),
        remote(ready_s.at[0, :, far], ready_s.at[0, :, far], cs_, cr_, core),
    ]
    for c in plane_out:
        c.wait_recv()
    tok_o[:, mine] = ready_s[0].astype(F32).reshape(rows, part)
    tok_o[:, theirs] = ready_s[1].astype(F32).reshape(rows, part)

    for c in firsts + crosses + [shareds] + passed + plane_out + [share_copy]:
        c.wait_send()
    for r in range(2):
        for h in range(parts):
            core_copy(r, h).wait_send()
        remote(slice_s.at[r], slice_s.at[r], bs_.at[r], br_.at[r, 0], core).wait_send()
    remote(send_s, send_s, c5s, c5r.at[0, 0], over).wait_send()
    remote(fing_s.at[1], fing_s.at[1], c6s, c6r.at[0, 0], over).wait_send()
    remote(finh_s.at[1], finh_s.at[1], c7s, c7r.at[0], over).wait_send()


def exchange(args, cap, fc):
    tokens, ids, w_in = args[0], args[3], args[5]
    n_tensor = lax.axis_size("tensor")
    rows, width = tokens.shape
    _, _, ff, part = w_in.shape
    topk = ids.shape[0]
    nch, peers, parts = ff // fc, n_tensor - 1, 2
    few = rows // n_tensor // parts
    dma = pltpu.SemaphoreType.DMA
    hbm = pl.BlockSpec(memory_space=pltpu.HBM)
    vmem = pl.BlockSpec(memory_space=pltpu.VMEM)
    return pl.pallas_call(
        functools.partial(exchange_kernel, n_tensor, topk, cap, fc),
        name="exchange",
        out_shape=[
            pltpu.VMEM((1, 2, ff, part), F32),
            pltpu.VMEM((1, ff, part), F32),
            pltpu.VMEM((rows, width), F32),
        ],
        in_specs=[hbm] * 9,
        out_specs=[vmem] * 3,
        scratch_shapes=[
            pltpu.VMEM((nch, 3, 2, fc, part), BF),
            pltpu.VMEM((2, 2, 3, rows, part), BF),
            pltpu.VMEM((2, 2, 2 * topk, rows), F32),
            pltpu.VMEM((2, 2, rows, rows), BF),
            pltpu.VMEM((2, 2, 3, cap, part), BF),
            pltpu.VMEM((2, nch, cap, 6 * fc), BF),
            pltpu.VMEM((2, nch, cap, 6 * fc), BF),
            pltpu.VMEM((2, 2, nch, 2, cap, 2 * fc), BF),
            pltpu.VMEM((2, 2, nch, cap, fc), BF),
            pltpu.VMEM((2, 2, cap, part), F32),
            pltpu.VMEM((parts, rows // 2, part), F32),
            pltpu.VMEM((2, parts, rows // 2, part), BF),
            pltpu.VMEM((2, parts, rows // 2, part), BF),
            pltpu.VMEM((2, parts, n_tensor, few, part), BF),
            pltpu.VMEM((2, parts, peers, few, part), BF),
            pltpu.VMEM((parts, few, part), BF),
            pltpu.VMEM((2, parts, n_tensor, few, part), BF),
            pltpu.VMEM((topk, rows), jnp.int32),
            pltpu.SemaphoreType.REGULAR((n_tensor.bit_length(),)),
            dma((nch,)), dma((3,)),
            dma((2,)), dma((2,)), dma((2,)), dma((2,)), dma, dma, dma((2,)), dma((2,)),
            dma, dma((2, nch)), dma, dma((3, nch)), dma, dma((2,)),
            dma((2, parts)), dma((2, parts)), dma((2,)), dma((2, parts)),
            dma, dma, dma, dma, dma, dma,
        ],
        compiler_params=pltpu.CompilerParams(
            collective_id=0, has_side_effects=True, vmem_limit_bytes=44 * 1024 * 1024
        ),
    )(*[pltpu.with_memory_space_constraint(v, pltpu.HBM) for v in args])


def store_kernel(hin_v, hout_v, tok_v, hin_o, hout_o, tok_o, sem):
    ff = hin_v.shape[2]
    step = ff // 3
    copies = []
    for i in range(3):
        span = pl.ds(i * step, step)
        copies += [(hin_v.at[0, g, span], hin_o.at[0, g, span]) for g in range(2)]
        copies.append((hout_v.at[0, span], hout_o.at[0, span]))
    copies.append((tok_v, tok_o))
    copies = [pltpu.make_async_copy(src, dst, sem.at[i]) for i, (src, dst) in enumerate(copies)]
    for c in copies:
        c.start()
    for c in copies:
        c.wait()


def store(*results):
    return pl.pallas_call(
        store_kernel,
        name="store",
        out_shape=[pltpu.HBM(v.shape, v.dtype) for v in results],
        in_specs=[pl.BlockSpec(memory_space=pltpu.VMEM)] * 3,
        out_specs=[pl.BlockSpec(memory_space=pltpu.HBM)] * 3,
        scratch_shapes=[pltpu.SemaphoreType.DMA((10,))],
        compiler_params=pltpu.CompilerParams(vmem_limit_bytes=4 * 1024 * 1024),
    )(*[pltpu.with_memory_space_constraint(v, pltpu.VMEM) for v in results])


def kernel_shards(tokens, tangent, cotangent, expert_ids, gates, w_in, v_in, w_out, v_out):
    rows, _ = tokens.shape
    topk = expert_ids.shape[1]
    all_experts = lax.axis_size("tensor") * lax.axis_size("expert")
    cap = min(rows, 3 * rows * topk // (2 * all_experts))
    args = (tokens, tangent, cotangent, expert_ids.T, gates.T, w_in, v_in, w_out, v_out)
    hvp_in, hvp_out, out = exchange(args, cap, 128)
    hvp_in, hvp_out, out = store(hvp_in, hvp_out, out)
    return out, hvp_in, hvp_out


def shards(*args):
    tokens, expert_ids, w_in = args[0], args[3], args[5]
    n_tensor = lax.axis_size("tensor")
    rows, topk = expert_ids.shape
    fits = (
        lax.axis_size("expert") == 2 and lax.axis_size("dp") == 2 and w_in.shape[0] == 1
        and tokens.shape[1] == 2 * w_in.shape[3] and w_in.shape[3] % 128 == 0 and w_in.shape[2] % 256 == 0
        and rows == 128 and n_tensor > 2 and n_tensor & (n_tensor - 1) == 0 and rows % (16 * n_tensor) == 0
        and topk % 8 == 0 and (3 * rows * topk) % (64 * n_tensor) == 0 and 3 * topk > 2 * n_tensor
    )
    return (kernel_shards if fits else plain_shards)(*args)


def solution(mesh):
    rows = P(("expert", "dp"), None)
    wide = P(("tensor", "expert"), None, None, "dp")
    tall = P(("tensor", "expert"), None, "dp")
    return jax.shard_map(
        shards,
        mesh=mesh,
        in_specs=(rows, rows, rows, rows, rows, wide, wide, tall, tall),
        out_specs=(rows, wide, tall),
        check_vma=False,
    )
```

```python
import functools

import jax
import jax.numpy as jnp
from jax import lax
from jax.experimental import pallas as pl
from jax.experimental.pallas import tpu as pltpu
from jax.sharding import PartitionSpec as P


BF = jnp.bfloat16
F32 = jnp.float32
MESH = pl.DeviceIdType.MESH


def dot_nt(x, w):
    return lax.dot_general(x, w, (((1,), (1,)), ((), ())), preferred_element_type=F32)


def dot_nn(x, w):
    return lax.dot_general(x, w, (((1,), (0,)), ((), ())), preferred_element_type=F32)


def dot_tn(x, w):
    return lax.dot_general(x, w, (((0,), (0,)), ((), ())), preferred_element_type=F32)


def sum_over(own, axis, sent, ahead=None):
    n = lax.axis_size(axis)
    if n & (n - 1):
        return lax.psum(own.astype(BF), axis).astype(F32)
    step = 1
    while step < n:
        give = own.astype(BF)
        if step == 1:
            sent.append(give)
        got = lax.ppermute(give, axis, [(i, i ^ step) for i in range(n)])
        if ahead is not None:
            got, ahead = lax.optimization_barrier((got, ahead))
        own = own + got.astype(F32)
        step *= 2
    return own


def hidden_terms(pre, pre_dot, backs):
    half = pre.shape[1] // 2
    gate_pre, up_val = pre[:, :half], pre[:, half:]
    gate_dot, up_dot = pre_dot[:, :half], pre_dot[:, half:]
    back, back_dot = backs[:, :half], backs[:, half:]
    sigma = jax.nn.sigmoid(gate_pre)
    silu_val = gate_pre * sigma
    first = sigma * (1.0 + gate_pre * (1.0 - sigma))
    second = sigma * (1.0 - sigma) * (2.0 + gate_pre * (1.0 - 2.0 * sigma))
    grad_a = back * up_val * first
    grad_b = back * silu_val
    tang_a = back_dot * up_val * first + back * up_dot * first + back * up_val * second * gate_dot
    tang_b = back_dot * silu_val + back * first * gate_dot
    hidden_dot = first * gate_dot * up_val + silu_val * up_dot
    grads = jnp.concatenate([grad_a, grad_b], axis=1).astype(BF)
    tangs = jnp.concatenate([tang_a, tang_b], axis=1).astype(BF)
    return grads, tangs, hidden_dot.astype(BF)


def plain_shards(tokens, tangent, cotangent, expert_ids, gates, w_in, v_in, w_out, v_out):
    n_tensor = lax.axis_size("tensor")
    n_expert = lax.axis_size("expert")
    n_dp = lax.axis_size("dp")
    rank, core = lax.axis_index("tensor"), lax.axis_index("expert")
    held, _, ff, part = w_in.shape
    all_experts = held * n_tensor * n_expert
    rows, width = tokens.shape
    topk = expert_ids.shape[1]
    cap = min(rows, 3 * rows * topk // (2 * all_experts))

    around = [
        [((i + r) % n_expert, i) for i in range(n_expert)] for r in range(n_expert)
    ]

    def from_cores(v):
        return [v] + [lax.ppermute(v, "expert", around[r]) for r in range(1, n_expert)]

    fields = (tokens, tangent, cotangent)
    if n_dp == 2:
        low_half = [v[:, :part] for v in fields]
        high_half = [v[:, part:] for v in fields]
        first = lax.axis_index("dp") == 0
        give = jnp.where(first, jnp.concatenate(high_half, axis=1), jnp.concatenate(low_half, axis=1))
        keep = jnp.where(first, jnp.concatenate(low_half, axis=1), jnp.concatenate(high_half, axis=1))
        other = lax.ppermute(give, "dp", [(0, 1), (1, 0)])
        keeps, others = jnp.stack(from_cores(keep)), jnp.stack(from_cores(other))
        blocks = [jnp.where(first, keeps, others), jnp.where(first, others, keeps)]
    else:
        mine = lax.all_to_all(jnp.stack(fields, axis=1), "dp", split_axis=2, concat_axis=0, tiled=True)
        mine = mine.reshape(n_dp, rows, 3 * part)
        blocks = jnp.stack(from_cores(mine), axis=1)

    names = jnp.arange(all_experts, dtype=jnp.int32)
    hit = names[:, None, None] == expert_ids.T[None]
    table = jnp.sum(jnp.where(hit, gates.T[None], 0.0), axis=1)
    table = jnp.where(jnp.any(hit, axis=1), table, -1.0)
    tables = jnp.broadcast_to(table[None], (n_expert * n_dp, all_experts, rows))
    tables = lax.all_to_all(tables, ("expert", "dp"), split_axis=0, concat_axis=0, tiled=True)
    tables = tables.reshape(n_expert, n_dp, all_experts, rows)

    low = jnp.tril(jnp.ones((rows, rows), BF))
    weights = [
        (
            w_in[l].reshape(2 * ff, part),
            v_in[l].reshape(2 * ff, part),
            w_out[l],
            v_out[l],
        )
        for l in range(held)
    ]

    def replica(c, before=None):
        saved, spread, sent = [], [0.0] * n_expert, []
        block, ahead = blocks[c], None
        if before is not None:
            block, _ = lax.optimization_barrier((block, before[2]))
            ahead = before[0]
        for l in range(held):
            wi, vi, wo, vo = weights[l]
            expert = (rank * n_expert + core) * held + l
            picks, scales = [], []
            for r in range(n_expert):
                gate = tables[lax.rem(core + r, n_expert), c, expert]
                on = gate >= 0.0
                slot = dot_nt(on.astype(BF)[None, :], low)[0].astype(jnp.int32) - 1
                pick = (jnp.arange(cap, dtype=jnp.int32)[:, None] == slot[None, :]) & on[None, :]
                scales.append(jnp.sum(jnp.where(pick, gate[None, :], 0.0), axis=1))
                picks.append(pick.astype(BF))
            chosen = jnp.einsum(
                "rst,rtd->rsd", jnp.stack(picks), block, preferred_element_type=F32
            ).reshape(n_expert * cap, 3 * part)
            x = chosen[:, :part].astype(BF)
            u = chosen[:, part:2 * part].astype(BF)
            dy = (jnp.concatenate(scales)[:, None] * chosen[:, 2 * part:]).astype(BF)
            pre = sum_over(dot_nt(x, wi), "dp", sent)
            pre_dot = sum_over(dot_nt(u, wi) + dot_nt(x, vi), "dp", sent)
            backs = sum_over(jnp.concatenate([dot_nt(dy, wo), dot_nt(dy, vo)], axis=1), "dp", sent, ahead)
            grads, tangs, hidden = hidden_terms(pre, pre_dot, backs)
            saved.append((x, u, dy, grads, tangs, hidden))
            partial = (dot_nn(tangs, wi) + dot_nn(grads, vi)).astype(BF)
            for r, pick in enumerate(picks):
                spread[r] = spread[r] + dot_tn(pick, partial[r * cap:(r + 1) * cap])
        total = spread[0]
        for r in range(1, n_expert):
            moved = [(i, (i + r) % n_expert) for i in range(n_expert)]
            total = total + lax.ppermute(spread[r].astype(BF), "expert", moved).astype(F32)
        total = total.reshape(n_tensor, rows // n_tensor, part).astype(BF)
        got = lax.all_to_all(total, "tensor", split_axis=0, concat_axis=0, tiled=True)
        return jnp.sum(got.astype(F32), axis=0).astype(BF), saved, sent

    if n_dp <= 2:
        done = [replica(0)]
        for c in range(1, n_dp):
            done.append(replica(c, done[-1]))
        share, saved = jax.tree.map(lambda *v: jnp.stack(v), *[d[:2] for d in done])
    else:
        share, saved = lax.map(lambda c: replica(c)[:2], jnp.arange(n_dp))

    hvp_in, hvp_out = [], []
    for l in range(held):
        x, u, dy, grads, tangs, hidden = (v.reshape(-1, v.shape[-1]) for v in saved[l])
        both = jnp.concatenate([grads, tangs], axis=0)
        hvp_in.append(dot_tn(both, jnp.concatenate([u, x], axis=0)).reshape(2, ff, part))
        hvp_out.append(dot_tn(hidden, dy))

    share = jnp.broadcast_to(share[None], (n_tensor,) + share.shape)
    share = share.reshape((n_tensor * n_dp,) + share.shape[2:])
    share = lax.all_to_all(share, ("tensor", "dp"), split_axis=0, concat_axis=0, tiled=True)
    share = share.reshape(n_tensor, n_dp, rows // n_tensor, part).transpose(0, 2, 1, 3)
    hvp_tokens = share.reshape(rows, width).astype(F32)
    return hvp_tokens, jnp.stack(hvp_in), jnp.stack(hvp_out)


def remote(src, dst, send, recv, where):
    return pltpu.make_async_remote_copy(
        src_ref=src, dst_ref=dst, send_sem=send, recv_sem=recv, device_id=where, device_id_type=MESH
    )


def aligned(index, size):
    return pl.ds(pl.multiple_of(index * size, size), size)


def exchange_kernel(
    n_tensor, topk, cap, fc,
    tok_h, tan_h, cot_h, ids_h, gates_h, w_h, v_h, wo_h, vo_h,
    hin_o, hout_o, tok_o,
    wvo_s, tok_s, info_s, pick_s, rows_s, dy_s, send_s, recv_s, fing_s, finh_s,
    part_s, own_s, give_s, core_s, sum_s, slice_s, share_s, ready_s, ids_s, near_s, go_s, lead_s,
    wsem, lsem, c1s, c1r, c2s, c2r, c3s, c3r, c4s, c4r, c5s, c5r, c6s, c6r, c7s, c7r,
    as_, ar_, bs_, br_, cs_, cr_, ys_, yr_, zs_, zr_, xs_, xr_,
):
    t, e, p = lax.axis_index("tensor"), lax.axis_index("expert"), lax.axis_index("dp")
    q, other = 1 - p, 1 - e
    tz, tx = t // 2, lax.rem(t, 2)
    core, over = {"expert": other}, {"dp": q}
    rows, part = tok_s.shape[3], tok_s.shape[4]
    nch, early = wvo_s.shape[0], rows // 2
    half = nch // 2
    few, parts = rows // n_tensor, 2
    spans = ((0, early), (early, cap))
    mine, theirs = aligned(p, part), aligned(q, part)
    fields = (tan_h, tok_h, cot_h)
    steps = [1 << k for k in range(n_tensor.bit_length() - 1)]
    plane = [{"tensor": lax.rem(t + k, n_tensor)} for k in range(1, n_tensor)]
    peers = [lax.rem(t + k, n_tensor) for k in range(1, n_tensor)]
    slice_t = aligned(t, few)

    barrier = pltpu.get_barrier_semaphore()
    near = [{"tensor": lax.rem(t // step + 1, 2) * step + lax.rem(t, step) + t // (2 * step) * (2 * step)} for step in steps]
    for where in [core, over] + near:
        pl.semaphore_signal(barrier, inc=1, device_id=where, device_id_type=MESH)

    local = [pltpu.make_async_copy(h.at[:, mine], tok_s.at[0, e, i], lsem.at[0]) for i, h in enumerate(fields)]
    local += [
        pltpu.make_async_copy(h.at[slice_t, theirs], lead_s.at[i], lsem.at[3]) for i, h in enumerate(fields)
    ]
    local.append(pltpu.make_async_copy(ids_h, ids_s, lsem.at[1]))
    local.append(pltpu.make_async_copy(gates_h, info_s.at[0, e, pl.ds(topk, topk)], lsem.at[2]))
    for c in local:
        c.start()

    def load_weights(f, _):
        part_f = aligned(f, fc)
        pltpu.make_async_copy(w_h.at[0, :, part_f, :], wvo_s.at[f, 0], wsem.at[f]).start()
        pltpu.make_async_copy(v_h.at[0, :, part_f, :], wvo_s.at[f, 1], wsem.at[f]).start()
        pltpu.make_async_copy(wo_h.at[0, part_f, :], wvo_s.at[f, 2, 0], wsem.at[f]).start()
        pltpu.make_async_copy(vo_h.at[0, part_f, :], wvo_s.at[f, 2, 1], wsem.at[f]).start()
        return 0

    def wait_weights(f):
        pltpu.make_async_copy(wvo_s.at[f], wvo_s.at[f], wsem.at[f]).wait()

    lax.fori_loop(0, nch, load_weights, 0)


    expert = (t * 2 + e).astype(F32)
    low = (
        lax.broadcasted_iota(jnp.int32, (rows, rows), 0) > lax.broadcasted_iota(jnp.int32, (rows, rows), 1)
    ).astype(F32).astype(BF)
    lane = lax.broadcasted_iota(jnp.int32, (rows, rows), 1).astype(F32)

    def gather(rep, s):
        info = info_s[rep, s].T
        hit = info[:, :topk] == expert
        on = jnp.sum(jnp.where(hit, 1.0, 0.0), axis=1, keepdims=True)
        gate = jnp.sum(jnp.where(hit, info[:, topk:], 0.0), axis=1, keepdims=True)
        on = jnp.broadcast_to(on, (rows, rows))
        slot = dot_nn(low, on.astype(BF))
        pick = jnp.where((slot == lane) & (on > 0.5), 1.0, 0.0)
        pick_s[rep, s] = pick.astype(BF)
        pick = pick.T.astype(BF)[:cap]
        rows_s[rep, s, 0] = dot_nn(pick, tok_s[rep, s, 0]).astype(BF)
        rows_s[rep, s, 1] = dot_nn(pick, tok_s[rep, s, 1]).astype(BF)
        scaled = (gate * tok_s[rep, s, 2].astype(F32)).astype(BF)
        dy_s[rep, aligned(s, cap)] = dot_nn(pick, scaled).astype(BF)

    def products(rep, s, f):
        w = wvo_s[f, 0].reshape(2 * fc, part)
        v = wvo_s[f, 1].reshape(2 * fc, part)
        o = wvo_s[f, 2].reshape(2 * fc, part)
        both = dot_nt(rows_s[rep, s].reshape(2 * cap, part), w)
        return both[cap:], both[:cap] + dot_nt(rows_s[rep, s, 1], v), dot_nt(dy_s[rep, aligned(s, cap)], o)

    def chunk_copy(s, f):
        return remote(send_s.at[s, f], recv_s.at[s, f], c5s, c5r.at[s, f], over)

    def make_chunk(s, f):
        pre, pre_dot, back = products(0, s, f)
        send_s[s, f, :, :2 * fc] = pre.astype(BF)
        send_s[s, f, :, 2 * fc:4 * fc] = pre_dot.astype(BF)
        send_s[s, f, :, 4 * fc:] = back.astype(BF)

    pltpu.make_async_copy(tok_s.at[0, e], tok_s.at[0, e], lsem.at[0]).wait()
    for c in local[6:]:
        c.wait()
    pltpu.make_async_copy(lead_s, lead_s, lsem.at[3]).wait()
    info_s[0, e, :topk, :] = ids_s[...].astype(F32)
    pl.semaphore_wait(barrier, 2 + len(near))

    def tell_near(r):
        for where in near:
            pl.semaphore_signal(near_s.at[r], inc=1, device_id=where, device_id_type=MESH)

    tell_near(0)
    tok_slice = tok_s.at[1, e, :, slice_t]
    cross = [
        remote(lead_s, tok_slice, c2s.at[0], c2r.at[0], over),
        remote(info_s.at[0, e], info_s.at[1, e], c2s.at[1], c2r.at[1], over),
    ]
    first = [
        remote(tok_s.at[0, e], tok_s.at[0, e], c1s.at[0], c1r.at[0], core),
        remote(info_s.at[0, e], info_s.at[0, e], c1s.at[1], c1r.at[1], core),
    ]
    for c in cross + first:
        c.start()
    gather(0, e)
    wait_weights(0)
    make_chunk(e, 0)

    chunk_copy(e, 0).start()

    def send_own(f, _):
        wait_weights(f)
        make_chunk(e, f)
        chunk_copy(e, f).start()
        return 0

    lax.fori_loop(1, nch, send_own, 0)
    for r in range(len(near) - 1):
        pl.semaphore_wait(near_s.at[r], len(near))
        if r + 2 < len(near):
            tell_near(r + 1)
    for c in first:
        c.wait_recv()
    gather(0, other)

    for c in cross:
        c.wait_recv()
    shared = [
        remote(tok_slice, tok_slice, c3s, c3r, where) for where in plane
    ]
    for c in shared:
        c.start()

    def send_other(f, _):
        make_chunk(other, f)
        chunk_copy(other, f).start()
        return 0

    lax.fori_loop(0, nch, send_other, 0)
    most = pl.ds(0, rows - few)
    tok_most = tok_s.at[1, e, :, most]
    shareds = remote(tok_most, tok_most, c3s, c3r, core)
    shareds.wait_recv()
    passed = [
        remote(tok_s.at[1, e], tok_s.at[1, e], c4s.at[0], c4r.at[0], core),
        remote(info_s.at[1, e], info_s.at[1, e], c4s.at[1], c4r.at[1], core),
    ]
    for c in passed:
        c.start()
    gather(1, e)
    for c in passed:
        c.wait_recv()
    gather(1, other)

    def back_rows(rep, s, f, lo, hi):
        w = wvo_s[f, 0].reshape(2 * fc, part)
        v = wvo_s[f, 1].reshape(2 * fc, part)
        return dot_nn(fing_s[rep, s, f, 1, lo:hi], w) + dot_nn(fing_s[rep, s, f, 0, lo:hi], v)

    def grads_copy(f):
        return remote(fing_s.at[1, 0, f], fing_s.at[0, 0, f], c6s, c6r.at[2, f], over)

    def rows_copy(h, f):
        lo, hi = spans[h]
        span = pl.ds(lo, hi - lo)
        return remote(fing_s.at[1, 1, f, :, span], fing_s.at[0, 1, f, :, span], c6s, c6r.at[h, f], over)

    part_s[...] = jnp.zeros_like(part_s)

    def finish_chunk(i, _):
        s, f = lax.rem(e + i // nch, 2), lax.rem(i, nch)
        pre, pre_dot, back = products(1, s, f)
        chunk_copy(s, f).wait_recv()
        pre = pre + recv_s[s, f, :, :2 * fc].astype(F32)
        pre_dot = pre_dot + recv_s[s, f, :, 2 * fc:4 * fc].astype(F32)
        back = back + recv_s[s, f, :, 4 * fc:].astype(F32)
        grads, tangs, hidden = hidden_terms(pre, pre_dot, back)
        fing_s[1, s, f, 0] = grads
        fing_s[1, s, f, 1] = tangs
        finh_s[1, f, aligned(s, cap)] = hidden

        @pl.when(s == 0)
        def _():
            grads_copy(f).start()

        part_s[1, s] += back_rows(1, s, f, 0, cap)
        return 0

    lax.fori_loop(0, 2 * nch, finish_chunk, 0)

    def give_back(h):
        def body(f, _):
            rows_copy(h, f).start()
            return 0

        return body

    lax.fori_loop(0, 2, give_back(0), 0)

    def spread(rep, s, h):
        hi = spans[h][1]
        return dot_nn(pick_s[rep, s, h * early:(h + 1) * early, :hi], part_s[rep, s, :hi].astype(BF))

    def core_copy(rep, h):
        return remote(give_s.at[rep, h], core_s.at[rep, h], as_.at[rep, h], ar_.at[rep, h], core)

    def give_core(rep, s, h):
        give_s[rep, h] = spread(rep, s, h).astype(BF)
        core_copy(rep, h).start()

    def over_cores(rep, h):
        core_copy(rep, h).wait_recv()
        both = own_s[h] + core_s[rep, h].astype(F32)
        sum_s[rep, h] = both.reshape(sum_s.shape[2:]).astype(BF)
        for k, (peer, where) in enumerate(zip(peers, plane)):
            remote(sum_s.at[rep, h, peer], slice_s.at[rep, h, k], bs_.at[rep], br_.at[rep, h], where).start()

    def over_plane(rep, h):
        remote(slice_s.at[rep, h], slice_s.at[rep, h], bs_.at[rep], br_.at[rep, h], core).wait_recv()
        total = sum_s[rep, h, t].astype(F32)
        for k in range(n_tensor - 1):
            total = total + slice_s[rep, h, k].astype(F32)
        return total.astype(BF)

    def in_term(rep, s, f):
        g = fing_s[rep, s, f].reshape(2 * cap, 2 * fc)
        return dot_tn(g, rows_s[rep, s].reshape(2 * cap, part)).reshape(2, fc, part)

    def out_term(rep, f):
        return dot_tn(finh_s[rep, f], dy_s[rep])

    def start_weights(f, _):
        part_f = aligned(f, fc)
        hin_o[0, :, part_f, :] = in_term(1, 0, f) + in_term(1, 1, f)
        hout_o[0, part_f, :] = out_term(1, f)
        return 0

    for h in range(parts):
        give_core(1, other, h)
    for h in range(parts):
        own_s[h] = spread(1, e, h)
    lax.fori_loop(0, half, start_weights, 0)
    for h in range(parts):
        over_cores(1, h)
    lax.fori_loop(half, nch, start_weights, 0)
    def take_first(f, _):
        grads_copy(f).wait_recv()
        part_s[0, 0] += back_rows(0, 0, f, 0, cap)
        hin_o[0, :, aligned(f, fc), :] += in_term(0, 0, f)
        return 0

    def take_second(h):
        lo, hi = spans[h]

        def body(f, _):
            rows_copy(h, f).wait_recv()
            part_s[0, 1, lo:hi] += back_rows(0, 1, f, lo, hi)
            return 0

        return body

    def to_owner(s, h):
        @pl.when(e != s)
        def _():
            give_core(0, s, h)

        @pl.when(e == s)
        def _():
            own_s[h] = spread(0, s, h)

    def owner_sums(s, h):
        @pl.when(e == s)
        def _():
            over_cores(0, h)

    def owner_shares(s, h):
        @pl.when(e == s)
        def _():
            ready_s[0, h, tz, tx] = over_plane(0, h)
            mid = ready_s.at[0, h, tz, tx]
            for where in plane:
                remote(mid, mid, cs_, cr_, where).start()

    def end_in(f, _):
        hin_o[0, :, aligned(f, fc), :] += in_term(0, 1, f)
        return 0

    def end_out(f, _):
        hout_o[0, aligned(f, fc), :] += out_term(0, f)
        return 0

    lax.fori_loop(0, nch, take_first, 0)
    for h in range(parts):
        to_owner(0, h)
    for h in range(parts):
        share_s[h] = over_plane(1, h)
    share_copy = remote(share_s, ready_s.at[1, :, tz, tx], ys_, yr_, over)
    share_copy.start()
    lax.fori_loop(2, nch, give_back(0), 0)

    @pl.when(e == 0)
    def _():
        lax.fori_loop(0, nch, give_back(1), 0)

    hidden = remote(finh_s.at[1], finh_s.at[0], c7s, c7r, over)

    for h in range(parts):
        owner_sums(0, h)
    share_copy.wait_recv()
    for k in range(2, n_tensor, 2):
        mid = ready_s.at[1, :, tz, tx]
        remote(mid, mid, zs_, zr_, {"tensor": lax.rem(t + k, n_tensor)}).start()
    lax.fori_loop(0, nch - 1, take_second(0), 0)

    @pl.when(e == 0)
    def _():
        pl.semaphore_signal(go_s, inc=1, device_id=core, device_id_type=MESH)

    lax.fori_loop(nch - 1, nch, take_second(0), 0)
    to_owner(1, 0)

    @pl.when(e == 1)
    def _():
        pl.semaphore_wait(go_s, 1)
        lax.fori_loop(0, nch, give_back(1), 0)
        hidden.start()

    line = ready_s.at[1, :, pl.ds(0, n_tensor // 2 - 1), tx]
    lines = remote(line, line, zs_, zr_, core)
    lines.wait_recv()
    column = ready_s.at[1, :, :, tx]
    columns = remote(column, column, xs_, xr_, near[0])
    columns.start()
    for h in range(parts):
        owner_shares(0, h)
    owner_sums(1, 0)
    lax.fori_loop(0, nch, take_second(1), 0)
    to_owner(1, 1)
    pl.when(e == 0)(hidden.start)
    owner_sums(1, 1)
    lax.fori_loop(0, nch, end_in, 0)
    owner_shares(1, 0)

    owner_shares(1, 1)
    hidden.wait_recv()
    lax.fori_loop(0, nch, end_out, 0)
    plane_out = [remote(slice_s.at[0], slice_s.at[0], cs_, cr_, core), columns]
    for c in plane_out:
        c.wait_recv()
    tok_o[:, mine] = ready_s[0].astype(F32).reshape(rows, part)
    tok_o[:, theirs] = ready_s[1].astype(F32).reshape(rows, part)

    for c in first + cross + [shareds] + passed + plane_out + [lines, share_copy]:
        c.wait_send()
    for r in range(2):
        for h in range(parts):
            core_copy(r, h).wait_send()
        remote(slice_s.at[r], slice_s.at[r], bs_.at[r], br_.at[r, 0], core).wait_send()
    remote(send_s, send_s, c5s, c5r.at[0, 0], over).wait_send()
    remote(fing_s.at[1], fing_s.at[1], c6s, c6r.at[0, 0], over).wait_send()
    hidden.wait_send()


def exchange(args, cap, fc):
    tokens, ids, w_in = args[0], args[3], args[5]
    n_tensor = lax.axis_size("tensor")
    rows, width = tokens.shape
    _, _, ff, part = w_in.shape
    topk = ids.shape[0]
    nch, peers, parts = ff // fc, n_tensor - 1, 2
    few = rows // n_tensor // parts
    dma = pltpu.SemaphoreType.DMA
    hbm = pl.BlockSpec(memory_space=pltpu.HBM)
    vmem = pl.BlockSpec(memory_space=pltpu.VMEM)
    return pl.pallas_call(
        functools.partial(exchange_kernel, n_tensor, topk, cap, fc),
        name="exchange",
        out_shape=[
            pltpu.VMEM((1, 2, ff, part), F32),
            pltpu.VMEM((1, ff, part), F32),
            pltpu.VMEM((rows, width), F32),
        ],
        in_specs=[hbm] * 9,
        out_specs=[vmem] * 3,
        scratch_shapes=[
            pltpu.VMEM((nch, 3, 2, fc, part), BF),
            pltpu.VMEM((2, 2, 3, rows, part), BF),
            pltpu.VMEM((2, 2, 2 * topk, rows), F32),
            pltpu.VMEM((2, 2, rows, rows), BF),
            pltpu.VMEM((2, 2, 2, cap, part), BF),
            pltpu.VMEM((2, 2 * cap, part), BF),
            pltpu.VMEM((2, nch, cap, 6 * fc), BF),
            pltpu.VMEM((2, nch, cap, 6 * fc), BF),
            pltpu.VMEM((2, 2, nch, 2, cap, 2 * fc), BF),
            pltpu.VMEM((2, nch, 2 * cap, fc), BF),
            pltpu.VMEM((2, 2, cap, part), F32),
            pltpu.VMEM((parts, rows // 2, part), F32),
            pltpu.VMEM((2, parts, rows // 2, part), BF),
            pltpu.VMEM((2, parts, rows // 2, part), BF),
            pltpu.VMEM((2, parts, n_tensor, few, part), BF),
            pltpu.VMEM((2, parts, peers, few, part), BF),
            pltpu.VMEM((parts, few, part), BF),
            pltpu.VMEM((2, parts, n_tensor // 2, 2, few, part), BF),
            pltpu.VMEM((topk, rows), jnp.int32),
            pltpu.SemaphoreType.REGULAR((n_tensor.bit_length(),)),
            pltpu.SemaphoreType.REGULAR,
            pltpu.VMEM((3, rows // n_tensor, part), BF),
            dma((nch,)), dma((4,)),
            dma((2,)), dma((2,)), dma((2,)), dma((2,)), dma, dma, dma((2,)), dma((2,)),
            dma, dma((2, nch)), dma, dma((3, nch)), dma, dma,
            dma((2, parts)), dma((2, parts)), dma((2,)), dma((2, parts)),
            dma, dma, dma, dma, dma, dma, dma, dma,
        ],
        compiler_params=pltpu.CompilerParams(
            collective_id=0, has_side_effects=True, vmem_limit_bytes=44 * 1024 * 1024
        ),
    )(*[pltpu.with_memory_space_constraint(v, pltpu.HBM) for v in args])


def store_kernel(hin_v, hout_v, tok_v, hin_o, hout_o, tok_o, sem):
    ff = hin_v.shape[2]
    step = ff // 3
    copies = []
    for i in range(3):
        span = pl.ds(i * step, step)
        copies += [(hin_v.at[0, g, span], hin_o.at[0, g, span]) for g in range(2)]
        copies.append((hout_v.at[0, span], hout_o.at[0, span]))
    copies.append((tok_v, tok_o))
    copies = [pltpu.make_async_copy(src, dst, sem.at[i]) for i, (src, dst) in enumerate(copies)]
    for c in copies:
        c.start()
    for c in copies:
        c.wait()


def store(*results):
    return pl.pallas_call(
        store_kernel,
        name="store",
        out_shape=[pltpu.HBM(v.shape, v.dtype) for v in results],
        in_specs=[pl.BlockSpec(memory_space=pltpu.VMEM)] * 3,
        out_specs=[pl.BlockSpec(memory_space=pltpu.HBM)] * 3,
        scratch_shapes=[pltpu.SemaphoreType.DMA((10,))],
        compiler_params=pltpu.CompilerParams(vmem_limit_bytes=4 * 1024 * 1024),
    )(*[pltpu.with_memory_space_constraint(v, pltpu.VMEM) for v in results])


def kernel_shards(tokens, tangent, cotangent, expert_ids, gates, w_in, v_in, w_out, v_out):
    rows, _ = tokens.shape
    topk = expert_ids.shape[1]
    all_experts = lax.axis_size("tensor") * lax.axis_size("expert")
    cap = min(rows, 3 * rows * topk // (2 * all_experts))
    args = (tokens, tangent, cotangent, expert_ids.T, gates.T, w_in, v_in, w_out, v_out)
    hvp_in, hvp_out, out = exchange(args, cap, 128)
    hvp_in, hvp_out, out = store(hvp_in, hvp_out, out)
    return out, hvp_in, hvp_out


def shards(*args):
    tokens, expert_ids, w_in = args[0], args[3], args[5]
    n_tensor = lax.axis_size("tensor")
    rows, topk = expert_ids.shape
    fits = (
        lax.axis_size("expert") == 2 and lax.axis_size("dp") == 2 and w_in.shape[0] == 1
        and tokens.shape[1] == 2 * w_in.shape[3] and w_in.shape[3] % 128 == 0 and w_in.shape[2] % 256 == 0
        and rows == 128 and n_tensor > 2 and n_tensor & (n_tensor - 1) == 0 and rows % (16 * n_tensor) == 0
        and topk % 8 == 0 and (3 * rows * topk) % (64 * n_tensor) == 0 and 3 * topk > 2 * n_tensor
    )
    return (kernel_shards if fits else plain_shards)(*args)


def solution(mesh):
    rows = P(("expert", "dp"), None)
    wide = P(("tensor", "expert"), None, None, "dp")
    tall = P(("tensor", "expert"), None, "dp")
    return jax.shard_map(
        shards,
        mesh=mesh,
        in_specs=(rows, rows, rows, rows, rows, wide, wide, tall, tall),
        out_specs=(rows, wide, tall),
        check_vma=False,
    )
```

```python
import functools

import jax
import jax.numpy as jnp
from jax import lax
from jax.experimental import pallas as pl
from jax.experimental.pallas import tpu as pltpu
from jax.sharding import PartitionSpec as P


BF = jnp.bfloat16
F32 = jnp.float32
MESH = pl.DeviceIdType.MESH


def dot_nt(x, w):
    return lax.dot_general(x, w, (((1,), (1,)), ((), ())), preferred_element_type=F32)


def dot_nn(x, w):
    return lax.dot_general(x, w, (((1,), (0,)), ((), ())), preferred_element_type=F32)


def dot_tn(x, w):
    return lax.dot_general(x, w, (((0,), (0,)), ((), ())), preferred_element_type=F32)


def sum_over(own, axis, sent, ahead=None):
    n = lax.axis_size(axis)
    if n & (n - 1):
        return lax.psum(own.astype(BF), axis).astype(F32)
    step = 1
    while step < n:
        give = own.astype(BF)
        if step == 1:
            sent.append(give)
        got = lax.ppermute(give, axis, [(i, i ^ step) for i in range(n)])
        if ahead is not None:
            got, ahead = lax.optimization_barrier((got, ahead))
        own = own + got.astype(F32)
        step *= 2
    return own


def hidden_terms(pre, pre_dot, backs):
    half = pre.shape[1] // 2
    gate_pre, up_val = pre[:, :half], pre[:, half:]
    gate_dot, up_dot = pre_dot[:, :half], pre_dot[:, half:]
    back, back_dot = backs[:, :half], backs[:, half:]
    sigma = jax.nn.sigmoid(gate_pre)
    silu_val = gate_pre * sigma
    first = sigma * (1.0 + gate_pre * (1.0 - sigma))
    second = sigma * (1.0 - sigma) * (2.0 + gate_pre * (1.0 - 2.0 * sigma))
    grad_a = back * up_val * first
    grad_b = back * silu_val
    tang_a = back_dot * up_val * first + back * up_dot * first + back * up_val * second * gate_dot
    tang_b = back_dot * silu_val + back * first * gate_dot
    hidden_dot = first * gate_dot * up_val + silu_val * up_dot
    grads = jnp.concatenate([grad_a, grad_b], axis=1).astype(BF)
    tangs = jnp.concatenate([tang_a, tang_b], axis=1).astype(BF)
    return grads, tangs, hidden_dot.astype(BF)


def plain_shards(tokens, tangent, cotangent, expert_ids, gates, w_in, v_in, w_out, v_out):
    n_tensor = lax.axis_size("tensor")
    n_expert = lax.axis_size("expert")
    n_dp = lax.axis_size("dp")
    rank, core = lax.axis_index("tensor"), lax.axis_index("expert")
    held, _, ff, part = w_in.shape
    all_experts = held * n_tensor * n_expert
    rows, width = tokens.shape
    topk = expert_ids.shape[1]
    cap = min(rows, 3 * rows * topk // (2 * all_experts))

    around = [
        [((i + r) % n_expert, i) for i in range(n_expert)] for r in range(n_expert)
    ]

    def from_cores(v):
        return [v] + [lax.ppermute(v, "expert", around[r]) for r in range(1, n_expert)]

    fields = (tokens, tangent, cotangent)
    if n_dp == 2:
        low_half = [v[:, :part] for v in fields]
        high_half = [v[:, part:] for v in fields]
        first = lax.axis_index("dp") == 0
        give = jnp.where(first, jnp.concatenate(high_half, axis=1), jnp.concatenate(low_half, axis=1))
        keep = jnp.where(first, jnp.concatenate(low_half, axis=1), jnp.concatenate(high_half, axis=1))
        other = lax.ppermute(give, "dp", [(0, 1), (1, 0)])
        keeps, others = jnp.stack(from_cores(keep)), jnp.stack(from_cores(other))
        blocks = [jnp.where(first, keeps, others), jnp.where(first, others, keeps)]
    else:
        mine = lax.all_to_all(jnp.stack(fields, axis=1), "dp", split_axis=2, concat_axis=0, tiled=True)
        mine = mine.reshape(n_dp, rows, 3 * part)
        blocks = jnp.stack(from_cores(mine), axis=1)

    names = jnp.arange(all_experts, dtype=jnp.int32)
    hit = names[:, None, None] == expert_ids.T[None]
    table = jnp.sum(jnp.where(hit, gates.T[None], 0.0), axis=1)
    table = jnp.where(jnp.any(hit, axis=1), table, -1.0)
    tables = jnp.broadcast_to(table[None], (n_expert * n_dp, all_experts, rows))
    tables = lax.all_to_all(tables, ("expert", "dp"), split_axis=0, concat_axis=0, tiled=True)
    tables = tables.reshape(n_expert, n_dp, all_experts, rows)

    low = jnp.tril(jnp.ones((rows, rows), BF))
    weights = [
        (
            w_in[l].reshape(2 * ff, part),
            v_in[l].reshape(2 * ff, part),
            w_out[l],
            v_out[l],
        )
        for l in range(held)
    ]

    def replica(c, before=None):
        saved, spread, sent = [], [0.0] * n_expert, []
        block, ahead = blocks[c], None
        if before is not None:
            block, _ = lax.optimization_barrier((block, before[2]))
            ahead = before[0]
        for l in range(held):
            wi, vi, wo, vo = weights[l]
            expert = (rank * n_expert + core) * held + l
            picks, scales = [], []
            for r in range(n_expert):
                gate = tables[lax.rem(core + r, n_expert), c, expert]
                on = gate >= 0.0
                slot = dot_nt(on.astype(BF)[None, :], low)[0].astype(jnp.int32) - 1
                pick = (jnp.arange(cap, dtype=jnp.int32)[:, None] == slot[None, :]) & on[None, :]
                scales.append(jnp.sum(jnp.where(pick, gate[None, :], 0.0), axis=1))
                picks.append(pick.astype(BF))
            chosen = jnp.einsum(
                "rst,rtd->rsd", jnp.stack(picks), block, preferred_element_type=F32
            ).reshape(n_expert * cap, 3 * part)
            x = chosen[:, :part].astype(BF)
            u = chosen[:, part:2 * part].astype(BF)
            dy = (jnp.concatenate(scales)[:, None] * chosen[:, 2 * part:]).astype(BF)
            pre = sum_over(dot_nt(x, wi), "dp", sent)
            pre_dot = sum_over(dot_nt(u, wi) + dot_nt(x, vi), "dp", sent)
            backs = sum_over(jnp.concatenate([dot_nt(dy, wo), dot_nt(dy, vo)], axis=1), "dp", sent, ahead)
            grads, tangs, hidden = hidden_terms(pre, pre_dot, backs)
            saved.append((x, u, dy, grads, tangs, hidden))
            partial = (dot_nn(tangs, wi) + dot_nn(grads, vi)).astype(BF)
            for r, pick in enumerate(picks):
                spread[r] = spread[r] + dot_tn(pick, partial[r * cap:(r + 1) * cap])
        total = spread[0]
        for r in range(1, n_expert):
            moved = [(i, (i + r) % n_expert) for i in range(n_expert)]
            total = total + lax.ppermute(spread[r].astype(BF), "expert", moved).astype(F32)
        total = total.reshape(n_tensor, rows // n_tensor, part).astype(BF)
        got = lax.all_to_all(total, "tensor", split_axis=0, concat_axis=0, tiled=True)
        return jnp.sum(got.astype(F32), axis=0).astype(BF), saved, sent

    if n_dp <= 2:
        done = [replica(0)]
        for c in range(1, n_dp):
            done.append(replica(c, done[-1]))
        share, saved = jax.tree.map(lambda *v: jnp.stack(v), *[d[:2] for d in done])
    else:
        share, saved = lax.map(lambda c: replica(c)[:2], jnp.arange(n_dp))

    hvp_in, hvp_out = [], []
    for l in range(held):
        x, u, dy, grads, tangs, hidden = (v.reshape(-1, v.shape[-1]) for v in saved[l])
        both = jnp.concatenate([grads, tangs], axis=0)
        hvp_in.append(dot_tn(both, jnp.concatenate([u, x], axis=0)).reshape(2, ff, part))
        hvp_out.append(dot_tn(hidden, dy))

    share = jnp.broadcast_to(share[None], (n_tensor,) + share.shape)
    share = share.reshape((n_tensor * n_dp,) + share.shape[2:])
    share = lax.all_to_all(share, ("tensor", "dp"), split_axis=0, concat_axis=0, tiled=True)
    share = share.reshape(n_tensor, n_dp, rows // n_tensor, part).transpose(0, 2, 1, 3)
    hvp_tokens = share.reshape(rows, width).astype(F32)
    return hvp_tokens, jnp.stack(hvp_in), jnp.stack(hvp_out)


def remote(src, dst, send, recv, where):
    return pltpu.make_async_remote_copy(
        src_ref=src, dst_ref=dst, send_sem=send, recv_sem=recv, device_id=where, device_id_type=MESH
    )


def aligned(index, size):
    return pl.ds(pl.multiple_of(index * size, size), size)


def exchange_kernel(
    n_tensor, topk, cap, fc,
    tok_h, tan_h, cot_h, ids_h, gates_h, w_h, v_h, wo_h, vo_h,
    hin_o, hout_o, tok_o,
    wvo_s, tok_s, info_s, pick_s, rows_s, dy_s, send_s, recv_s, fing_s, finh_s,
    part_s, own_s, give_s, core_s, sum_s, slice_s, share_s, ready_s, ids_s, near_s, go_s, lead_s,
    wsem, lsem, c1s, c1r, c2s, c2r, c3s, c3r, c4s, c4r, c5s, c5r, c6s, c6r, c7s, c7r,
    as_, ar_, bs_, br_, cs_, cr_, ys_, yr_, zs_, zr_, xs_, xr_, ks_, kr_,
):
    t, e, p = lax.axis_index("tensor"), lax.axis_index("expert"), lax.axis_index("dp")
    q, other = 1 - p, 1 - e
    tz, tx = t // 2, lax.rem(t, 2)
    core, over = {"expert": other}, {"dp": q}
    rows, part = tok_s.shape[3], tok_s.shape[4]
    nch, early = wvo_s.shape[0], rows // 2
    half = nch // 2
    few, parts = rows // n_tensor, 2
    spans = ((0, early), (early, cap))
    mine, theirs = aligned(p, part), aligned(q, part)
    fields = (tan_h, tok_h, cot_h)
    steps = [1 << k for k in range(n_tensor.bit_length() - 1)]
    plane = [{"tensor": lax.rem(t + k, n_tensor)} for k in range(1, n_tensor)]
    peers = [lax.rem(t + k, n_tensor) for k in range(1, n_tensor)]
    slice_t = aligned(t, few)

    barrier = pltpu.get_barrier_semaphore()
    near = [{"tensor": lax.rem(t // step + 1, 2) * step + lax.rem(t, step) + t // (2 * step) * (2 * step)} for step in steps]
    for where in [core, over] + near:
        pl.semaphore_signal(barrier, inc=1, device_id=where, device_id_type=MESH)

    lead = [pltpu.make_async_copy(h.at[slice_t, theirs], lead_s.at[i], lsem.at[3]) for i, h in enumerate(fields)]
    table = [
        pltpu.make_async_copy(ids_h, ids_s, lsem.at[1]),
        pltpu.make_async_copy(gates_h, info_s.at[0, e, pl.ds(topk, topk)], lsem.at[2]),
    ]
    local = [pltpu.make_async_copy(h.at[:, mine], tok_s.at[0, e, i], lsem.at[0]) for i, h in enumerate(fields)]
    for c in lead + table + local:
        c.start()

    def load_weights(f, _):
        part_f = aligned(f, fc)
        pltpu.make_async_copy(w_h.at[0, :, part_f, :], wvo_s.at[f, 0], wsem.at[f]).start()
        pltpu.make_async_copy(v_h.at[0, :, part_f, :], wvo_s.at[f, 1], wsem.at[f]).start()
        pltpu.make_async_copy(wo_h.at[0, part_f, :], wvo_s.at[f, 2, 0], wsem.at[f]).start()
        pltpu.make_async_copy(vo_h.at[0, part_f, :], wvo_s.at[f, 2, 1], wsem.at[f]).start()
        return 0

    def wait_weights(f):
        pltpu.make_async_copy(wvo_s.at[f], wvo_s.at[f], wsem.at[f]).wait()

    lax.fori_loop(0, nch, load_weights, 0)


    expert = (t * 2 + e).astype(F32)
    low = (
        lax.broadcasted_iota(jnp.int32, (rows, rows), 0) > lax.broadcasted_iota(jnp.int32, (rows, rows), 1)
    ).astype(F32).astype(BF)
    lane = lax.broadcasted_iota(jnp.int32, (rows, rows), 1).astype(F32)

    def gather(rep, s):
        info = info_s[rep, s].T
        hit = info[:, :topk] == expert
        on = jnp.sum(jnp.where(hit, 1.0, 0.0), axis=1, keepdims=True)
        gate = jnp.sum(jnp.where(hit, info[:, topk:], 0.0), axis=1, keepdims=True)
        on = jnp.broadcast_to(on, (rows, rows))
        slot = dot_nn(low, on.astype(BF))
        pick = jnp.where((slot == lane) & (on > 0.5), 1.0, 0.0)
        pick_s[rep, s] = pick.astype(BF)
        pick = pick.T.astype(BF)[:cap]
        rows_s[rep, s, 0] = dot_nn(pick, tok_s[rep, s, 0]).astype(BF)
        rows_s[rep, s, 1] = dot_nn(pick, tok_s[rep, s, 1]).astype(BF)
        scaled = (gate * tok_s[rep, s, 2].astype(F32)).astype(BF)
        dy_s[rep, aligned(s, cap)] = dot_nn(pick, scaled).astype(BF)

    def products(rep, s, f):
        w = wvo_s[f, 0].reshape(2 * fc, part)
        v = wvo_s[f, 1].reshape(2 * fc, part)
        o = wvo_s[f, 2].reshape(2 * fc, part)
        both = dot_nt(rows_s[rep, s].reshape(2 * cap, part), w)
        return both[cap:], both[:cap] + dot_nt(rows_s[rep, s, 1], v), dot_nt(dy_s[rep, aligned(s, cap)], o)

    def chunk_copy(s, f):
        return remote(send_s.at[s, f], recv_s.at[s, f], c5s, c5r.at[s, f], over)

    def make_chunk(s, f):
        pre, pre_dot, back = products(0, s, f)
        send_s[s, f, :, :2 * fc] = pre.astype(BF)
        send_s[s, f, :, 2 * fc:4 * fc] = pre_dot.astype(BF)
        send_s[s, f, :, 4 * fc:] = back.astype(BF)

    for c in table:
        c.wait()
    pltpu.make_async_copy(lead_s, lead_s, lsem.at[3]).wait()
    info_s[0, e, :topk, :] = ids_s[...].astype(F32)
    pl.semaphore_wait(barrier, 2 + len(near))

    def tell_near(r):
        for where in near:
            pl.semaphore_signal(near_s.at[r], inc=1, device_id=where, device_id_type=MESH)

    tell_near(0)
    tok_slice = tok_s.at[1, e, :, slice_t]
    cross = [
        remote(lead_s, tok_slice, c2s.at[0], c2r.at[0], over),
        remote(info_s.at[0, e], info_s.at[1, e], c2s.at[1], c2r.at[1], over),
    ]
    first = [
        remote(tok_s.at[0, e], tok_s.at[0, e], c1s.at[0], c1r.at[0], core),
        remote(info_s.at[0, e], info_s.at[0, e], c1s.at[1], c1r.at[1], core),
    ]
    for c in cross:
        c.start()
    pltpu.make_async_copy(tok_s.at[0, e], tok_s.at[0, e], lsem.at[0]).wait()
    for c in first:
        c.start()
    gather(0, e)
    wait_weights(0)
    make_chunk(e, 0)

    chunk_copy(e, 0).start()

    def send_own(f, _):
        wait_weights(f)
        make_chunk(e, f)
        chunk_copy(e, f).start()
        return 0

    lax.fori_loop(1, nch, send_own, 0)
    for r in range(len(near) - 1):
        pl.semaphore_wait(near_s.at[r], len(near))
        if r + 2 < len(near):
            tell_near(r + 1)
    for c in first:
        c.wait_recv()
    gather(0, other)

    for c in cross:
        c.wait_recv()
    line_sems = (c3s.at[0], c3r.at[0])
    for k in range(2, n_tensor, 2):
        remote(tok_slice, tok_slice, *line_sems, {"tensor": lax.rem(t + k, n_tensor)}).start()

    def send_other(f, _):
        make_chunk(other, f)
        chunk_copy(other, f).start()
        return 0

    lax.fori_loop(0, half, send_other, 0)
    tok_line = tok_s.at[1, e, :, pl.ds(0, rows // 2 - few)]
    tok_lines = remote(tok_line, tok_line, *line_sems, core)
    tok_lines.wait_recv()
    for k in range(n_tensor // 2):
        piece = tok_s.at[1, e, :, aligned(2 * k + tx, few)]
        remote(piece, piece, c3s.at[1], c3r.at[1], near[0]).start()
    lax.fori_loop(half, nch, send_other, 0)
    tok_half = tok_s.at[1, e, :, pl.ds(0, rows // 2)]
    tok_halves = remote(tok_half, tok_half, c3s.at[1], c3r.at[1], core)
    tok_halves.wait_recv()
    passed = [
        remote(tok_s.at[1, e], tok_s.at[1, e], c4s.at[0], c4r.at[0], core),
        remote(info_s.at[1, e], info_s.at[1, e], c4s.at[1], c4r.at[1], core),
    ]
    for c in passed:
        c.start()
    gather(1, e)
    for c in passed:
        c.wait_recv()
    gather(1, other)

    def back_rows(rep, s, f, lo, hi):
        w = wvo_s[f, 0].reshape(2 * fc, part)
        v = wvo_s[f, 1].reshape(2 * fc, part)
        return dot_nn(fing_s[rep, f, 1, s, lo:hi], w) + dot_nn(fing_s[rep, f, 0, s, lo:hi], v)

    def both_rows(f):
        w = wvo_s[f, 0].reshape(2 * fc, part)
        v = wvo_s[f, 1].reshape(2 * fc, part)
        grads, tangs = (fing_s[1, f, g].reshape(2 * cap, 2 * fc) for g in range(2))
        return (dot_nn(tangs, w) + dot_nn(grads, v)).reshape(2, cap, part)

    def grads_copy(f):
        return remote(fing_s.at[1, f, :, 0], fing_s.at[0, f, :, 0], c6s, c6r.at[2, f], over)

    def rows_copy(h, f):
        lo, hi = spans[h]
        span = pl.ds(lo, hi - lo)
        return remote(fing_s.at[1, f, :, 1, span], fing_s.at[0, f, :, 1, span], c6s, c6r.at[h, f], over)

    part_s[...] = jnp.zeros_like(part_s)

    def finish_chunk(i, _):
        s, f = lax.rem(e + i // nch, 2), lax.rem(i, nch)
        pre, pre_dot, back = products(1, s, f)
        chunk_copy(s, f).wait_recv()
        pre = pre + recv_s[s, f, :, :2 * fc].astype(F32)
        pre_dot = pre_dot + recv_s[s, f, :, 2 * fc:4 * fc].astype(F32)
        back = back + recv_s[s, f, :, 4 * fc:].astype(F32)
        grads, tangs, hidden = hidden_terms(pre, pre_dot, back)
        fing_s[1, f, 0, s] = grads
        fing_s[1, f, 1, s] = tangs
        finh_s[1, f, aligned(s, cap)] = hidden

        @pl.when(s == 0)
        def _():
            grads_copy(f).start()

        @pl.when(i >= nch)
        def _():
            part_s[1] += both_rows(f)

        return 0

    lax.fori_loop(0, 2 * nch, finish_chunk, 0)

    def give_back(h):
        def body(f, _):
            rows_copy(h, f).start()
            return 0

        return body

    lax.fori_loop(0, 3, give_back(0), 0)

    def spread(rep, s, h):
        hi = spans[h][1]
        return dot_nn(pick_s[rep, s, h * early:(h + 1) * early, :hi], part_s[rep, s, :hi].astype(BF))

    def core_copy(rep, h):
        return remote(give_s.at[rep, h], core_s.at[rep, h], as_.at[rep, h], ar_.at[rep, h], core)

    def give_core(rep, s, h):
        give_s[rep, h] = spread(rep, s, h).astype(BF)
        core_copy(rep, h).start()

    def over_cores(rep, h):
        core_copy(rep, h).wait_recv()
        both = own_s[h] + core_s[rep, h].astype(F32)
        sum_s[rep, h] = both.reshape(sum_s.shape[2:]).astype(BF)
        for k, (peer, where) in enumerate(zip(peers, plane)):
            remote(sum_s.at[rep, h, peer], slice_s.at[rep, h, k], bs_.at[rep], br_.at[rep, h], where).start()

    def over_plane(rep, h):
        remote(slice_s.at[rep, h], slice_s.at[rep, h], bs_.at[rep], br_.at[rep, h], core).wait_recv()
        total = sum_s[rep, h, t].astype(F32)
        for k in range(n_tensor - 1):
            total = total + slice_s[rep, h, k].astype(F32)
        return total.astype(BF)

    def in_term(rep, s, f):
        g = fing_s[rep, f, :, s].reshape(2 * cap, 2 * fc)
        return dot_tn(g, rows_s[rep, s].reshape(2 * cap, part)).reshape(2, fc, part)

    def out_term(rep, f):
        return dot_tn(finh_s[rep, f], dy_s[rep])

    def start_weights(f, _):
        part_f = aligned(f, fc)
        hin_o[0, :, part_f, :] = in_term(1, 0, f) + in_term(1, 1, f)
        hout_o[0, part_f, :] = out_term(1, f)
        return 0

    for h in range(parts):
        give_core(1, other, h)
    for h in range(parts):
        own_s[h] = spread(1, e, h)
    lax.fori_loop(0, half, start_weights, 0)
    for h in range(parts):
        over_cores(1, h)
    lax.fori_loop(half, nch, start_weights, 0)
    def take_first(f, _):
        grads_copy(f).wait_recv()
        part_s[0, 0] += back_rows(0, 0, f, 0, cap)
        hin_o[0, :, aligned(f, fc), :] += in_term(0, 0, f)
        return 0

    def take_second(h):
        lo, hi = spans[h]

        def body(f, _):
            rows_copy(h, f).wait_recv()
            part_s[0, 1, lo:hi] += back_rows(0, 1, f, lo, hi)
            return 0

        return body

    def to_owner(s, h):
        @pl.when(e != s)
        def _():
            give_core(0, s, h)

        @pl.when(e == s)
        def _():
            own_s[h] = spread(0, s, h)

    def owner_sums(s, h):
        @pl.when(e == s)
        def _():
            over_cores(0, h)

    def owner_shares(s, h):
        @pl.when(e == s)
        def _():
            ready_s[0, h, tz, tx] = over_plane(0, h)
            mid = ready_s.at[0, h, tz, tx]
            if s == 0:
                for k in range(2, n_tensor, 2):
                    remote(mid, mid, ks_.at[0], kr_.at[0], {"tensor": lax.rem(t + k, n_tensor)}).start()
            else:
                for where in plane:
                    remote(mid, mid, cs_, cr_, where).start()

    def end_in(f, _):
        hin_o[0, :, aligned(f, fc), :] += in_term(0, 1, f)
        return 0

    def end_out(f, _):
        hout_o[0, aligned(f, fc), :] += out_term(0, f)
        return 0

    lax.fori_loop(0, nch, take_first, 0)
    for h in range(parts):
        to_owner(0, h)
    for h in range(parts):
        share_s[h] = over_plane(1, h)
    share_copy = remote(share_s, ready_s.at[1, :, tz, tx], ys_, yr_, over)
    share_copy.start()
    lax.fori_loop(3, nch, give_back(0), 0)

    @pl.when(e == 0)
    def _():
        lax.fori_loop(0, nch, give_back(1), 0)

    hidden = remote(finh_s.at[1], finh_s.at[0], c7s, c7r, over)

    for h in range(parts):
        owner_sums(0, h)
    share_copy.wait_recv()
    for k in range(2, n_tensor, 2):
        mid = ready_s.at[1, :, tz, tx]
        remote(mid, mid, zs_, zr_, {"tensor": lax.rem(t + k, n_tensor)}).start()
    lax.fori_loop(0, nch - 1, take_second(0), 0)

    @pl.when(e == 0)
    def _():
        pl.semaphore_signal(go_s, inc=1, device_id=core, device_id_type=MESH)

    lax.fori_loop(nch - 1, nch, take_second(0), 0)
    to_owner(1, 0)

    @pl.when(e == 1)
    def _():
        pl.semaphore_wait(go_s, 1)
        lax.fori_loop(0, nch, give_back(1), 0)
        hidden.start()

    line = ready_s.at[1, :, pl.ds(0, n_tensor // 2 - 1), tx]
    lines = remote(line, line, zs_, zr_, core)
    lines.wait_recv()
    column = ready_s.at[1, :, :, tx]
    columns = remote(column, column, xs_, xr_, near[0])
    columns.start()
    for h in range(parts):
        owner_shares(0, h)
    owner_sums(1, 0)
    lax.fori_loop(0, nch, take_second(1), 0)
    to_owner(1, 1)

    line = ready_s.at[0, :, pl.ds(0, n_tensor // 2 - 1), tx]
    column = ready_s.at[0, :, :, tx]
    owner_lines = remote(line, line, ks_.at[0], kr_.at[0], core)
    owner_columns = remote(column, column, ks_.at[1], kr_.at[1], near[0])

    @pl.when(e == 0)
    def _():
        owner_lines.wait_recv()
        owner_columns.start()

    owner_sums(1, 1)
    lax.fori_loop(0, nch, end_in, 0)
    pl.when(e == 0)(hidden.start)
    owner_shares(1, 0)

    owner_shares(1, 1)
    hidden.wait_recv()
    lax.fori_loop(0, nch, end_out, 0)
    owner_slices = remote(slice_s.at[0], slice_s.at[0], cs_, cr_, core)
    columns.wait_recv()
    pl.when(e == 0)(owner_columns.wait_recv)
    pl.when(e == 1)(owner_slices.wait_recv)
    tok_o[:, mine] = ready_s[0].astype(F32).reshape(rows, part)
    tok_o[:, theirs] = ready_s[1].astype(F32).reshape(rows, part)

    for c in first + cross + [tok_lines, tok_halves] + passed + [columns, lines, share_copy]:
        c.wait_send()

    @pl.when(e == 0)
    def _():
        owner_lines.wait_send()
        owner_columns.wait_send()

    pl.when(e == 1)(owner_slices.wait_send)
    for r in range(2):
        for h in range(parts):
            core_copy(r, h).wait_send()
        remote(slice_s.at[r], slice_s.at[r], bs_.at[r], br_.at[r, 0], core).wait_send()
    remote(send_s, send_s, c5s, c5r.at[0, 0], over).wait_send()
    remote(fing_s.at[1], fing_s.at[1], c6s, c6r.at[0, 0], over).wait_send()
    hidden.wait_send()


def exchange(args, cap, fc):
    tokens, ids, w_in = args[0], args[3], args[5]
    n_tensor = lax.axis_size("tensor")
    rows, width = tokens.shape
    _, _, ff, part = w_in.shape
    topk = ids.shape[0]
    nch, peers, parts = ff // fc, n_tensor - 1, 2
    few = rows // n_tensor // parts
    dma = pltpu.SemaphoreType.DMA
    hbm = pl.BlockSpec(memory_space=pltpu.HBM)
    vmem = pl.BlockSpec(memory_space=pltpu.VMEM)
    return pl.pallas_call(
        functools.partial(exchange_kernel, n_tensor, topk, cap, fc),
        name="exchange",
        out_shape=[
            pltpu.VMEM((1, 2, ff, part), F32),
            pltpu.VMEM((1, ff, part), F32),
            pltpu.VMEM((rows, width), F32),
        ],
        in_specs=[hbm] * 9,
        out_specs=[vmem] * 3,
        scratch_shapes=[
            pltpu.VMEM((nch, 3, 2, fc, part), BF),
            pltpu.VMEM((2, 2, 3, rows, part), BF),
            pltpu.VMEM((2, 2, 2 * topk, rows), F32),
            pltpu.VMEM((2, 2, rows, rows), BF),
            pltpu.VMEM((2, 2, 2, cap, part), BF),
            pltpu.VMEM((2, 2 * cap, part), BF),
            pltpu.VMEM((2, nch, cap, 6 * fc), BF),
            pltpu.VMEM((2, nch, cap, 6 * fc), BF),
            pltpu.VMEM((2, nch, 2, 2, cap, 2 * fc), BF),
            pltpu.VMEM((2, nch, 2 * cap, fc), BF),
            pltpu.VMEM((2, 2, cap, part), F32),
            pltpu.VMEM((parts, rows // 2, part), F32),
            pltpu.VMEM((2, parts, rows // 2, part), BF),
            pltpu.VMEM((2, parts, rows // 2, part), BF),
            pltpu.VMEM((2, parts, n_tensor, few, part), BF),
            pltpu.VMEM((2, parts, peers, few, part), BF),
            pltpu.VMEM((parts, few, part), BF),
            pltpu.VMEM((2, parts, n_tensor // 2, 2, few, part), BF),
            pltpu.VMEM((topk, rows), jnp.int32),
            pltpu.SemaphoreType.REGULAR((n_tensor.bit_length(),)),
            pltpu.SemaphoreType.REGULAR,
            pltpu.VMEM((3, rows // n_tensor, part), BF),
            dma((nch,)), dma((4,)),
            dma((2,)), dma((2,)), dma((2,)), dma((2,)), dma((2,)), dma((2,)), dma((2,)), dma((2,)),
            dma, dma((2, nch)), dma, dma((3, nch)), dma, dma,
            dma((2, parts)), dma((2, parts)), dma((2,)), dma((2, parts)),
            dma, dma, dma, dma, dma, dma, dma, dma, dma((2,)), dma((2,)),
        ],
        compiler_params=pltpu.CompilerParams(
            collective_id=0, has_side_effects=True, vmem_limit_bytes=44 * 1024 * 1024
        ),
    )(*[pltpu.with_memory_space_constraint(v, pltpu.HBM) for v in args])


def store_kernel(hin_v, hout_v, tok_v, hin_o, hout_o, tok_o, sem):
    ff = hin_v.shape[2]
    step = ff // 3
    copies = []
    for i in range(3):
        span = pl.ds(i * step, step)
        copies += [(hin_v.at[0, g, span], hin_o.at[0, g, span]) for g in range(2)]
        copies.append((hout_v.at[0, span], hout_o.at[0, span]))
    copies.append((tok_v, tok_o))
    copies = [pltpu.make_async_copy(src, dst, sem.at[i]) for i, (src, dst) in enumerate(copies)]
    for c in copies:
        c.start()
    for c in copies:
        c.wait()


def store(*results):
    return pl.pallas_call(
        store_kernel,
        name="store",
        out_shape=[pltpu.HBM(v.shape, v.dtype) for v in results],
        in_specs=[pl.BlockSpec(memory_space=pltpu.VMEM)] * 3,
        out_specs=[pl.BlockSpec(memory_space=pltpu.HBM)] * 3,
        scratch_shapes=[pltpu.SemaphoreType.DMA((10,))],
        compiler_params=pltpu.CompilerParams(vmem_limit_bytes=4 * 1024 * 1024),
    )(*[pltpu.with_memory_space_constraint(v, pltpu.VMEM) for v in results])


def kernel_shards(tokens, tangent, cotangent, expert_ids, gates, w_in, v_in, w_out, v_out):
    rows, _ = tokens.shape
    topk = expert_ids.shape[1]
    all_experts = lax.axis_size("tensor") * lax.axis_size("expert")
    cap = min(rows, 3 * rows * topk // (2 * all_experts))
    args = (tokens, tangent, cotangent, expert_ids.T, gates.T, w_in, v_in, w_out, v_out)
    hvp_in, hvp_out, out = exchange(args, cap, 128)
    hvp_in, hvp_out, out = store(hvp_in, hvp_out, out)
    return out, hvp_in, hvp_out


def shards(*args):
    tokens, expert_ids, w_in = args[0], args[3], args[5]
    n_tensor = lax.axis_size("tensor")
    rows, topk = expert_ids.shape
    fits = (
        lax.axis_size("expert") == 2 and lax.axis_size("dp") == 2 and w_in.shape[0] == 1
        and tokens.shape[1] == 2 * w_in.shape[3] and w_in.shape[3] % 128 == 0 and w_in.shape[2] % 256 == 0
        and rows == 128 and n_tensor > 2 and n_tensor & (n_tensor - 1) == 0 and rows % (16 * n_tensor) == 0
        and topk % 8 == 0 and (3 * rows * topk) % (64 * n_tensor) == 0 and 3 * topk > 2 * n_tensor
    )
    return (kernel_shards if fits else plain_shards)(*args)


def solution(mesh):
    rows = P(("expert", "dp"), None)
    wide = P(("tensor", "expert"), None, None, "dp")
    tall = P(("tensor", "expert"), None, "dp")
    return jax.shard_map(
        shards,
        mesh=mesh,
        in_specs=(rows, rows, rows, rows, rows, wide, wide, tall, tall),
        out_specs=(rows, wide, tall),
        check_vma=False,
    )
```

```python
import functools

import jax
import jax.numpy as jnp
from jax import lax
from jax.experimental import pallas as pl
from jax.experimental.pallas import tpu as pltpu
from jax.sharding import PartitionSpec as P


BF = jnp.bfloat16
F32 = jnp.float32
MESH = pl.DeviceIdType.MESH


def dot_nt(x, w):
    return lax.dot_general(x, w, (((1,), (1,)), ((), ())), preferred_element_type=F32)


def dot_nn(x, w):
    return lax.dot_general(x, w, (((1,), (0,)), ((), ())), preferred_element_type=F32)


def dot_tn(x, w):
    return lax.dot_general(x, w, (((0,), (0,)), ((), ())), preferred_element_type=F32)


def sum_over(own, axis, sent, ahead=None):
    n = lax.axis_size(axis)
    if n & (n - 1):
        return lax.psum(own.astype(BF), axis).astype(F32)
    step = 1
    while step < n:
        give = own.astype(BF)
        if step == 1:
            sent.append(give)
        got = lax.ppermute(give, axis, [(i, i ^ step) for i in range(n)])
        if ahead is not None:
            got, ahead = lax.optimization_barrier((got, ahead))
        own = own + got.astype(F32)
        step *= 2
    return own


def hidden_terms(pre, pre_dot, backs):
    half = pre.shape[1] // 2
    gate_pre, up_val = pre[:, :half], pre[:, half:]
    gate_dot, up_dot = pre_dot[:, :half], pre_dot[:, half:]
    back, back_dot = backs[:, :half], backs[:, half:]
    sigma = jax.nn.sigmoid(gate_pre)
    silu_val = gate_pre * sigma
    first = sigma * (1.0 + gate_pre * (1.0 - sigma))
    second = sigma * (1.0 - sigma) * (2.0 + gate_pre * (1.0 - 2.0 * sigma))
    grad_a = back * up_val * first
    grad_b = back * silu_val
    tang_a = back_dot * up_val * first + back * up_dot * first + back * up_val * second * gate_dot
    tang_b = back_dot * silu_val + back * first * gate_dot
    hidden_dot = first * gate_dot * up_val + silu_val * up_dot
    grads = jnp.concatenate([grad_a, grad_b], axis=1).astype(BF)
    tangs = jnp.concatenate([tang_a, tang_b], axis=1).astype(BF)
    return grads, tangs, hidden_dot.astype(BF)


def plain_shards(tokens, tangent, cotangent, expert_ids, gates, w_in, v_in, w_out, v_out):
    n_tensor = lax.axis_size("tensor")
    n_expert = lax.axis_size("expert")
    n_dp = lax.axis_size("dp")
    rank, core = lax.axis_index("tensor"), lax.axis_index("expert")
    held, _, ff, part = w_in.shape
    all_experts = held * n_tensor * n_expert
    rows, width = tokens.shape
    topk = expert_ids.shape[1]
    cap = min(rows, 3 * rows * topk // (2 * all_experts))

    around = [
        [((i + r) % n_expert, i) for i in range(n_expert)] for r in range(n_expert)
    ]

    def from_cores(v):
        return [v] + [lax.ppermute(v, "expert", around[r]) for r in range(1, n_expert)]

    fields = (tokens, tangent, cotangent)
    if n_dp == 2:
        low_half = [v[:, :part] for v in fields]
        high_half = [v[:, part:] for v in fields]
        first = lax.axis_index("dp") == 0
        give = jnp.where(first, jnp.concatenate(high_half, axis=1), jnp.concatenate(low_half, axis=1))
        keep = jnp.where(first, jnp.concatenate(low_half, axis=1), jnp.concatenate(high_half, axis=1))
        other = lax.ppermute(give, "dp", [(0, 1), (1, 0)])
        keeps, others = jnp.stack(from_cores(keep)), jnp.stack(from_cores(other))
        blocks = [jnp.where(first, keeps, others), jnp.where(first, others, keeps)]
    else:
        mine = lax.all_to_all(jnp.stack(fields, axis=1), "dp", split_axis=2, concat_axis=0, tiled=True)
        mine = mine.reshape(n_dp, rows, 3 * part)
        blocks = jnp.stack(from_cores(mine), axis=1)

    names = jnp.arange(all_experts, dtype=jnp.int32)
    hit = names[:, None, None] == expert_ids.T[None]
    table = jnp.sum(jnp.where(hit, gates.T[None], 0.0), axis=1)
    table = jnp.where(jnp.any(hit, axis=1), table, -1.0)
    tables = jnp.broadcast_to(table[None], (n_expert * n_dp, all_experts, rows))
    tables = lax.all_to_all(tables, ("expert", "dp"), split_axis=0, concat_axis=0, tiled=True)
    tables = tables.reshape(n_expert, n_dp, all_experts, rows)

    low = jnp.tril(jnp.ones((rows, rows), BF))
    weights = [
        (
            w_in[l].reshape(2 * ff, part),
            v_in[l].reshape(2 * ff, part),
            w_out[l],
            v_out[l],
        )
        for l in range(held)
    ]

    def replica(c, before=None):
        saved, spread, sent = [], [0.0] * n_expert, []
        block, ahead = blocks[c], None
        if before is not None:
            block, _ = lax.optimization_barrier((block, before[2]))
            ahead = before[0]
        for l in range(held):
            wi, vi, wo, vo = weights[l]
            expert = (rank * n_expert + core) * held + l
            picks, scales = [], []
            for r in range(n_expert):
                gate = tables[lax.rem(core + r, n_expert), c, expert]
                on = gate >= 0.0
                slot = dot_nt(on.astype(BF)[None, :], low)[0].astype(jnp.int32) - 1
                pick = (jnp.arange(cap, dtype=jnp.int32)[:, None] == slot[None, :]) & on[None, :]
                scales.append(jnp.sum(jnp.where(pick, gate[None, :], 0.0), axis=1))
                picks.append(pick.astype(BF))
            chosen = jnp.einsum(
                "rst,rtd->rsd", jnp.stack(picks), block, preferred_element_type=F32
            ).reshape(n_expert * cap, 3 * part)
            x = chosen[:, :part].astype(BF)
            u = chosen[:, part:2 * part].astype(BF)
            dy = (jnp.concatenate(scales)[:, None] * chosen[:, 2 * part:]).astype(BF)
            pre = sum_over(dot_nt(x, wi), "dp", sent)
            pre_dot = sum_over(dot_nt(u, wi) + dot_nt(x, vi), "dp", sent)
            backs = sum_over(jnp.concatenate([dot_nt(dy, wo), dot_nt(dy, vo)], axis=1), "dp", sent, ahead)
            grads, tangs, hidden = hidden_terms(pre, pre_dot, backs)
            saved.append((x, u, dy, grads, tangs, hidden))
            partial = (dot_nn(tangs, wi) + dot_nn(grads, vi)).astype(BF)
            for r, pick in enumerate(picks):
                spread[r] = spread[r] + dot_tn(pick, partial[r * cap:(r + 1) * cap])
        total = spread[0]
        for r in range(1, n_expert):
            moved = [(i, (i + r) % n_expert) for i in range(n_expert)]
            total = total + lax.ppermute(spread[r].astype(BF), "expert", moved).astype(F32)
        total = total.reshape(n_tensor, rows // n_tensor, part).astype(BF)
        got = lax.all_to_all(total, "tensor", split_axis=0, concat_axis=0, tiled=True)
        return jnp.sum(got.astype(F32), axis=0).astype(BF), saved, sent

    if n_dp <= 2:
        done = [replica(0)]
        for c in range(1, n_dp):
            done.append(replica(c, done[-1]))
        share, saved = jax.tree.map(lambda *v: jnp.stack(v), *[d[:2] for d in done])
    else:
        share, saved = lax.map(lambda c: replica(c)[:2], jnp.arange(n_dp))

    hvp_in, hvp_out = [], []
    for l in range(held):
        x, u, dy, grads, tangs, hidden = (v.reshape(-1, v.shape[-1]) for v in saved[l])
        both = jnp.concatenate([grads, tangs], axis=0)
        hvp_in.append(dot_tn(both, jnp.concatenate([u, x], axis=0)).reshape(2, ff, part))
        hvp_out.append(dot_tn(hidden, dy))

    share = jnp.broadcast_to(share[None], (n_tensor,) + share.shape)
    share = share.reshape((n_tensor * n_dp,) + share.shape[2:])
    share = lax.all_to_all(share, ("tensor", "dp"), split_axis=0, concat_axis=0, tiled=True)
    share = share.reshape(n_tensor, n_dp, rows // n_tensor, part).transpose(0, 2, 1, 3)
    hvp_tokens = share.reshape(rows, width).astype(F32)
    return hvp_tokens, jnp.stack(hvp_in), jnp.stack(hvp_out)


def remote(src, dst, send, recv, where):
    return pltpu.make_async_remote_copy(
        src_ref=src, dst_ref=dst, send_sem=send, recv_sem=recv, device_id=where, device_id_type=MESH
    )


def aligned(index, size):
    return pl.ds(pl.multiple_of(index * size, size), size)


def exchange_kernel(
    n_tensor, topk, cap, fc,
    tok_h, tan_h, cot_h, ids_h, gates_h, w_h, v_h, wo_h, vo_h,
    hin_o, hout_o, tok_o,
    wvo_s, tok_s, info_s, pick_s, rows_s, dy_s, send_s, recv_s, fing_s, finh_s,
    part_s, own_s, give_s, core_s, sum_s, slice_s, share_s, ready_s, ids_s, near_s, go_s, lead_s,
    wsem, lsem, c1s, c1r, c2s, c2r, c3s, c3r, c4s, c4r, c5s, c5r, c6s, c6r, c7s, c7r,
    as_, ar_, bs_, br_, cs_, cr_, ys_, yr_, zs_, zr_, xs_, xr_,
):
    t, e, p = lax.axis_index("tensor"), lax.axis_index("expert"), lax.axis_index("dp")
    q, other = 1 - p, 1 - e
    tz, tx = t // 2, lax.rem(t, 2)
    core, over = {"expert": other}, {"dp": q}
    rows, part = tok_s.shape[3], tok_s.shape[4]
    nch, early = wvo_s.shape[0], rows // 2
    half = nch // 2
    few, parts = rows // n_tensor, 2
    spans = ((0, early), (early, cap))
    mine, theirs = aligned(p, part), aligned(q, part)
    fields = (tan_h, tok_h, cot_h)
    steps = [1 << k for k in range(n_tensor.bit_length() - 1)]
    plane = [{"tensor": lax.rem(t + k, n_tensor)} for k in range(1, n_tensor)]
    peers = [lax.rem(t + k, n_tensor) for k in range(1, n_tensor)]
    slice_t = aligned(t, few)

    barrier = pltpu.get_barrier_semaphore()
    near = [{"tensor": lax.rem(t // step + 1, 2) * step + lax.rem(t, step) + t // (2 * step) * (2 * step)} for step in steps]
    for where in [core, over] + near:
        pl.semaphore_signal(barrier, inc=1, device_id=where, device_id_type=MESH)

    local = [pltpu.make_async_copy(h.at[:, mine], tok_s.at[0, e, i], lsem.at[0]) for i, h in enumerate(fields)]
    local += [
        pltpu.make_async_copy(h.at[slice_t, theirs], lead_s.at[i], lsem.at[3]) for i, h in enumerate(fields)
    ]
    local.append(pltpu.make_async_copy(ids_h, ids_s, lsem.at[1]))
    local.append(pltpu.make_async_copy(gates_h, info_s.at[0, e, pl.ds(topk, topk)], lsem.at[2]))
    for c in local:
        c.start()

    def load_weights(f, _):
        part_f = aligned(f, fc)
        pltpu.make_async_copy(w_h.at[0, :, part_f, :], wvo_s.at[f, 0], wsem.at[f]).start()
        pltpu.make_async_copy(v_h.at[0, :, part_f, :], wvo_s.at[f, 1], wsem.at[f]).start()
        pltpu.make_async_copy(wo_h.at[0, part_f, :], wvo_s.at[f, 2, 0], wsem.at[f]).start()
        pltpu.make_async_copy(vo_h.at[0, part_f, :], wvo_s.at[f, 2, 1], wsem.at[f]).start()
        return 0

    def wait_weights(f):
        pltpu.make_async_copy(wvo_s.at[f], wvo_s.at[f], wsem.at[f]).wait()

    lax.fori_loop(0, nch, load_weights, 0)


    expert = (t * 2 + e).astype(F32)
    low = (
        lax.broadcasted_iota(jnp.int32, (rows, rows), 0) > lax.broadcasted_iota(jnp.int32, (rows, rows), 1)
    ).astype(F32).astype(BF)
    lane = lax.broadcasted_iota(jnp.int32, (rows, rows), 1).astype(F32)

    def gather(rep, s):
        info = info_s[rep, s].T
        hit = info[:, :topk] == expert
        on = jnp.sum(jnp.where(hit, 1.0, 0.0), axis=1, keepdims=True)
        gate = jnp.sum(jnp.where(hit, info[:, topk:], 0.0), axis=1, keepdims=True)
        on = jnp.broadcast_to(on, (rows, rows))
        slot = dot_nn(low, on.astype(BF))
        pick = jnp.where((slot == lane) & (on > 0.5), 1.0, 0.0)
        pick_s[rep, s] = pick.astype(BF)
        pick = pick.T.astype(BF)[:cap]
        rows_s[rep, s, 0] = dot_nn(pick, tok_s[rep, s, 0]).astype(BF)
        rows_s[rep, s, 1] = dot_nn(pick, tok_s[rep, s, 1]).astype(BF)
        scaled = (gate * tok_s[rep, s, 2].astype(F32)).astype(BF)
        dy_s[rep, aligned(s, cap)] = dot_nn(pick, scaled).astype(BF)

    def products(rep, s, f):
        w = wvo_s[f, 0].reshape(2 * fc, part)
        v = wvo_s[f, 1].reshape(2 * fc, part)
        o = wvo_s[f, 2].reshape(2 * fc, part)
        both = dot_nt(rows_s[rep, s].reshape(2 * cap, part), w)
        return both[cap:], both[:cap] + dot_nt(rows_s[rep, s, 1], v), dot_nt(dy_s[rep, aligned(s, cap)], o)

    def chunk_copy(s, f):
        return remote(send_s.at[s, f], recv_s.at[s, f], c5s, c5r.at[s, f], over)

    def make_chunk(s, f):
        pre, pre_dot, back = products(0, s, f)
        send_s[s, f, :, :2 * fc] = pre.astype(BF)
        send_s[s, f, :, 2 * fc:4 * fc] = pre_dot.astype(BF)
        send_s[s, f, :, 4 * fc:] = back.astype(BF)

    pltpu.make_async_copy(tok_s.at[0, e], tok_s.at[0, e], lsem.at[0]).wait()
    for c in local[6:]:
        c.wait()
    pltpu.make_async_copy(lead_s, lead_s, lsem.at[3]).wait()
    info_s[0, e, :topk, :] = ids_s[...].astype(F32)
    pl.semaphore_wait(barrier, 2 + len(near))

    def tell_near(r):
        for where in near:
            pl.semaphore_signal(near_s.at[r], inc=1, device_id=where, device_id_type=MESH)

    tell_near(0)
    tok_slice = tok_s.at[1, e, :, slice_t]
    cross = [
        remote(lead_s, tok_slice, c2s.at[0], c2r.at[0], over),
        remote(info_s.at[0, e], info_s.at[1, e], c2s.at[1], c2r.at[1], over),
    ]
    first = [
        remote(tok_s.at[0, e], tok_s.at[0, e], c1s.at[0], c1r.at[0], core),
        remote(info_s.at[0, e], info_s.at[0, e], c1s.at[1], c1r.at[1], core),
    ]
    for c in cross + first:
        c.start()
    gather(0, e)
    wait_weights(0)
    make_chunk(e, 0)

    chunk_copy(e, 0).start()

    def send_own(f, _):
        wait_weights(f)
        make_chunk(e, f)
        chunk_copy(e, f).start()
        return 0

    lax.fori_loop(1, nch, send_own, 0)
    for r in range(len(near) - 1):
        pl.semaphore_wait(near_s.at[r], len(near))
        if r + 2 < len(near):
            tell_near(r + 1)
    for c in first:
        c.wait_recv()
    gather(0, other)

    for c in cross:
        c.wait_recv()
    shared = [
        remote(tok_slice, tok_slice, c3s, c3r, where) for where in plane
    ]
    for c in shared:
        c.start()

    def send_other(f, _):
        make_chunk(other, f)
        chunk_copy(other, f).start()
        return 0

    lax.fori_loop(0, nch, send_other, 0)
    most = pl.ds(0, rows - few)
    tok_most = tok_s.at[1, e, :, most]
    shareds = remote(tok_most, tok_most, c3s, c3r, core)
    shareds.wait_recv()
    passed = [
        remote(tok_s.at[1, e], tok_s.at[1, e], c4s.at[0], c4r.at[0], core),
        remote(info_s.at[1, e], info_s.at[1, e], c4s.at[1], c4r.at[1], core),
    ]
    for c in passed:
        c.start()
    gather(1, e)
    for c in passed:
        c.wait_recv()
    gather(1, other)

    def back_rows(rep, s, f, lo, hi):
        w = wvo_s[f, 0].reshape(2 * fc, part)
        v = wvo_s[f, 1].reshape(2 * fc, part)
        return dot_nn(fing_s[rep, f, 1, s, lo:hi], w) + dot_nn(fing_s[rep, f, 0, s, lo:hi], v)

    def both_rows(f):
        w = wvo_s[f, 0].reshape(2 * fc, part)
        v = wvo_s[f, 1].reshape(2 * fc, part)
        grads, tangs = (fing_s[1, f, g].reshape(2 * cap, 2 * fc) for g in range(2))
        return (dot_nn(tangs, w) + dot_nn(grads, v)).reshape(2, cap, part)

    def grads_copy(f):
        return remote(fing_s.at[1, f, :, 0], fing_s.at[0, f, :, 0], c6s, c6r.at[2, f], over)

    def rows_copy(h, f):
        lo, hi = spans[h]
        span = pl.ds(lo, hi - lo)
        return remote(fing_s.at[1, f, :, 1, span], fing_s.at[0, f, :, 1, span], c6s, c6r.at[h, f], over)

    part_s[...] = jnp.zeros_like(part_s)

    def finish_chunk(i, _):
        s, f = lax.rem(e + i // nch, 2), lax.rem(i, nch)
        pre, pre_dot, back = products(1, s, f)
        chunk_copy(s, f).wait_recv()
        pre = pre + recv_s[s, f, :, :2 * fc].astype(F32)
        pre_dot = pre_dot + recv_s[s, f, :, 2 * fc:4 * fc].astype(F32)
        back = back + recv_s[s, f, :, 4 * fc:].astype(F32)
        grads, tangs, hidden = hidden_terms(pre, pre_dot, back)
        fing_s[1, f, 0, s] = grads
        fing_s[1, f, 1, s] = tangs
        finh_s[1, f, aligned(s, cap)] = hidden

        @pl.when(s == 0)
        def _():
            grads_copy(f).start()

        @pl.when(i >= nch)
        def _():
            part_s[1] += both_rows(f)

        return 0

    lax.fori_loop(0, 2 * nch, finish_chunk, 0)

    def give_back(h):
        def body(f, _):
            rows_copy(h, f).start()
            return 0

        return body

    lax.fori_loop(0, 3, give_back(0), 0)

    def spread(rep, s, h):
        hi = spans[h][1]
        return dot_nn(pick_s[rep, s, h * early:(h + 1) * early, :hi], part_s[rep, s, :hi].astype(BF))

    def core_copy(rep, h):
        return remote(give_s.at[rep, h], core_s.at[rep, h], as_.at[rep, h], ar_.at[rep, h], core)

    def give_core(rep, s, h):
        give_s[rep, h] = spread(rep, s, h).astype(BF)
        core_copy(rep, h).start()

    def over_cores(rep, h):
        core_copy(rep, h).wait_recv()
        both = own_s[h] + core_s[rep, h].astype(F32)
        sum_s[rep, h] = both.reshape(sum_s.shape[2:]).astype(BF)
        for k, (peer, where) in enumerate(zip(peers, plane)):
            remote(sum_s.at[rep, h, peer], slice_s.at[rep, h, k], bs_.at[rep], br_.at[rep, h], where).start()

    def over_plane(rep, h):
        remote(slice_s.at[rep, h], slice_s.at[rep, h], bs_.at[rep], br_.at[rep, h], core).wait_recv()
        total = sum_s[rep, h, t].astype(F32)
        for k in range(n_tensor - 1):
            total = total + slice_s[rep, h, k].astype(F32)
        return total.astype(BF)

    def in_term(rep, s, f):
        g = fing_s[rep, f, :, s].reshape(2 * cap, 2 * fc)
        return dot_tn(g, rows_s[rep, s].reshape(2 * cap, part)).reshape(2, fc, part)

    def out_term(rep, f):
        return dot_tn(finh_s[rep, f], dy_s[rep])

    def start_weights(f, _):
        part_f = aligned(f, fc)
        hin_o[0, :, part_f, :] = in_term(1, 0, f) + in_term(1, 1, f)
        hout_o[0, part_f, :] = out_term(1, f)
        return 0

    for h in range(parts):
        give_core(1, other, h)
    for h in range(parts):
        own_s[h] = spread(1, e, h)
    lax.fori_loop(0, half, start_weights, 0)
    for h in range(parts):
        over_cores(1, h)
    lax.fori_loop(half, nch, start_weights, 0)
    def take_first(f, _):
        grads_copy(f).wait_recv()
        part_s[0, 0] += back_rows(0, 0, f, 0, cap)
        hin_o[0, :, aligned(f, fc), :] += in_term(0, 0, f)
        return 0

    def take_second(h):
        lo, hi = spans[h]

        def body(f, _):
            rows_copy(h, f).wait_recv()
            part_s[0, 1, lo:hi] += back_rows(0, 1, f, lo, hi)
            return 0

        return body

    def to_owner(s, h):
        @pl.when(e != s)
        def _():
            give_core(0, s, h)

        @pl.when(e == s)
        def _():
            own_s[h] = spread(0, s, h)

    def owner_sums(s, h):
        @pl.when(e == s)
        def _():
            over_cores(0, h)

    def owner_shares(s, h):
        @pl.when(e == s)
        def _():
            ready_s[0, h, tz, tx] = over_plane(0, h)
            mid = ready_s.at[0, h, tz, tx]
            for where in plane:
                remote(mid, mid, cs_, cr_, where).start()

    def end_in(f, _):
        hin_o[0, :, aligned(f, fc), :] += in_term(0, 1, f)
        return 0

    def end_out(f, _):
        hout_o[0, aligned(f, fc), :] += out_term(0, f)
        return 0

    lax.fori_loop(0, nch, take_first, 0)
    for h in range(parts):
        to_owner(0, h)
    for h in range(parts):
        share_s[h] = over_plane(1, h)
    share_copy = remote(share_s, ready_s.at[1, :, tz, tx], ys_, yr_, over)
    share_copy.start()
    lax.fori_loop(3, nch, give_back(0), 0)

    @pl.when(e == 0)
    def _():
        lax.fori_loop(0, nch, give_back(1), 0)

    hidden = remote(finh_s.at[1], finh_s.at[0], c7s, c7r, over)

    for h in range(parts):
        owner_sums(0, h)
    share_copy.wait_recv()
    for k in range(2, n_tensor, 2):
        mid = ready_s.at[1, :, tz, tx]
        remote(mid, mid, zs_, zr_, {"tensor": lax.rem(t + k, n_tensor)}).start()
    lax.fori_loop(0, nch - 1, take_second(0), 0)

    @pl.when(e == 0)
    def _():
        pl.semaphore_signal(go_s, inc=1, device_id=core, device_id_type=MESH)

    lax.fori_loop(nch - 1, nch, take_second(0), 0)
    to_owner(1, 0)

    @pl.when(e == 1)
    def _():
        pl.semaphore_wait(go_s, 1)
        lax.fori_loop(0, nch, give_back(1), 0)
        hidden.start()

    line = ready_s.at[1, :, pl.ds(0, n_tensor // 2 - 1), tx]
    lines = remote(line, line, zs_, zr_, core)
    lines.wait_recv()
    column = ready_s.at[1, :, :, tx]
    columns = remote(column, column, xs_, xr_, near[0])
    columns.start()
    for h in range(parts):
        owner_shares(0, h)
    owner_sums(1, 0)
    lax.fori_loop(0, nch, take_second(1), 0)
    to_owner(1, 1)
    pl.when(e == 0)(hidden.start)
    owner_sums(1, 1)
    lax.fori_loop(0, nch, end_in, 0)
    owner_shares(1, 0)

    owner_shares(1, 1)
    hidden.wait_recv()
    lax.fori_loop(0, nch, end_out, 0)
    plane_out = [remote(slice_s.at[0], slice_s.at[0], cs_, cr_, core), columns]
    for c in plane_out:
        c.wait_recv()
    tok_o[:, mine] = ready_s[0].astype(F32).reshape(rows, part)
    tok_o[:, theirs] = ready_s[1].astype(F32).reshape(rows, part)

    for c in first + cross + [shareds] + passed + plane_out + [lines, share_copy]:
        c.wait_send()
    for r in range(2):
        for h in range(parts):
            core_copy(r, h).wait_send()
        remote(slice_s.at[r], slice_s.at[r], bs_.at[r], br_.at[r, 0], core).wait_send()
    remote(send_s, send_s, c5s, c5r.at[0, 0], over).wait_send()
    remote(fing_s.at[1], fing_s.at[1], c6s, c6r.at[0, 0], over).wait_send()
    hidden.wait_send()


def exchange(args, cap, fc):
    tokens, ids, w_in = args[0], args[3], args[5]
    n_tensor = lax.axis_size("tensor")
    rows, width = tokens.shape
    _, _, ff, part = w_in.shape
    topk = ids.shape[0]
    nch, peers, parts = ff // fc, n_tensor - 1, 2
    few = rows // n_tensor // parts
    dma = pltpu.SemaphoreType.DMA
    hbm = pl.BlockSpec(memory_space=pltpu.HBM)
    vmem = pl.BlockSpec(memory_space=pltpu.VMEM)
    return pl.pallas_call(
        functools.partial(exchange_kernel, n_tensor, topk, cap, fc),
        name="exchange",
        out_shape=[
            pltpu.VMEM((1, 2, ff, part), F32),
            pltpu.VMEM((1, ff, part), F32),
            pltpu.VMEM((rows, width), F32),
        ],
        in_specs=[hbm] * 9,
        out_specs=[vmem] * 3,
        scratch_shapes=[
            pltpu.VMEM((nch, 3, 2, fc, part), BF),
            pltpu.VMEM((2, 2, 3, rows, part), BF),
            pltpu.VMEM((2, 2, 2 * topk, rows), F32),
            pltpu.VMEM((2, 2, rows, rows), BF),
            pltpu.VMEM((2, 2, 2, cap, part), BF),
            pltpu.VMEM((2, 2 * cap, part), BF),
            pltpu.VMEM((2, nch, cap, 6 * fc), BF),
            pltpu.VMEM((2, nch, cap, 6 * fc), BF),
            pltpu.VMEM((2, nch, 2, 2, cap, 2 * fc), BF),
            pltpu.VMEM((2, nch, 2 * cap, fc), BF),
            pltpu.VMEM((2, 2, cap, part), F32),
            pltpu.VMEM((parts, rows // 2, part), F32),
            pltpu.VMEM((2, parts, rows // 2, part), BF),
            pltpu.VMEM((2, parts, rows // 2, part), BF),
            pltpu.VMEM((2, parts, n_tensor, few, part), BF),
            pltpu.VMEM((2, parts, peers, few, part), BF),
            pltpu.VMEM((parts, few, part), BF),
            pltpu.VMEM((2, parts, n_tensor // 2, 2, few, part), BF),
            pltpu.VMEM((topk, rows), jnp.int32),
            pltpu.SemaphoreType.REGULAR((n_tensor.bit_length(),)),
            pltpu.SemaphoreType.REGULAR,
            pltpu.VMEM((3, rows // n_tensor, part), BF),
            dma((nch,)), dma((4,)),
            dma((2,)), dma((2,)), dma((2,)), dma((2,)), dma, dma, dma((2,)), dma((2,)),
            dma, dma((2, nch)), dma, dma((3, nch)), dma, dma,
            dma((2, parts)), dma((2, parts)), dma((2,)), dma((2, parts)),
            dma, dma, dma, dma, dma, dma, dma, dma,
        ],
        compiler_params=pltpu.CompilerParams(
            collective_id=0, has_side_effects=True, vmem_limit_bytes=44 * 1024 * 1024
        ),
    )(*[pltpu.with_memory_space_constraint(v, pltpu.HBM) for v in args])


def store_kernel(hin_v, hout_v, tok_v, hin_o, hout_o, tok_o, sem):
    ff = hin_v.shape[2]
    step = ff // 3
    copies = []
    for i in range(3):
        span = pl.ds(i * step, step)
        copies += [(hin_v.at[0, g, span], hin_o.at[0, g, span]) for g in range(2)]
        copies.append((hout_v.at[0, span], hout_o.at[0, span]))
    copies.append((tok_v, tok_o))
    copies = [pltpu.make_async_copy(src, dst, sem.at[i]) for i, (src, dst) in enumerate(copies)]
    for c in copies:
        c.start()
    for c in copies:
        c.wait()


def store(*results):
    return pl.pallas_call(
        store_kernel,
        name="store",
        out_shape=[pltpu.HBM(v.shape, v.dtype) for v in results],
        in_specs=[pl.BlockSpec(memory_space=pltpu.VMEM)] * 3,
        out_specs=[pl.BlockSpec(memory_space=pltpu.HBM)] * 3,
        scratch_shapes=[pltpu.SemaphoreType.DMA((10,))],
        compiler_params=pltpu.CompilerParams(vmem_limit_bytes=4 * 1024 * 1024),
    )(*[pltpu.with_memory_space_constraint(v, pltpu.VMEM) for v in results])


def kernel_shards(tokens, tangent, cotangent, expert_ids, gates, w_in, v_in, w_out, v_out):
    rows, _ = tokens.shape
    topk = expert_ids.shape[1]
    all_experts = lax.axis_size("tensor") * lax.axis_size("expert")
    cap = min(rows, 3 * rows * topk // (2 * all_experts))
    args = (tokens, tangent, cotangent, expert_ids.T, gates.T, w_in, v_in, w_out, v_out)
    hvp_in, hvp_out, out = exchange(args, cap, 128)
    hvp_in, hvp_out, out = store(hvp_in, hvp_out, out)
    return out, hvp_in, hvp_out


def shards(*args):
    tokens, expert_ids, w_in = args[0], args[3], args[5]
    n_tensor = lax.axis_size("tensor")
    rows, topk = expert_ids.shape
    fits = (
        lax.axis_size("expert") == 2 and lax.axis_size("dp") == 2 and w_in.shape[0] == 1
        and tokens.shape[1] == 2 * w_in.shape[3] and w_in.shape[3] % 128 == 0 and w_in.shape[2] % 256 == 0
        and rows == 128 and n_tensor > 2 and n_tensor & (n_tensor - 1) == 0 and rows % (16 * n_tensor) == 0
        and topk % 8 == 0 and (3 * rows * topk) % (64 * n_tensor) == 0 and 3 * topk > 2 * n_tensor
    )
    return (kernel_shards if fits else plain_shards)(*args)


def solution(mesh):
    rows = P(("expert", "dp"), None)
    wide = P(("tensor", "expert"), None, None, "dp")
    tall = P(("tensor", "expert"), None, "dp")
    return jax.shard_map(
        shards,
        mesh=mesh,
        in_specs=(rows, rows, rows, rows, rows, wide, wide, tall, tall),
        out_specs=(rows, wide, tall),
        check_vma=False,
    )
```
